32 devices in a mesh: groups: 2 (over y), ctx: 4 (over z), role: 2 (over x), seq: 2 (over core).
Axes of the slice: x: 2, y: 2, z: 4, core: 2. Of those that a mesh axis runs over, the one named last changes fastest.
Arguments:
- queries: bfloat16 [32, 128, 576], P(('groups', 'role', 'seq'), 'ctx'), parts along dimension 0, may hold values from -24 to 24
- cache: bfloat16 [16, 4096, 576], P(('groups', 'role', 'seq'), 'ctx'), parts along dimension 0, may hold values from -4 to 4
- lengths: int32 [16], P(('groups', 'role', 'seq')), parts along dimension 0, may hold values from 4 to 4096, as said below
- positions: int32 [32], P(('groups', 'role', 'seq')), parts along dimension 0, may hold values from 0 to 4098, as said below
- value_up_weight: bfloat16 [128, 512, 128], P('ctx', ('role', 'seq')), may hold values from -0.25 to 0.25
- out_proj: bfloat16 [16384, 7168], P('ctx', ('role', 'seq')), may hold values from -0.046875 to 0.046875
- residual: bfloat16 [32, 7168], P('groups', ('role', 'seq')), parts along dimension 0, may hold values from -4 to 4
- norm_gain: float32 [7168], P(('role', 'seq')), may hold values from 0.5 to 1.5
- gate_weight: bfloat16 [7168, 9216], P(('role', 'seq'), 'ctx'), may hold values from -0.0625 to 0.0625
- up_weight: bfloat16 [7168, 9216], P(('role', 'seq'), 'ctx'), may hold values from -0.0625 to 0.0625
- down_weight: bfloat16 [9216, 7168], P('ctx', ('role', 'seq')), may hold values from -0.0625 to 0.0625
Outputs:
- layer_out: bfloat16 [32, 7168], P(('groups', 'ctx'), ('role', 'seq')), parts along dimension 0
The draws below stay inside these ranges and needn't reach their ends.
There are 2 independent parts, one for each index of `groups`. The reference program is written for one: setup_inputs(seed, part) draws one part's arguments, and reference() takes and returns one part's arrays. A program takes and returns all parts, laid end to end along the dimension named above; an argument that names none is the same for every part. Nothing has to cross between parts.
Inputs may be any that keep to these rules, and one draw needn't show every extreme that they name: `lengths`: every sequence has at least 4 cached positions, and in every draw some sequence has all 4096. positions[r] lies between lengths[r // 2] - 4 and lengths[r // 2] + 2.
All inputs are finite; a program needn't handle non-finite values.
Results may differ from the reference program's by a relative error of at most 0.013.
Values may be sent and summed in bfloat16 or wider, within the bound.
A program may use at most 128 MiB of HBM per device.

```python
import jax
import jax.numpy as jnp
from jax import lax

D = 7168
HEADS = 128
LATENT = 512
ROPE = 64
VDIM = 128
FF = 9216
MTP = 2
CTX_DEV = 1024
SEQS = 8
ROWS = 16
CTX_LEN = 4096
N_CTX = 4


def length_table(key):
    base = jax.random.fold_in(key, 101)
    first_key, second_key = jax.random.split(base)
    spread = jax.random.randint(first_key, (SEQS,), 0, 1024)
    counts = 4 + spread * spread // 1024 * (CTX_LEN - 4) // 1024
    chosen = jax.random.randint(second_key, (), 0, SEQS)
    counts = jnp.where(jnp.arange(SEQS) == chosen, CTX_LEN, counts)
    return counts.astype(jnp.int32)


def draw_lengths(key, part):
    return length_table(key)


def draw_positions(key, part):
    counts = jnp.repeat(length_table(key), MTP)
    offsets = jax.random.randint(jax.random.fold_in(key, 102), (ROWS,), -4, 3)
    return (counts + offsets).astype(jnp.int32)


def draw_cache(key, part):
    value_vectors = jax.random.truncated_normal(jax.random.fold_in(key, 202), -4.0, 4.0, (SEQS, CTX_LEN, LATENT + ROPE), jnp.float32)
    return value_vectors.astype(jnp.bfloat16)


def draw_queries(key, part):
    value_vectors = jax.random.truncated_normal(jax.random.fold_in(key, 204), -4.0, 4.0, (ROWS, HEADS, LATENT + ROPE), jnp.float32)
    return value_vectors.astype(jnp.bfloat16)


def levels(own_key, shape, cuts, smallest, top_value):
    loudness = 1.0
    for position, blocks in cuts:
        heights = jax.random.uniform(jax.random.fold_in(jax.random.fold_in(own_key, 6), position), (blocks,), jnp.float32, smallest / len(cuts), top_value / len(cuts))
        loudness = loudness * jnp.repeat(jnp.exp(heights), shape[position] // blocks).reshape((-1,) + (1,) * (len(shape) - 1 - position))
    return loudness


def normal_values(key, dims, scale, limit, cuts=(), held_as=jnp.bfloat16):
    entries = jax.random.normal(key, dims, jnp.float32) * scale
    if len(cuts) > 0:
        entries = levels(key, dims, cuts, -0.22, 0.18) * entries
    return jnp.clip(entries, min=-limit, max=limit).astype(held_as)


def setup_inputs(seed: int = 0, part: int = 0) -> dict:
    keys = jax.random.split(jax.random.key(seed), 12)
    part_keys = jax.random.split(jax.random.fold_in(keys[11], part), 12)
    return {
        "queries": draw_queries(jax.random.fold_in(jax.random.fold_in(keys[11], part), 71), part),
        "cache": draw_cache(jax.random.fold_in(jax.random.fold_in(keys[11], part), 71), part),
        "lengths": draw_lengths(jax.random.fold_in(jax.random.fold_in(keys[11], part), 71), part),
        "positions": draw_positions(jax.random.fold_in(jax.random.fold_in(keys[11], part), 71), part),
        "value_up_weight": normal_values(keys[4], (HEADS, LATENT, VDIM), LATENT ** -0.5, 0.25, ((0, 4), (1, 4))),
        "out_proj": normal_values(keys[5], (HEADS * VDIM, D), (HEADS * VDIM) ** -0.5, 0.046875, ((0, 4), (1, 4))),
        "residual": normal_values(part_keys[6], (ROWS, D), 0.25, 4.0, ((1, 4),)),
        "norm_gain": jnp.clip(1.0 + 0.1 * jax.random.normal(keys[7], (D,), jnp.float32), 0.5, 1.5),
        "gate_weight": normal_values(keys[8], (D, FF), D ** -0.5, 0.0625, ((0, 4), (1, 4))),
        "up_weight": normal_values(keys[9], (D, FF), D ** -0.5, 0.0625, ((0, 4), (1, 4))),
        "down_weight": normal_values(keys[10], (FF, D), FF ** -0.5, 0.0625, ((0, 4), (1, 4))),
    }


softmax_scale = 0.07216878364870323
epsilon = 1e-06

def attend_single_sequence(packed):
    rows_pair, keys_all, length, spots = packed
    width = LATENT + ROPE
    flat_rows = rows_pair.reshape(MTP * HEADS, width)
    scores = jnp.dot(flat_rows, keys_all.T, preferred_element_type=jnp.float32) * softmax_scale
    places = jnp.arange(CTX_LEN, dtype=jnp.int32)
    limits = jnp.repeat(spots, HEADS)
    live = (places[None, :] < length) & (places[None, :] <= limits[:, None])
    scores = scores.reshape(MTP * HEADS, N_CTX, CTX_DEV)
    live = live.reshape(MTP * HEADS, N_CTX, CTX_DEV)
    block_max = lax.optimization_barrier(jnp.max(jnp.where(live, scores, jnp.float32(-1e+30)), axis=-1))
    probs = jnp.exp(jnp.where(live, scores - block_max[..., None], jnp.float32(-1e+30))).astype(jnp.bfloat16)
    block_weight_sum = lax.optimization_barrier(jnp.sum(probs.astype(jnp.float32), axis=-1))
    latents = keys_all[:, :LATENT].reshape(N_CTX, CTX_DEV, LATENT)
    block_out = jnp.einsum('hbj,bjd->hbd', probs.astype(jnp.float32), latents.astype(jnp.float32))
    highest = lax.optimization_barrier(jnp.max(block_max, axis=-1))
    factor = jnp.exp(block_max - highest[:, None])
    numer = lax.optimization_barrier(jnp.sum(factor[..., None] * block_out, axis=1))
    denom = lax.optimization_barrier(jnp.sum(factor * block_weight_sum, axis=1))
    return (numer / denom[:, None]).reshape(MTP, HEADS, LATENT)

def reference(queries, cache, lengths, positions, value_up_weight, out_proj, residual, norm_gain, gate_weight, up_weight, down_weight):
    grouped = queries.reshape(SEQS, MTP, HEADS, LATENT + ROPE)
    spots = positions.reshape(SEQS, MTP)
    attended_values = lax.map(attend_single_sequence, (grouped, cache, lengths, spots))
    attended_values = attended_values.reshape(ROWS, HEADS, LATENT).astype(jnp.bfloat16)
    value_vectors = jnp.einsum('nut,utc->nuc', attended_values.astype(jnp.float32), value_up_weight.astype(jnp.float32))
    value_vectors = value_vectors.astype(jnp.bfloat16).reshape(ROWS, HEADS * VDIM)
    attn_out = jnp.dot(value_vectors, out_proj, preferred_element_type=jnp.float32)
    resid = residual.astype(jnp.float32) + attn_out
    sumsq = lax.optimization_barrier(jnp.sum(resid * resid, axis=1))
    normed = (resid * lax.rsqrt(sumsq / D + epsilon)[:, None] * norm_gain[None, :]).astype(jnp.bfloat16)
    gate = jnp.dot(normed, gate_weight, preferred_element_type=jnp.float32)
    up = jnp.dot(normed, up_weight, preferred_element_type=jnp.float32)
    hidden = (jax.nn.silu(gate) * up).astype(jnp.bfloat16)
    return (resid + jnp.dot(hidden, down_weight, preferred_element_type=jnp.float32)).astype(jnp.bfloat16)
```

```python
import functools

import jax
import jax.numpy as jnp
from jax import lax
from jax.experimental import pallas as pl
from jax.experimental.pallas import tpu as pltpu
from jax.sharding import PartitionSpec as P

D = 7168
LATENT = 512
MTP = 2

softmax_scale = 0.07216878364870323
epsilon = 1e-06
MESH = pl.DeviceIdType.MESH
VMEM_BYTES = 60 * 1024 * 1024
f32, bf16 = jnp.float32, jnp.bfloat16


def ctx_group(n):
    me = lax.axis_index("ctx")

    def peer(d):
        k = lax.rem(me + d, n)
        return k, {"ctx": k}

    return me, peer


def feature_group(n_role, n_seq):
    n = n_role * n_seq
    me = lax.axis_index("role") * n_seq + lax.axis_index("seq")

    def peer(d):
        k = lax.rem(me + d, n)
        return k, {"role": k // n_seq, "seq": lax.rem(k, n_seq)}

    return me, peer


def enter(groups):
    barrier = pltpu.get_barrier_semaphore()
    count = 0
    for n, peer in groups:
        for d in range(1, n):
            pl.semaphore_signal(barrier, inc=1, device_id=peer(d)[1], device_id_type=MESH)
            count += 1
    pl.semaphore_wait(barrier, count)


def remote(src, dst, send, recv, device):
    return pltpu.make_async_remote_copy(
        src_ref=src, dst_ref=dst, send_sem=send, recv_sem=recv,
        device_id=device, device_id_type=MESH,
    )


def attend(n, n_role, n_seq, q_ref, cache_ref, cache_copy, len_ref, pos_ref, out_ref,
           q_all, o_send, o_recv, s_send, s_recv, a_send, sems):
    nr = n_role * n_seq
    me, peer = ctx_group(n)
    fme, fpeer = feature_group(n_role, n_seq)
    seqs, _, context = cache_ref.shape
    rows = q_ref.shape[1]
    heads = rows // MTP

    q_copies = []
    for s in range(seqs):
        for d in range(1, n):
            c = remote(q_ref.at[s], q_all.at[me, s], sems.at[s, d], sems.at[seqs + s, d],
                       peer(d)[1])
            c.start()
            q_copies.append(c)

    places = me * context + lax.broadcasted_iota(jnp.int32, (rows, context), 1)
    first = lax.broadcasted_iota(jnp.int32, (rows, context), 0) < heads
    lives = []
    for s in range(seqs):
        limit = jnp.where(first, pos_ref[MTP * s], pos_ref[MTP * s + 1])
        lives.append((places < len_ref[s]) & (places <= limit))

    lane = lax.broadcasted_iota(jnp.int32, (rows, 128), 1)

    def block(q, s):
        keys = cache_ref[s]
        scores = jnp.dot(q, keys, preferred_element_type=f32) * softmax_scale
        live = lives[s]
        top = jnp.max(jnp.where(live, scores, -1e30), axis=1, keepdims=True)
        probs = jnp.exp(jnp.where(live, scores - top, -1e30)).astype(bf16)
        total = jnp.sum(probs.astype(f32), axis=1, keepdims=True)
        out = lax.dot_general(
            probs, keys[:LATENT], (((1,), (1,)), ((), ())), preferred_element_type=f32)
        return out, top, total

    cache_copy.wait()
    own = [block(q_ref[s], s) for s in range(seqs)]
    o_copies, s_copies = {}, {}
    for s in range(seqs):
        for d in range(1, n):
            src, device = peer(n - d)
            remote(q_ref.at[s], q_all.at[src, s], sems.at[s, d], sems.at[seqs + s, d],
                   device).wait_recv()
            o, top, total = block(q_all[src, s], s)
            o_send[d, s] = o.astype(bf16)
            s_send[d, s] = jnp.where(lane == 0, top, total).T[0:8]
            c = remote(o_send.at[d, s], o_recv.at[d, s], sems.at[2 * seqs + s, d],
                       sems.at[3 * seqs + s, d], device)
            c.start()
            o_copies[s, d] = c
            c = remote(s_send.at[d, s], s_recv.at[d, s], sems.at[4 * seqs + s, d],
                       sems.at[5 * seqs + s, d], device)
            c.start()
            s_copies[s, d] = c
    for c in q_copies:
        c.wait_send()

    heads = rows // MTP
    merged = []
    for s in range(seqs):
        own_o, top, total = own[s]
        tops, totals = [top], [total]
        for d in range(1, n):
            s_copies[s, d].wait()
            back = jnp.concatenate([s_recv[d, s]] * 16, axis=0).T
            tops.append(back[:, 0:1])
            totals.append(back[:, 1:2])
        highest = functools.reduce(jnp.maximum, tops)
        factors = [jnp.exp(t - highest) for t in tops]
        denom = sum(f * t for f, t in zip(factors, totals))
        numer = factors[0] * own_o
        for d in range(1, n):
            o_copies[s, d].wait()
            numer = numer + factors[d] * o_recv[d, s].astype(f32)
        merged.append((numer / denom).astype(bf16))

    part = LATENT // nr
    for k in range(nr):
        for r in range(seqs * MTP):
            t = r % MTP
            a_send[k, r] = merged[r // MTP][t * heads:(t + 1) * heads, k * part:(k + 1) * part]
    copies = []
    for d in range(1, nr):
        k, device = fpeer(d)
        c = remote(a_send.at[k], out_ref.at[fme], sems.at[6 * seqs, d], sems.at[7 * seqs, d], device)
        c.start()
        copies.append(c)
    out_ref[fme] = a_send[fme]
    for d in range(1, nr):
        k, device = fpeer(nr - d)
        copies[d - 1].wait_send()
        remote(a_send.at[k], out_ref.at[k], sems.at[6 * seqs, d], sems.at[7 * seqs, d],
               device).wait_recv()


def layer_kernel(n, n_role, n_seq, q_ref, cache_hbm, len_ref, pos_ref, vu_hbm, res_ref, gain_ref,
                 wo_hbm, wg_hbm, wu_hbm, wd_hbm,
                 out_ref, cache, vu, q_all, o_send, o_recv, s_send, s_recv, a_send, a_all, a_head,
                 mixed, pv_ref, wo, wg, wu, wd, pv_recv, v_send, v_all, v_full, acc, po_send,
                 po_recv, resid, xg_ref, g_acc, u_acc, gu_send, gu_recv, ss_send, ss_recv, h_send,
                 h_all, h_full, dn, dn_send, dn_recv, wsem, lsem, asems, sems):
    nr = n_role * n_seq
    me, peer = ctx_group(n)
    fme, fpeer = feature_group(n_role, n_seq)

    cache_copy = pltpu.make_async_copy(cache_hbm, cache, lsem.at[0])
    cache_copy.start()
    vu_copy = pltpu.make_async_copy(vu_hbm, vu, lsem.at[1])
    vu_copy.start()
    weights = []
    for which, (hbm, vmem) in enumerate(((wo_hbm, wo), (wg_hbm, wg), (wu_hbm, wu), (wd_hbm, wd))):
        depth = vmem.shape[1]

        def fetch(i, hbm=hbm, vmem=vmem, depth=depth, which=which):
            return pltpu.make_async_copy(
                hbm.at[pl.ds(i * depth, depth)], vmem.at[i], wsem.at[which, i])

        weights.append((fetch, vmem))
    for fetch, vmem in weights:
        for i in range(vmem.shape[0]):
            fetch(i).start()
    enter(((n, peer), (nr, fpeer)))
    attend(n, n_role, n_seq, q_ref, cache, cache_copy, len_ref, pos_ref, a_all,
           q_all, o_send, o_recv, s_send, s_recv, a_send, asems)
    rows, heads = a_all.shape[1:3]
    for j in range(nr):
        for r in range(rows):
            a_head[:, j * rows + r, :] = a_all[j, r].astype(f32)
    vu_copy.wait()
    vdim = vu.shape[2]
    for h in range(heads):
        mixed[:, h * vdim:(h + 1) * vdim] = jnp.dot(
            a_head[h].astype(bf16), vu[h], preferred_element_type=f32)
    for k in range(nr):
        pv_ref[k] = mixed[k * rows:(k + 1) * rows, :].astype(bf16)

    def matmul(x_ref, *pairs):
        chunks, depth, _ = weights[pairs[0][0]][1].shape
        for which, acc_ref in pairs:
            fetch, vmem = weights[which]
            fetch(0).wait()
            acc_ref[...] = jnp.dot(x_ref[:, :depth], vmem[0], preferred_element_type=f32)
        if chunks == 1:
            return

        @pl.loop(1, chunks)
        def _(i):
            x = x_ref[:, pl.ds(pl.multiple_of(i * depth, depth), depth)]
            for which, acc_ref in pairs:
                fetch, vmem = weights[which]
                fetch(i).wait()
                acc_ref[...] += jnp.dot(x, vmem[i], preferred_element_type=f32)

    def swap(size, peer_of, chunk, recv, row):
        copies = []
        for d in range(1, size):
            k, device = peer_of(d)
            c = remote(chunk(k), recv.at[d], sems.at[row, d], sems.at[row + 1, d], device)
            c.start()
            copies.append(c)
        return copies

    def gather(size, my, peer_of, send, full, row):
        copies = []
        for d in range(1, size):
            c = remote(send, full.at[my], sems.at[row, d], sems.at[row + 1, d], peer_of(d)[1])
            c.start()
            copies.append(c)
        full[my] = send[...]
        for d in range(1, size):
            k, device = peer_of(size - d)
            copies[d - 1].wait_send()
            remote(send, full.at[k], sems.at[row, d], sems.at[row + 1, d], device).wait_recv()

    part = res_ref.shape[0] // nr
    copies = swap(nr, fpeer, lambda k: pv_ref.at[k], pv_recv, 0)
    vals = pv_ref[fme].astype(f32)
    for d in range(1, nr):
        copies[d - 1].wait()
        vals = vals + pv_recv[d].astype(f32)
    v_send[...] = vals.astype(bf16)
    gather(nr, fme, fpeer, v_send, v_all, 2)
    for k in range(nr):
        acc_rows = v_all[k].astype(f32)
        v_full[k * part:(k + 1) * part, :] = acc_rows
    x_ref = xg_ref[0]
    x_ref[...] = v_full[...].astype(bf16)
    matmul(x_ref, (0, acc))

    po_send[...] = acc[...].astype(bf16)
    copies = swap(n, peer, lambda k: po_send, po_recv, 4)
    total = res_ref[...].astype(f32) + acc[...]
    for d in range(1, n):
        copies[d - 1].wait()
        total = total + po_recv[d].astype(f32)
    crows = res_ref.shape[0] // n
    for k in range(n):
        resid[k] = total[k * crows:(k + 1) * crows]
    sumsq = jnp.sum(total * total, axis=1, keepdims=True)
    sumsq = jnp.broadcast_to(sumsq, (total.shape[0], 128))
    for k in range(nr):
        ss_send[k] = sumsq[k * part:(k + 1) * part]
    s_copies = swap(nr, fpeer, lambda k: ss_send.at[k], ss_recv, 6)
    x_ref = xg_ref[1]
    x_ref[...] = (total * gain_ref[...]).astype(bf16)
    matmul(x_ref, (1, g_acc), (2, u_acc))

    for j, a in enumerate((g_acc, u_acc)):
        for k in range(nr):
            gu_send[k, j] = a[k * part:(k + 1) * part, :].astype(bf16)
    copies = swap(nr, fpeer, lambda k: gu_send.at[k], gu_recv, 8)
    ss = ss_send[fme]
    for d in range(1, nr):
        s_copies[d - 1].wait()
        ss = ss + ss_recv[d]
    inv = lax.rsqrt(ss[:, 0:1] / D + epsilon)
    gate = gu_send[fme, 0].astype(f32)
    up = gu_send[fme, 1].astype(f32)
    for d in range(1, nr):
        copies[d - 1].wait()
        gate = gate + gu_recv[d, 0].astype(f32)
        up = up + gu_recv[d, 1].astype(f32)
    gate = gate * inv
    up = up * inv
    h_send[...] = (gate / (1.0 + jnp.exp(-gate)) * up).astype(bf16)
    gather(nr, fme, fpeer, h_send, h_all, 10)
    for k in range(nr):
        h_full[k * part:(k + 1) * part, :] = h_all[k].astype(f32)
    x_ref = xg_ref[2]
    x_ref[...] = h_full[...].astype(bf16)
    matmul(x_ref, (3, acc))

    for k in range(n):
        piece = acc[k * crows:(k + 1) * crows, :]
        dn[k] = piece
        dn_send[k] = piece.astype(bf16)
    copies = swap(n, peer, lambda k: dn_send.at[k], dn_recv, 12)
    result = resid[me] + dn[me]
    for d in range(1, n):
        copies[d - 1].wait()
        result = result + dn_recv[d].astype(f32)
    out_ref[...] = result.astype(bf16)


def chunk_of(depth):
    for size in (1024, 768, 512, 256):
        if depth % size == 0:
            return size
    return depth


def per_device_latents(sizes, queries, cache, lengths, positions, value_up_weight, out_proj, residual,
               norm_gain, gate_weight, up_weight, down_weight):
    n, n_role, n_seq = sizes
    nr = n_role * n_seq
    rows, heads, width = queries.shape
    seqs = cache.shape[0]
    span = rows * heads // seqs
    lat = LATENT // nr
    vmem = pl.BlockSpec(memory_space=pltpu.VMEM)
    smem = pl.BlockSpec(memory_space=pltpu.SMEM)
    hbm = pl.BlockSpec(memory_space=pl.ANY)
    most = max(n, nr)
    sems = lambda k: pltpu.SemaphoreType.DMA((k, most))
    vwide = heads * value_up_weight.shape[2]
    all_rows, dd = residual.shape
    ff = gate_weight.shape[1]
    part, crows = all_rows // nr, all_rows // n

    def held(w):
        size = chunk_of(w.shape[0])
        return pltpu.VMEM((w.shape[0] // size, size, w.shape[1]), bf16)

    ws = (out_proj, gate_weight, up_weight, down_weight)
    most_chunks = max(w.shape[0] // chunk_of(w.shape[0]) for w in ws)
    V = pltpu.VMEM
    return pl.pallas_call(
        functools.partial(layer_kernel, n, n_role, n_seq),
        out_shape=jax.ShapeDtypeStruct((crows, dd), bf16),
        in_specs=[vmem, hbm, smem, smem, hbm, vmem, vmem] + [hbm] * 4,
        out_specs=vmem,
        scratch_shapes=[
            V((cache.shape[0], width, cache.shape[1]), bf16),
            V(value_up_weight.shape, bf16),
            V((n, seqs, span, width), bf16),
            V((n, seqs, span, LATENT), bf16),
            V((n, seqs, span, LATENT), bf16),
            V((n, seqs, 8, span), f32),
            V((n, seqs, 8, span), f32),
            V((nr, rows, heads, lat), bf16),
            V((nr, rows, heads, lat), bf16),
            V((heads, all_rows, lat), f32),
            V((all_rows, vwide), f32),
            V((nr, part, vwide), bf16),
            *[held(w) for w in ws],
            V((nr, part, vwide), bf16),
            V((part, vwide), bf16),
            V((nr, part, vwide), bf16),
            V((all_rows, vwide), f32),
            V((all_rows, dd), f32),
            V((all_rows, dd), bf16),
            V((n, all_rows, dd), bf16),
            V((n, crows, dd), f32),
            [V((all_rows, vwide), bf16), V((all_rows, dd), bf16), V((all_rows, ff), bf16)],
            V((all_rows, ff), f32),
            V((all_rows, ff), f32),
            V((nr, 2, part, ff), bf16),
            V((nr, 2, part, ff), bf16),
            V((nr, part, 128), f32),
            V((nr, part, 128), f32),
            V((part, ff), bf16),
            V((nr, part, ff), bf16),
            V((all_rows, ff), f32),
            V((n, crows, dd), f32),
            V((n, crows, dd), bf16),
            V((n, crows, dd), bf16),
            pltpu.SemaphoreType.DMA((4, most_chunks)),
            pltpu.SemaphoreType.DMA((2,)),
            sems(8 * seqs),
            sems(14),
        ],
        compiler_params=pltpu.CompilerParams(
            collective_id=0, has_side_effects=True, vmem_limit_bytes=VMEM_BYTES),
        name="layer",
    )(queries.reshape(seqs, span, width), cache.transpose(0, 2, 1), lengths, positions, value_up_weight,
      residual, norm_gain.reshape(1, dd), *ws)


LOG2E = 1.4426950408889634


def by_distance(n, me):
    found = []
    for i in range(n - 1):
        k = jnp.int32(0)
        for z in range(n):
            others = sorted((j for j in range(n) if j != z), key=lambda j: (abs(j - z), j))
            k = jnp.where(me == z, others[i], k)
        found.append(k)
    return found


def cut(width):
    unit = 256 if width % 256 == 0 else 128
    if width % unit or width < 2 * unit:
        return [(0, width)]
    first = -(-(width // unit) // 2) * unit
    return [(0, first), (first, width)]


def heads_kernel(n, n_role, n_seq, q_hbm, cache_hbm, len_ref, pos_ref, vu_hbm, res_hbm, gain_hbm,
                 wo_hbm, wg_hbm, wu_hbm, wd_hbm, out_ref,
                 q_ref, cache, vu, res_ref, gain_ref, wo, wg, wu, wd,
                 qn_send, qr_send, qn_all, qr_all, o_send, o_recv, st_send, st_recv, w_ref,
                 a_head, v_send, xv, acc, po_send, po_recv, resid, ss_send, ss_recv,
                 g_acc, u_acc, gu_send, gu_recv, h_send, h_all, h_full, dn, dn_send, dn_recv,
                 lsem, wsem, qsem, vusem, osem, ssem, vsem, posem, sssem, gusem, hsem, dnsem):
    nr = n_role * n_seq
    me = lax.axis_index("ctx")
    role, seq = lax.axis_index("role"), lax.axis_index("seq")
    fme = role * n_seq + seq
    near = by_distance(n, me)
    mates = []
    for dr in range(n_role):
        for ds in range(n_seq):
            if dr or ds:
                r, s = lax.rem(role + dr, n_role), lax.rem(seq + ds, n_seq)
                mates.append((r * n_seq + s, {"role": r, "seq": s}))
    seqs, span, width = q_ref.shape
    context = cache.shape[2]
    heads = span // MTP
    hk = heads // nr
    rope = width - LATENT
    lat = LATENT // nr
    own = n - 1

    q_copy = pltpu.make_async_copy(q_hbm, q_ref, lsem.at[0])
    q_copy.start()
    cache_copies = [
        pltpu.make_async_copy(cache_hbm, cache.at[:, pl.ds(0, width), :], lsem.at[1]),
        pltpu.make_async_copy(cache_hbm.at[:, pl.ds(LATENT, rope), :],
                              cache.at[:, pl.ds(width, rope), :], lsem.at[2]),
    ]
    for c in cache_copies:
        c.start()
    barrier = pltpu.get_barrier_semaphore()
    for k in near:
        pl.semaphore_signal(barrier, inc=1, device_id={"ctx": k}, device_id_type=MESH)
    for _, device in mates:
        pl.semaphore_signal(barrier, inc=1, device_id=device, device_id_type=MESH)
    vu_own = pltpu.make_async_copy(
        vu_hbm.at[pl.ds(pl.multiple_of(fme * hk, hk), hk)],
        vu.at[:, pl.ds(pl.multiple_of(fme * lat, lat), lat), :], lsem.at[3])
    vu_own.start()
    res_copy = pltpu.make_async_copy(res_hbm, res_ref, lsem.at[4])
    res_copy.start()
    gain_copy = pltpu.make_async_copy(gain_hbm, gain_ref.at[0], lsem.at[5])
    gain_copy.start()

    q_copy.wait()
    for s in range(seqs):
        qn, qr = [], []
        for k in range(nr):
            for t in range(MTP):
                at = t * heads + k * hk
                rows = q_ref[s, at:at + hk, :].astype(f32)
                qn.append(rows[:, :LATENT])
                qr.append(rows[:, LATENT:])
        qn_send[s] = jnp.concatenate(qn, axis=0).astype(bf16)
        qr = jnp.concatenate(qr, axis=0)
        qr_send[s] = jnp.concatenate([qr[:span // 2], qr[span // 2:]], axis=1).astype(bf16)
    weights = []
    for which, (hbm, vmem) in enumerate(((wo_hbm, wo), (wg_hbm, wg), (wu_hbm, wu), (wd_hbm, wd))):
        weights.append(pltpu.make_async_copy(hbm, vmem, wsem.at[which]))
    for c in weights:
        c.start()
    pl.semaphore_wait(barrier, len(near) + len(mates))

    sent = []

    def send(src, dst, send_sem, recv_sem, device):
        c = remote(src, dst, send_sem, recv_sem, device)
        c.start()
        sent.append(c)

    def drain():
        for c in sent:
            c.wait_send()
        sent.clear()

    for s in range(seqs):
        for k in near[::-1]:
            send(qn_send.at[s], qn_all.at[me, s], qsem.at[0, s, k], qsem.at[1, s, me], {"ctx": k})
            send(qr_send.at[s], qr_all.at[me, s], qsem.at[2, s, k], qsem.at[3, s, me], {"ctx": k})
    for k, device in mates:
        send(vu_hbm.at[pl.ds(pl.multiple_of(k * hk, hk), hk)],
             vu.at[:, pl.ds(pl.multiple_of(fme * lat, lat), lat), :],
             vusem.at[0, k], vusem.at[1, fme], device)

    column = lax.broadcasted_iota(jnp.int32, (span, context), 1)
    row = lax.broadcasted_iota(jnp.int32, (span, 1), 0)
    even = lax.rem(row, MTP * hk) < hk
    lane = lax.broadcasted_iota(jnp.int32, (span, 128), 1)
    half = lax.broadcasted_iota(jnp.int32, (span // 2, 2 * rope), 1) < rope
    ends = []
    for s in range(seqs):
        limit = jnp.where(even, pos_ref[MTP * s], pos_ref[MTP * s + 1]) + 1
        ends.append(jnp.minimum(limit, len_ref[s]) - me * context)

    def block(qn, qr, s, slot):
        zero = jnp.zeros_like(qr)
        q = jnp.concatenate(
            [qn, jnp.concatenate([jnp.where(half, qr, zero), jnp.where(half, zero, qr)], axis=0)],
            axis=1)
        keys = cache[s]
        scores = jnp.dot(q, keys, preferred_element_type=f32) * (softmax_scale * LOG2E)
        scores = jnp.where(column < ends[s], scores, -1e30)
        top = jnp.maximum(jnp.max(scores, axis=1, keepdims=True), -1e29)
        probs = jnp.exp2(scores - top).astype(bf16)
        total = jnp.sum(probs.astype(f32), axis=1, keepdims=True)
        out = lax.dot_general(
            probs, keys[:LATENT], (((1,), (1,)), ((), ())), preferred_element_type=f32)
        out = out.astype(bf16)
        for k in range(nr):
            o_send[slot, s, k] = out[k * MTP * hk:(k + 1) * MTP * hk]
        st_send[slot, s] = jnp.where(lane == 0, top, total).T[0:2]

    mine = me * nr + fme
    for c in cache_copies:
        c.wait()
    home = []
    for s in range(seqs):
        block(qn_send[s], qr_send[s], s, own)
        for k, device in mates:
            send(o_send.at[own, s, k], o_recv.at[mine, s], osem.at[0, s, own, k],
                 osem.at[1, s, me, fme], device)
            send(st_send.at[own, s], st_recv.at[mine, s], ssem.at[0, s, own, k],
                 ssem.at[1, s, me, fme], device)
        for c in (
            pltpu.make_async_copy(o_send.at[own, s, fme], o_recv.at[mine, s], osem.at[1, s, me, fme]),
            pltpu.make_async_copy(st_send.at[own, s], st_recv.at[mine, s], ssem.at[1, s, me, fme]),
        ):
            c.start()
    for s in range(seqs):
        for i, b in enumerate(near):
            there = {"ctx": b}
            remote(qn_send.at[s], qn_all.at[b, s], qsem.at[0, s, b], qsem.at[1, s, b],
                   there).wait_recv()
            remote(qr_send.at[s], qr_all.at[b, s], qsem.at[2, s, b], qsem.at[3, s, b],
                   there).wait_recv()
            block(qn_all[b, s], qr_all[b, s], s, i)
            for k in range(nr):
                device = {"ctx": b, "role": k // n_seq, "seq": k % n_seq}
                send(o_send.at[i, s, k], o_recv.at[mine, s], osem.at[0, s, i, k],
                     osem.at[1, s, me, fme], device)
                send(st_send.at[i, s], st_recv.at[mine, s], ssem.at[0, s, i, k],
                     ssem.at[1, s, me, fme], device)

    rows = seqs * MTP
    all_rows = nr * rows
    mine_at = pl.ds(pl.multiple_of(fme * MTP * hk, MTP * hk), MTP * hk)
    first = {"ctx": near[0]}
    for s in range(seqs):
        tops, totals = [], []
        for b in range(n):
            for j in range(nr):
                remote(st_send.at[0, s], st_recv.at[b * nr + j, s], ssem.at[0, s, 0, 0],
                       ssem.at[1, s, b, j], first).wait_recv()
            stats = [st_recv[b * nr + j, s] for j in range(nr)]
            tops.append(jnp.concatenate([x[0:1] for x in stats], axis=0))
            totals.append(jnp.concatenate([x[1:2] for x in stats], axis=0))
        highest = functools.reduce(jnp.maximum, tops)
        factors = [jnp.exp2(t - highest) for t in tops]
        denom = sum(f * t for f, t in zip(factors, totals))
        shares = jnp.concatenate([f / denom for f in factors], axis=0)
        copies = -(-128 // (n * nr))
        shares = jnp.concatenate([shares] * copies, axis=0)[:128]
        w_ref[s] = shares.T
        share = w_ref[s, mine_at, :]
        for j in range(nr):
            mixed = None
            for b in range(n):
                i = b * nr + j
                remote(o_send.at[0, s, 0], o_recv.at[i, s], osem.at[0, s, 0, 0],
                       osem.at[1, s, b, j], first).wait_recv()
                term = share[:, i:i + 1] * o_recv[i, s].astype(f32)
                mixed = term if mixed is None else mixed + term
            for t in range(MTP):
                a_head[:, j * rows + s * MTP + t, :] = mixed[t * hk:(t + 1) * hk]

    vu_own.wait()
    for k, device in mates:
        remote(vu_hbm.at[pl.ds(0, hk)], vu.at[:, pl.ds(pl.multiple_of(k * lat, lat), lat), :],
               vusem.at[0, k], vusem.at[1, k], device).wait_recv()
    vdim = vu.shape[2]
    for h in range(hk):
        v_send[:, h * vdim:(h + 1) * vdim] = jnp.dot(
            a_head[h].astype(bf16), vu[h], preferred_element_type=f32).astype(bf16)
    for k, device in mates:
        send(v_send, xv.at[fme], vsem.at[0, k], vsem.at[1, fme], device)
    weights[0].wait()
    deep = hk * vdim

    def wo_rows(k):
        return pl.ds(pl.multiple_of(k * deep, deep), deep)

    acc[...] = jnp.dot(v_send[...], wo[wo_rows(fme), :], preferred_element_type=f32)

    def arrived(k, device):
        remote(v_send, xv.at[k], vsem.at[0, k], vsem.at[1, k], device).wait_recv()

    early, late = mates[:n_seq - 1], mates[n_seq - 1:]
    for k, device in early:
        arrived(k, device)
        acc[...] += jnp.dot(xv[k], wo[wo_rows(k), :], preferred_element_type=f32)
    for k, device in late:
        arrived(k, device)
    dd = acc.shape[1]
    parts = cut(dd)
    for p, (c0, c1) in enumerate(parts):
        total = acc[:, c0:c1]
        for k, device in late:
            total = total + jnp.dot(xv[k], wo[wo_rows(k), c0:c1], preferred_element_type=f32)
        acc[:, c0:c1] = total
        po_send[:, c0:c1] = total.astype(bf16)
        for k in near[::-1]:
            send(po_send.at[:, c0:c1], po_recv.at[me, :, c0:c1], posem.at[0, p, k],
                 posem.at[1, p, me], {"ctx": k})
    drain()
    res_copy.wait()
    gain_copy.wait()
    weights[1].wait()
    weights[2].wait()

    part, crows = all_rows // nr, all_rows // n
    ff = g_acc.shape[1]
    fparts = [(f, min(f + 768, ff)) for f in range(0, ff, 768)]
    sumsq = jnp.zeros((all_rows, 1), f32)
    for p, (c0, c1) in enumerate(parts):
        total = res_ref[:, c0:c1].astype(f32) + acc[:, c0:c1]
        for k in near:
            remote(po_send.at[:, c0:c1], po_recv.at[k, :, c0:c1], posem.at[0, p, k],
                   posem.at[1, p, k], {"ctx": k}).wait_recv()
            total = total + po_recv[k, :, c0:c1].astype(f32)
        for k in range(n):
            resid[k, :, c0:c1] = total[k * crows:(k + 1) * crows]
        sumsq = sumsq + jnp.sum(total * total, axis=1, keepdims=True)
        x = (total * gain_ref[:, c0:c1]).astype(bf16)
        last = p == len(parts) - 1
        if last:
            wide = jnp.broadcast_to(sumsq, (all_rows, 128))
            for k in range(nr):
                ss_send[k] = wide[k * part:(k + 1) * part]
            for k, device in mates:
                send(ss_send.at[k], ss_recv.at[fme], sssem.at[0, k], sssem.at[1, fme], device)
        for q, (f0, f1) in enumerate(fparts if last else [(0, ff)]):
            for j, (w, a) in enumerate(((wg, g_acc), (wu, u_acc))):
                y = jnp.dot(x, w[c0:c1, f0:f1], preferred_element_type=f32)
                if p:
                    y = y + a[:, f0:f1]
                if not last:
                    a[:, f0:f1] = y
                    continue
                for k in range(nr):
                    gu_send[k, j, :, f0:f1] = y[k * part:(k + 1) * part].astype(bf16)
            if last:
                for k, device in mates:
                    send(gu_send.at[k, :, :, f0:f1], gu_recv.at[fme, :, :, f0:f1],
                         gusem.at[0, q, k], gusem.at[1, q, fme], device)
    ss = ss_send[fme]
    for k, device in mates:
        remote(ss_send.at[k], ss_recv.at[k], sssem.at[0, k], sssem.at[1, k], device).wait_recv()
        ss = ss + ss_recv[k]
    inv = lax.rsqrt(ss[:, 0:1] / D + epsilon)
    for q, (f0, f1) in enumerate(fparts):
        gate = gu_send[fme, 0, :, f0:f1].astype(f32)
        up = gu_send[fme, 1, :, f0:f1].astype(f32)
        for k, device in mates:
            remote(gu_send.at[k, :, :, f0:f1], gu_recv.at[k, :, :, f0:f1], gusem.at[0, q, k],
                   gusem.at[1, q, k], device).wait_recv()
            gate = gate + gu_recv[k, 0, :, f0:f1].astype(f32)
            up = up + gu_recv[k, 1, :, f0:f1].astype(f32)
        gate = gate * inv
        up = up * inv
        h = (gate / (1.0 + jnp.exp(-gate)) * up).astype(bf16)
        h_send[:, f0:f1] = h
        h_all[fme, :, f0:f1] = h
        for k, device in mates:
            send(h_send.at[:, f0:f1], h_all.at[fme, :, f0:f1], hsem.at[0, q, k],
                 hsem.at[1, q, fme], device)
    weights[3].wait()
    for q, (f0, f1) in enumerate(fparts):
        for k, device in mates:
            remote(h_send.at[:, f0:f1], h_all.at[k, :, f0:f1], hsem.at[0, q, k],
                   hsem.at[1, q, k], device).wait_recv()
        for k in range(nr):
            h_full[k * part:(k + 1) * part, f0:f1] = h_all[k, :, f0:f1].astype(f32)
        x = h_full[:, f0:f1].astype(bf16)
        last = q == len(fparts) - 1
        for p, (c0, c1) in enumerate(parts if last else [(0, dd)]):
            y = jnp.dot(x, wd[f0:f1, c0:c1], preferred_element_type=f32)
            if q:
                y = y + acc[:, c0:c1]
            if not last:
                acc[:, c0:c1] = y
                continue
            for k in range(n):
                piece = y[k * crows:(k + 1) * crows]
                dn[k, :, c0:c1] = piece
                dn_send[k, :, c0:c1] = piece.astype(bf16)
            for k in near[::-1]:
                send(dn_send.at[k, :, c0:c1], dn_recv.at[me, :, c0:c1], dnsem.at[0, p, k],
                     dnsem.at[1, p, me], {"ctx": k})
    drain()
    for p, (c0, c1) in enumerate(parts):
        result = resid[me, :, c0:c1] + dn[me, :, c0:c1]
        for k in near:
            remote(dn_send.at[k, :, c0:c1], dn_recv.at[k, :, c0:c1], dnsem.at[0, p, k],
                   dnsem.at[1, p, k], {"ctx": k}).wait_recv()
            result = result + dn_recv[k, :, c0:c1].astype(f32)
        out_ref[:, c0:c1] = result.astype(bf16)


def per_device(sizes, queries, cache, lengths, positions, value_up_weight, out_proj, residual,
               norm_gain, gate_weight, up_weight, down_weight):
    n, n_role, n_seq = sizes
    nr = n_role * n_seq
    rows, heads, width = queries.shape
    seqs, context = cache.shape[:2]
    rope = width - LATENT
    if heads % (8 * nr) or 2 * rope != 128 or n < 2 or nr < 2:
        return per_device_latents(
            sizes, queries, cache, lengths, positions, value_up_weight, out_proj, residual,
            norm_gain, gate_weight, up_weight, down_weight)
    hk = heads // nr
    span = rows * heads // seqs
    vdim = value_up_weight.shape[2]
    all_rows, dd = residual.shape
    ff = gate_weight.shape[1]
    part, crows = all_rows // nr, all_rows // n
    nf = -(-ff // 768)
    vmem = pl.BlockSpec(memory_space=pltpu.VMEM)
    smem = pl.BlockSpec(memory_space=pltpu.SMEM)
    hbm = pl.BlockSpec(memory_space=pl.ANY)
    V = pltpu.VMEM
    sems = lambda *k: pltpu.SemaphoreType.DMA(k)
    return pl.pallas_call(
        functools.partial(heads_kernel, n, n_role, n_seq),
        out_shape=jax.ShapeDtypeStruct((crows, dd), bf16),
        in_specs=[hbm, hbm, smem, smem] + [hbm] * 7,
        out_specs=vmem,
        scratch_shapes=[
            V((seqs, span, width), bf16),
            V((seqs, width + rope, context), bf16),
            V((hk, LATENT, vdim), bf16),
            V((all_rows, dd), bf16),
            V((1, dd), f32),
            V(out_proj.shape, bf16),
            V(gate_weight.shape, bf16),
            V(up_weight.shape, bf16),
            V(down_weight.shape, bf16),
            V((seqs, span, LATENT), bf16),
            V((seqs, span // 2, 2 * rope), bf16),
            V((n, seqs, span, LATENT), bf16),
            V((n, seqs, span // 2, 2 * rope), bf16),
            V((n, seqs, nr, MTP * hk, LATENT), bf16),
            V((n * nr, seqs, MTP * hk, LATENT), bf16),
            V((n, seqs, 2, span), f32),
            V((n * nr, seqs, 2, span), f32),
            V((seqs, span, 128), f32),
            V((hk, all_rows, LATENT), f32),
            V((all_rows, hk * vdim), bf16),
            V((nr, all_rows, hk * vdim), bf16),
            V((all_rows, dd), f32),
            V((all_rows, dd), bf16),
            V((n, all_rows, dd), bf16),
            V((n, crows, dd), f32),
            V((nr, part, 128), f32),
            V((nr, part, 128), f32),
            V((all_rows, ff), f32),
            V((all_rows, ff), f32),
            V((nr, 2, part, ff), bf16),
            V((nr, 2, part, ff), bf16),
            V((part, ff), bf16),
            V((nr, part, ff), bf16),
            V((all_rows, ff), f32),
            V((n, crows, dd), f32),
            V((n, crows, dd), bf16),
            V((n, crows, dd), bf16),
            sems(6),
            sems(4),
            sems(4, seqs, n),
            sems(2, nr),
            sems(2, seqs, n, nr),
            sems(2, seqs, n, nr),
            sems(2, nr),
            sems(2, 2, n),
            sems(2, nr),
            sems(2, nf, nr),
            sems(2, nf, nr),
            sems(2, 2, n),
        ],
        compiler_params=pltpu.CompilerParams(
            collective_id=0, has_side_effects=True, vmem_limit_bytes=VMEM_BYTES),
        name="layer",
    )(queries.reshape(seqs, span, width), cache.transpose(0, 2, 1), lengths, positions, value_up_weight,
      residual, norm_gain, out_proj, gate_weight, up_weight, down_weight)


def solution(mesh):
    placed = (
        P(("groups", "role", "seq"), "ctx", None),
        P(("groups", "role", "seq"), "ctx", None),
        P(("groups", "role", "seq")),
        P(("groups", "role", "seq")),
        P("ctx", ("role", "seq"), None),
        P("ctx", ("role", "seq")),
        P("groups", ("role", "seq")),
        P(("role", "seq")),
        P(("role", "seq"), "ctx"),
        P(("role", "seq"), "ctx"),
        P("ctx", ("role", "seq")),
    )
    sizes = (mesh.shape["ctx"], mesh.shape["role"], mesh.shape["seq"])
    return jax.shard_map(
        functools.partial(per_device, sizes),
        mesh=mesh,
        in_specs=placed,
        out_specs=P(("groups", "ctx"), ("role", "seq")),
        check_vma=False,
    )
```

```python
import functools

import jax
import jax.numpy as jnp
from jax import lax
from jax.experimental import pallas as pl
from jax.experimental.pallas import tpu as pltpu
from jax.sharding import PartitionSpec as P

D = 7168
LATENT = 512
MTP = 2

softmax_scale = 0.07216878364870323
epsilon = 1e-06
MESH = pl.DeviceIdType.MESH
VMEM_BYTES = 60 * 1024 * 1024
f32, bf16 = jnp.float32, jnp.bfloat16


def ctx_group(n):
    me = lax.axis_index("ctx")

    def peer(d):
        k = lax.rem(me + d, n)
        return k, {"ctx": k}

    return me, peer


def feature_group(n_role, n_seq):
    n = n_role * n_seq
    me = lax.axis_index("role") * n_seq + lax.axis_index("seq")

    def peer(d):
        k = lax.rem(me + d, n)
        return k, {"role": k // n_seq, "seq": lax.rem(k, n_seq)}

    return me, peer


def enter(groups):
    barrier = pltpu.get_barrier_semaphore()
    count = 0
    for n, peer in groups:
        for d in range(1, n):
            pl.semaphore_signal(barrier, inc=1, device_id=peer(d)[1], device_id_type=MESH)
            count += 1
    pl.semaphore_wait(barrier, count)


def remote(src, dst, send, recv, device):
    return pltpu.make_async_remote_copy(
        src_ref=src, dst_ref=dst, send_sem=send, recv_sem=recv,
        device_id=device, device_id_type=MESH,
    )


def attend(n, n_role, n_seq, q_ref, cache_ref, cache_copy, len_ref, pos_ref, out_ref,
           q_all, o_send, o_recv, s_send, s_recv, a_send, sems):
    nr = n_role * n_seq
    me, peer = ctx_group(n)
    fme, fpeer = feature_group(n_role, n_seq)
    seqs, _, context = cache_ref.shape
    rows = q_ref.shape[1]
    heads = rows // MTP

    q_copies = []
    for s in range(seqs):
        for d in range(1, n):
            c = remote(q_ref.at[s], q_all.at[me, s], sems.at[s, d], sems.at[seqs + s, d],
                       peer(d)[1])
            c.start()
            q_copies.append(c)

    places = me * context + lax.broadcasted_iota(jnp.int32, (rows, context), 1)
    first = lax.broadcasted_iota(jnp.int32, (rows, context), 0) < heads
    lives = []
    for s in range(seqs):
        limit = jnp.where(first, pos_ref[MTP * s], pos_ref[MTP * s + 1])
        lives.append((places < len_ref[s]) & (places <= limit))

    lane = lax.broadcasted_iota(jnp.int32, (rows, 128), 1)

    def block(q, s):
        keys = cache_ref[s]
        scores = jnp.dot(q, keys, preferred_element_type=f32) * softmax_scale
        live = lives[s]
        top = jnp.max(jnp.where(live, scores, -1e30), axis=1, keepdims=True)
        probs = jnp.exp(jnp.where(live, scores - top, -1e30)).astype(bf16)
        total = jnp.sum(probs.astype(f32), axis=1, keepdims=True)
        out = lax.dot_general(
            probs, keys[:LATENT], (((1,), (1,)), ((), ())), preferred_element_type=f32)
        return out, top, total

    cache_copy.wait()
    own = [block(q_ref[s], s) for s in range(seqs)]
    o_copies, s_copies = {}, {}
    for s in range(seqs):
        for d in range(1, n):
            src, device = peer(n - d)
            remote(q_ref.at[s], q_all.at[src, s], sems.at[s, d], sems.at[seqs + s, d],
                   device).wait_recv()
            o, top, total = block(q_all[src, s], s)
            o_send[d, s] = o.astype(bf16)
            s_send[d, s] = jnp.where(lane == 0, top, total).T[0:8]
            c = remote(o_send.at[d, s], o_recv.at[d, s], sems.at[2 * seqs + s, d],
                       sems.at[3 * seqs + s, d], device)
            c.start()
            o_copies[s, d] = c
            c = remote(s_send.at[d, s], s_recv.at[d, s], sems.at[4 * seqs + s, d],
                       sems.at[5 * seqs + s, d], device)
            c.start()
            s_copies[s, d] = c
    for c in q_copies:
        c.wait_send()

    heads = rows // MTP
    merged = []
    for s in range(seqs):
        own_o, top, total = own[s]
        tops, totals = [top], [total]
        for d in range(1, n):
            s_copies[s, d].wait()
            back = jnp.concatenate([s_recv[d, s]] * 16, axis=0).T
            tops.append(back[:, 0:1])
            totals.append(back[:, 1:2])
        highest = functools.reduce(jnp.maximum, tops)
        factors = [jnp.exp(t - highest) for t in tops]
        denom = sum(f * t for f, t in zip(factors, totals))
        numer = factors[0] * own_o
        for d in range(1, n):
            o_copies[s, d].wait()
            numer = numer + factors[d] * o_recv[d, s].astype(f32)
        merged.append((numer / denom).astype(bf16))

    part = LATENT // nr
    for k in range(nr):
        for r in range(seqs * MTP):
            t = r % MTP
            a_send[k, r] = merged[r // MTP][t * heads:(t + 1) * heads, k * part:(k + 1) * part]
    copies = []
    for d in range(1, nr):
        k, device = fpeer(d)
        c = remote(a_send.at[k], out_ref.at[fme], sems.at[6 * seqs, d], sems.at[7 * seqs, d], device)
        c.start()
        copies.append(c)
    out_ref[fme] = a_send[fme]
    for d in range(1, nr):
        k, device = fpeer(nr - d)
        copies[d - 1].wait_send()
        remote(a_send.at[k], out_ref.at[k], sems.at[6 * seqs, d], sems.at[7 * seqs, d],
               device).wait_recv()


def layer_kernel(n, n_role, n_seq, q_ref, cache_hbm, len_ref, pos_ref, vu_hbm, res_ref, gain_ref,
                 wo_hbm, wg_hbm, wu_hbm, wd_hbm,
                 out_ref, cache, vu, q_all, o_send, o_recv, s_send, s_recv, a_send, a_all, a_head,
                 mixed, pv_ref, wo, wg, wu, wd, pv_recv, v_send, v_all, v_full, acc, po_send,
                 po_recv, resid, xg_ref, g_acc, u_acc, gu_send, gu_recv, ss_send, ss_recv, h_send,
                 h_all, h_full, dn, dn_send, dn_recv, wsem, lsem, asems, sems):
    nr = n_role * n_seq
    me, peer = ctx_group(n)
    fme, fpeer = feature_group(n_role, n_seq)

    cache_copy = pltpu.make_async_copy(cache_hbm, cache, lsem.at[0])
    cache_copy.start()
    vu_copy = pltpu.make_async_copy(vu_hbm, vu, lsem.at[1])
    vu_copy.start()
    weights = []
    for which, (hbm, vmem) in enumerate(((wo_hbm, wo), (wg_hbm, wg), (wu_hbm, wu), (wd_hbm, wd))):
        depth = vmem.shape[1]

        def fetch(i, hbm=hbm, vmem=vmem, depth=depth, which=which):
            return pltpu.make_async_copy(
                hbm.at[pl.ds(i * depth, depth)], vmem.at[i], wsem.at[which, i])

        weights.append((fetch, vmem))
    for fetch, vmem in weights:
        for i in range(vmem.shape[0]):
            fetch(i).start()
    enter(((n, peer), (nr, fpeer)))
    attend(n, n_role, n_seq, q_ref, cache, cache_copy, len_ref, pos_ref, a_all,
           q_all, o_send, o_recv, s_send, s_recv, a_send, asems)
    rows, heads = a_all.shape[1:3]
    for j in range(nr):
        for r in range(rows):
            a_head[:, j * rows + r, :] = a_all[j, r].astype(f32)
    vu_copy.wait()
    vdim = vu.shape[2]
    for h in range(heads):
        mixed[:, h * vdim:(h + 1) * vdim] = jnp.dot(
            a_head[h].astype(bf16), vu[h], preferred_element_type=f32)
    for k in range(nr):
        pv_ref[k] = mixed[k * rows:(k + 1) * rows, :].astype(bf16)

    def matmul(x_ref, *pairs):
        chunks, depth, _ = weights[pairs[0][0]][1].shape
        for which, acc_ref in pairs:
            fetch, vmem = weights[which]
            fetch(0).wait()
            acc_ref[...] = jnp.dot(x_ref[:, :depth], vmem[0], preferred_element_type=f32)
        if chunks == 1:
            return

        @pl.loop(1, chunks)
        def _(i):
            x = x_ref[:, pl.ds(pl.multiple_of(i * depth, depth), depth)]
            for which, acc_ref in pairs:
                fetch, vmem = weights[which]
                fetch(i).wait()
                acc_ref[...] += jnp.dot(x, vmem[i], preferred_element_type=f32)

    def swap(size, peer_of, chunk, recv, row):
        copies = []
        for d in range(1, size):
            k, device = peer_of(d)
            c = remote(chunk(k), recv.at[d], sems.at[row, d], sems.at[row + 1, d], device)
            c.start()
            copies.append(c)
        return copies

    def gather(size, my, peer_of, send, full, row):
        copies = []
        for d in range(1, size):
            c = remote(send, full.at[my], sems.at[row, d], sems.at[row + 1, d], peer_of(d)[1])
            c.start()
            copies.append(c)
        full[my] = send[...]
        for d in range(1, size):
            k, device = peer_of(size - d)
            copies[d - 1].wait_send()
            remote(send, full.at[k], sems.at[row, d], sems.at[row + 1, d], device).wait_recv()

    part = res_ref.shape[0] // nr
    copies = swap(nr, fpeer, lambda k: pv_ref.at[k], pv_recv, 0)
    vals = pv_ref[fme].astype(f32)
    for d in range(1, nr):
        copies[d - 1].wait()
        vals = vals + pv_recv[d].astype(f32)
    v_send[...] = vals.astype(bf16)
    gather(nr, fme, fpeer, v_send, v_all, 2)
    for k in range(nr):
        acc_rows = v_all[k].astype(f32)
        v_full[k * part:(k + 1) * part, :] = acc_rows
    x_ref = xg_ref[0]
    x_ref[...] = v_full[...].astype(bf16)
    matmul(x_ref, (0, acc))

    po_send[...] = acc[...].astype(bf16)
    copies = swap(n, peer, lambda k: po_send, po_recv, 4)
    total = res_ref[...].astype(f32) + acc[...]
    for d in range(1, n):
        copies[d - 1].wait()
        total = total + po_recv[d].astype(f32)
    crows = res_ref.shape[0] // n
    for k in range(n):
        resid[k] = total[k * crows:(k + 1) * crows]
    sumsq = jnp.sum(total * total, axis=1, keepdims=True)
    sumsq = jnp.broadcast_to(sumsq, (total.shape[0], 128))
    for k in range(nr):
        ss_send[k] = sumsq[k * part:(k + 1) * part]
    s_copies = swap(nr, fpeer, lambda k: ss_send.at[k], ss_recv, 6)
    x_ref = xg_ref[1]
    x_ref[...] = (total * gain_ref[...]).astype(bf16)
    matmul(x_ref, (1, g_acc), (2, u_acc))

    for j, a in enumerate((g_acc, u_acc)):
        for k in range(nr):
            gu_send[k, j] = a[k * part:(k + 1) * part, :].astype(bf16)
    copies = swap(nr, fpeer, lambda k: gu_send.at[k], gu_recv, 8)
    ss = ss_send[fme]
    for d in range(1, nr):
        s_copies[d - 1].wait()
        ss = ss + ss_recv[d]
    inv = lax.rsqrt(ss[:, 0:1] / D + epsilon)
    gate = gu_send[fme, 0].astype(f32)
    up = gu_send[fme, 1].astype(f32)
    for d in range(1, nr):
        copies[d - 1].wait()
        gate = gate + gu_recv[d, 0].astype(f32)
        up = up + gu_recv[d, 1].astype(f32)
    gate = gate * inv
    up = up * inv
    h_send[...] = (gate / (1.0 + jnp.exp(-gate)) * up).astype(bf16)
    gather(nr, fme, fpeer, h_send, h_all, 10)
    for k in range(nr):
        h_full[k * part:(k + 1) * part, :] = h_all[k].astype(f32)
    x_ref = xg_ref[2]
    x_ref[...] = h_full[...].astype(bf16)
    matmul(x_ref, (3, acc))

    for k in range(n):
        piece = acc[k * crows:(k + 1) * crows, :]
        dn[k] = piece
        dn_send[k] = piece.astype(bf16)
    copies = swap(n, peer, lambda k: dn_send.at[k], dn_recv, 12)
    result = resid[me] + dn[me]
    for d in range(1, n):
        copies[d - 1].wait()
        result = result + dn_recv[d].astype(f32)
    out_ref[...] = result.astype(bf16)


def chunk_of(depth):
    for size in (1024, 768, 512, 256):
        if depth % size == 0:
            return size
    return depth


def per_device_latents(sizes, queries, cache, lengths, positions, value_up_weight, out_proj, residual,
               norm_gain, gate_weight, up_weight, down_weight):
    n, n_role, n_seq = sizes
    nr = n_role * n_seq
    rows, heads, width = queries.shape
    seqs = cache.shape[0]
    span = rows * heads // seqs
    lat = LATENT // nr
    vmem = pl.BlockSpec(memory_space=pltpu.VMEM)
    smem = pl.BlockSpec(memory_space=pltpu.SMEM)
    hbm = pl.BlockSpec(memory_space=pl.ANY)
    most = max(n, nr)
    sems = lambda k: pltpu.SemaphoreType.DMA((k, most))
    vwide = heads * value_up_weight.shape[2]
    all_rows, dd = residual.shape
    ff = gate_weight.shape[1]
    part, crows = all_rows // nr, all_rows // n

    def held(w):
        size = chunk_of(w.shape[0])
        return pltpu.VMEM((w.shape[0] // size, size, w.shape[1]), bf16)

    ws = (out_proj, gate_weight, up_weight, down_weight)
    most_chunks = max(w.shape[0] // chunk_of(w.shape[0]) for w in ws)
    V = pltpu.VMEM
    return pl.pallas_call(
        functools.partial(layer_kernel, n, n_role, n_seq),
        out_shape=jax.ShapeDtypeStruct((crows, dd), bf16),
        in_specs=[vmem, hbm, smem, smem, hbm, vmem, vmem] + [hbm] * 4,
        out_specs=vmem,
        scratch_shapes=[
            V((cache.shape[0], width, cache.shape[1]), bf16),
            V(value_up_weight.shape, bf16),
            V((n, seqs, span, width), bf16),
            V((n, seqs, span, LATENT), bf16),
            V((n, seqs, span, LATENT), bf16),
            V((n, seqs, 8, span), f32),
            V((n, seqs, 8, span), f32),
            V((nr, rows, heads, lat), bf16),
            V((nr, rows, heads, lat), bf16),
            V((heads, all_rows, lat), f32),
            V((all_rows, vwide), f32),
            V((nr, part, vwide), bf16),
            *[held(w) for w in ws],
            V((nr, part, vwide), bf16),
            V((part, vwide), bf16),
            V((nr, part, vwide), bf16),
            V((all_rows, vwide), f32),
            V((all_rows, dd), f32),
            V((all_rows, dd), bf16),
            V((n, all_rows, dd), bf16),
            V((n, crows, dd), f32),
            [V((all_rows, vwide), bf16), V((all_rows, dd), bf16), V((all_rows, ff), bf16)],
            V((all_rows, ff), f32),
            V((all_rows, ff), f32),
            V((nr, 2, part, ff), bf16),
            V((nr, 2, part, ff), bf16),
            V((nr, part, 128), f32),
            V((nr, part, 128), f32),
            V((part, ff), bf16),
            V((nr, part, ff), bf16),
            V((all_rows, ff), f32),
            V((n, crows, dd), f32),
            V((n, crows, dd), bf16),
            V((n, crows, dd), bf16),
            pltpu.SemaphoreType.DMA((4, most_chunks)),
            pltpu.SemaphoreType.DMA((2,)),
            sems(8 * seqs),
            sems(14),
        ],
        compiler_params=pltpu.CompilerParams(
            collective_id=0, has_side_effects=True, vmem_limit_bytes=VMEM_BYTES),
        name="layer",
    )(queries.reshape(seqs, span, width), cache.transpose(0, 2, 1), lengths, positions, value_up_weight,
      residual, norm_gain.reshape(1, dd), *ws)


LOG2E = 1.4426950408889634


def by_distance(n, me):
    found = []
    for i in range(n - 1):
        k = jnp.int32(0)
        for z in range(n):
            others = sorted((j for j in range(n) if j != z), key=lambda j: (abs(j - z), j))
            k = jnp.where(me == z, others[i], k)
        found.append(k)
    return found


def cut(width):
    unit = 256 if width % 256 == 0 else 128
    if width % unit or width < 2 * unit:
        return [(0, width)]
    first = -(-(width // unit) // 2) * unit
    return [(0, first), (first, width)]


def heads_kernel(n, n_role, n_seq, q_hbm, cache_hbm, len_ref, pos_ref, vu_hbm, res_hbm, gain_hbm,
                 wo_hbm, wg_hbm, wu_hbm, wd_hbm, out_ref,
                 q_ref, cache, vu, res_ref, gain_ref, wo, wg, wu, wd,
                 qn_send, qr_send, qn_all, qr_all, o_send, o_recv, st_send, st_recv, w_ref,
                 a_head, v_send, xv, acc, po_send, po_recv, resid, ss_send, ss_recv,
                 g_acc, u_acc, gu_send, gu_recv, h_send, h_all, h_full, dn, dn_send, dn_recv,
                 lsem, wsem, qsem, vusem, osem, ssem, vsem, posem, sssem, gusem, hsem, dnsem):
    nr = n_role * n_seq
    me = lax.axis_index("ctx")
    role, seq = lax.axis_index("role"), lax.axis_index("seq")
    fme = role * n_seq + seq
    near = by_distance(n, me)
    mates = []
    for dr in range(n_role):
        for ds in range(n_seq):
            if dr or ds:
                r, s = lax.rem(role + dr, n_role), lax.rem(seq + ds, n_seq)
                mates.append((r * n_seq + s, {"role": r, "seq": s}))
    seqs, span, width = q_ref.shape
    context = cache.shape[2]
    heads = span // MTP
    hk = heads // nr
    rope = width - LATENT
    lat = LATENT // nr
    own = n - 1

    q_copy = pltpu.make_async_copy(q_hbm, q_ref, lsem.at[0])
    q_copy.start()
    cache_copies = [
        pltpu.make_async_copy(cache_hbm, cache.at[:, pl.ds(0, width), :], lsem.at[1]),
        pltpu.make_async_copy(cache_hbm.at[:, pl.ds(LATENT, rope), :],
                              cache.at[:, pl.ds(width, rope), :], lsem.at[2]),
    ]
    for c in cache_copies:
        c.start()
    barrier = pltpu.get_barrier_semaphore()
    for k in near:
        pl.semaphore_signal(barrier, inc=1, device_id={"ctx": k}, device_id_type=MESH)
    for _, device in mates:
        pl.semaphore_signal(barrier, inc=1, device_id=device, device_id_type=MESH)
    vu_own = pltpu.make_async_copy(
        vu_hbm.at[pl.ds(pl.multiple_of(fme * hk, hk), hk)],
        vu.at[:, pl.ds(pl.multiple_of(fme * lat, lat), lat), :], lsem.at[3])
    vu_own.start()
    res_copy = pltpu.make_async_copy(res_hbm, res_ref, lsem.at[4])
    res_copy.start()
    gain_copy = pltpu.make_async_copy(gain_hbm, gain_ref.at[0], lsem.at[5])
    gain_copy.start()

    q_copy.wait()
    for s in range(seqs):
        qn, qr = [], []
        for k in range(nr):
            for t in range(MTP):
                at = t * heads + k * hk
                rows = q_ref[s, at:at + hk, :].astype(f32)
                qn.append(rows[:, :LATENT])
                qr.append(rows[:, LATENT:])
        qn_send[s] = jnp.concatenate(qn, axis=0).astype(bf16)
        qr = jnp.concatenate(qr, axis=0)
        qr_send[s] = jnp.concatenate([qr[:span // 2], qr[span // 2:]], axis=1).astype(bf16)
    weights = []
    for which, (hbm, vmem) in enumerate(((wo_hbm, wo), (wg_hbm, wg), (wu_hbm, wu), (wd_hbm, wd))):
        weights.append(pltpu.make_async_copy(hbm, vmem, wsem.at[which]))
    for c in weights:
        c.start()
    pl.semaphore_wait(barrier, len(near) + len(mates))

    sent = []

    def send(src, dst, send_sem, recv_sem, device):
        c = remote(src, dst, send_sem, recv_sem, device)
        c.start()
        sent.append(c)

    passed = []

    def drain():
        for c in sent:
            c.wait_send()
        sent.clear()
        if passed:
            @pl.when(inner == 1)
            def _():
                for b, s in passed:
                    for r, ref in ((0, qn_send), (2, qr_send)):
                        remote(ref.at[s], ref.at[s], qsem.at[r, s, b, beside],
                               qsem.at[r + 1, s, b, 0], {"ctx": beside}).wait_send()
            passed.clear()

    def pass_on(b, s, k, source):
        qn, qr = (qn_send.at[s], qr_send.at[s]) if source is None else (qn_all.at[b, s], qr_all.at[b, s])
        given = [
            remote(qn, qn_all.at[b, s], qsem.at[0, s, b, k], qsem.at[1, s, b, 0], {"ctx": k}),
            remote(qr, qr_all.at[b, s], qsem.at[2, s, b, k], qsem.at[3, s, b, 0], {"ctx": k}),
        ]
        for c in given:
            c.start()
        return given

    def take(b, s):
        remote(qn_send.at[s], qn_all.at[b, s], qsem.at[0, s, b, b], qsem.at[1, s, b, 0],
               {"ctx": b}).wait_recv()
        remote(qr_send.at[s], qr_all.at[b, s], qsem.at[2, s, b, b], qsem.at[3, s, b, 0],
               {"ctx": b}).wait_recv()

    paired = n == 4
    if paired:
        beside = me + 1 - 2 * lax.rem(me, 2)
        across = 2 - me // 2
        beyond = 3 - 3 * (me // 2)
        inner = lax.rem((me + 1) // 2, 2)
        reach = [beside, across]
    else:
        reach = near[::-1]
    for s in range(seqs):
        for k in reach:
            sent.extend(pass_on(me, s, k, None))
    for k, device in mates:
        send(vu_hbm.at[pl.ds(pl.multiple_of(k * hk, hk), hk)],
             vu.at[:, pl.ds(pl.multiple_of(fme * lat, lat), lat), :],
             vusem.at[0, k], vusem.at[1, fme], device)

    column = lax.broadcasted_iota(jnp.int32, (span, context), 1)
    row = lax.broadcasted_iota(jnp.int32, (span, 1), 0)
    even = lax.rem(row, MTP * hk) < hk
    lane = lax.broadcasted_iota(jnp.int32, (span, 128), 1)
    half = lax.broadcasted_iota(jnp.int32, (span // 2, 2 * rope), 1) < rope
    ends = []
    for s in range(seqs):
        limit = jnp.where(even, pos_ref[MTP * s], pos_ref[MTP * s + 1]) + 1
        ends.append(jnp.minimum(limit, len_ref[s]) - me * context)

    def block(qn, qr, s, slot):
        zero = jnp.zeros_like(qr)
        q = jnp.concatenate(
            [qn, jnp.concatenate([jnp.where(half, qr, zero), jnp.where(half, zero, qr)], axis=0)],
            axis=1)
        keys = cache[s]
        scores = jnp.dot(q, keys, preferred_element_type=f32) * (softmax_scale * LOG2E)
        scores = jnp.where(column < ends[s], scores, -1e30)
        top = jnp.maximum(jnp.max(scores, axis=1, keepdims=True), -1e29)
        probs = jnp.exp2(scores - top).astype(bf16)
        total = jnp.sum(probs.astype(f32), axis=1, keepdims=True)
        out = lax.dot_general(
            probs, keys[:LATENT], (((1,), (1,)), ((), ())), preferred_element_type=f32)
        out = out.astype(bf16)
        for k in range(nr):
            o_send[slot, s, k] = out[k * MTP * hk:(k + 1) * MTP * hk]
        stats = jnp.where(lane == 0, top, total).T
        st_send[slot, s] = jnp.concatenate([stats[0:1], stats[1:2]], axis=1)

    mine = me * nr + fme
    for c in cache_copies:
        c.wait()
    home = []
    for s in range(seqs):
        block(qn_send[s], qr_send[s], s, own)
        for k, device in mates:
            send(o_send.at[own, s, k], o_recv.at[mine, s], osem.at[0, s, own, k],
                 osem.at[1, s, me, fme], device)
            send(st_send.at[own, s], st_recv.at[mine, s], ssem.at[0, s, own, k],
                 ssem.at[1, s, me, fme], device)
        for c in (
            pltpu.make_async_copy(o_send.at[own, s, fme], o_recv.at[mine, s], osem.at[1, s, me, fme]),
            pltpu.make_async_copy(st_send.at[own, s], st_recv.at[mine, s], ssem.at[1, s, me, fme]),
        ):
            c.start()

    def answer(b, s, slot):
        block(qn_all[b, s], qr_all[b, s], s, slot)
        for k in range(nr):
            device = {"ctx": b, "role": k // n_seq, "seq": k % n_seq}
            send(o_send.at[slot, s, k], o_recv.at[mine, s], osem.at[0, s, slot, k],
                 osem.at[1, s, me, fme], device)
            send(st_send.at[slot, s], st_recv.at[mine, s], ssem.at[0, s, slot, k],
                 ssem.at[1, s, me, fme], device)

    if paired:
        def relay(b, s):
            @pl.when(inner == 1)
            def _():
                take(b, s)
                pass_on(b, s, beside, b)

            passed.append((b, s))

        def take_outer(b, s):
            @pl.when(inner == 0)
            def _():
                take(b, s)

        relay(across, 0)
        for s in range(seqs):
            take(beside, s)
            answer(beside, s, 0)
            if s == 0:
                relay(beyond, 0)
            take_outer(across, s)
            answer(across, s, 1)
            if s + 1 < seqs:
                relay(across, s + 1)
            take_outer(beyond, s)
            answer(beyond, s, 2)
            if s + 1 < seqs:
                relay(beyond, s + 1)
    else:
        for s in range(seqs):
            for i, b in enumerate(near):
                take(b, s)
                answer(b, s, i)

    rows = seqs * MTP
    all_rows = nr * rows
    mine_at = pl.ds(pl.multiple_of(fme * MTP * hk, MTP * hk), MTP * hk)
    first = {"ctx": near[0]}
    for s in range(seqs):
        tops, totals = [], []
        for b in range(n):
            for j in range(nr):
                remote(st_send.at[0, s], st_recv.at[b * nr + j, s], ssem.at[0, s, 0, 0],
                       ssem.at[1, s, b, j], first).wait_recv()
            stats = [st_recv[b * nr + j, s] for j in range(nr)]
            stats = jnp.concatenate(stats, axis=0)
            tops.append(stats[:, :span])
            totals.append(stats[:, span:])
        highest = functools.reduce(jnp.maximum, tops)
        factors = [jnp.exp2(t - highest) for t in tops]
        denom = sum(f * t for f, t in zip(factors, totals))
        shares = jnp.concatenate([f / denom for f in factors], axis=0)
        copies = -(-128 // (n * nr))
        shares = jnp.concatenate([shares] * copies, axis=0)[:128]
        w_ref[s] = shares.T
        share = w_ref[s, mine_at, :]
        for j in range(nr):
            mixed = None
            for b in range(n):
                i = b * nr + j
                remote(o_send.at[0, s, 0], o_recv.at[i, s], osem.at[0, s, 0, 0],
                       osem.at[1, s, b, j], first).wait_recv()
                term = share[:, i:i + 1] * o_recv[i, s].astype(f32)
                mixed = term if mixed is None else mixed + term
            for t in range(MTP):
                a_head[:, j * rows + s * MTP + t, :] = mixed[t * hk:(t + 1) * hk]

    vu_own.wait()
    for k, device in mates:
        remote(vu_hbm.at[pl.ds(0, hk)], vu.at[:, pl.ds(pl.multiple_of(k * lat, lat), lat), :],
               vusem.at[0, k], vusem.at[1, k], device).wait_recv()
    vdim = vu.shape[2]
    for h in range(hk):
        v_send[:, h * vdim:(h + 1) * vdim] = jnp.dot(
            a_head[h].astype(bf16), vu[h], preferred_element_type=f32).astype(bf16)
    for k, device in mates:
        send(v_send, xv.at[fme], vsem.at[0, k], vsem.at[1, fme], device)
    weights[0].wait()
    deep = hk * vdim

    def wo_rows(k):
        return pl.ds(pl.multiple_of(k * deep, deep), deep)

    acc[...] = jnp.dot(v_send[...], wo[wo_rows(fme), :], preferred_element_type=f32)

    def arrived(k, device):
        remote(v_send, xv.at[k], vsem.at[0, k], vsem.at[1, k], device).wait_recv()

    early, late = mates[:n_seq - 1], mates[n_seq - 1:]
    for k, device in early:
        arrived(k, device)
        acc[...] += jnp.dot(xv[k], wo[wo_rows(k), :], preferred_element_type=f32)
    for k, device in late:
        arrived(k, device)
    dd = acc.shape[1]
    parts = cut(dd)
    for p, (c0, c1) in enumerate(parts):
        total = acc[:, c0:c1]
        for k, device in late:
            total = total + jnp.dot(xv[k], wo[wo_rows(k), c0:c1], preferred_element_type=f32)
        acc[:, c0:c1] = total
        po_send[:, c0:c1] = total.astype(bf16)
        for k in near[::-1]:
            send(po_send.at[:, c0:c1], po_recv.at[me, :, c0:c1], posem.at[0, p, k],
                 posem.at[1, p, me], {"ctx": k})
    drain()
    res_copy.wait()
    gain_copy.wait()
    weights[1].wait()
    weights[2].wait()

    part, crows = all_rows // nr, all_rows // n
    ff = g_acc.shape[1]
    fparts = [(f, min(f + 768, ff)) for f in range(0, ff, 768)]
    sumsq = jnp.zeros((all_rows, 1), f32)
    for p, (c0, c1) in enumerate(parts):
        total = res_ref[:, c0:c1].astype(f32) + acc[:, c0:c1]
        for k in near:
            remote(po_send.at[:, c0:c1], po_recv.at[k, :, c0:c1], posem.at[0, p, k],
                   posem.at[1, p, k], {"ctx": k}).wait_recv()
            total = total + po_recv[k, :, c0:c1].astype(f32)
        for k in range(n):
            resid[k, :, c0:c1] = total[k * crows:(k + 1) * crows]
        sumsq = sumsq + jnp.sum(total * total, axis=1, keepdims=True)
        x = (total * gain_ref[:, c0:c1]).astype(bf16)
        last = p == len(parts) - 1
        if last:
            wide = jnp.broadcast_to(sumsq, (all_rows, 128))
            for k in range(nr):
                ss_send[k] = wide[k * part:(k + 1) * part]
            for k, device in mates:
                send(ss_send.at[k], ss_recv.at[fme], sssem.at[0, k], sssem.at[1, fme], device)
        for q, (f0, f1) in enumerate(fparts if last else [(0, ff)]):
            for j, (w, a) in enumerate(((wg, g_acc), (wu, u_acc))):
                y = jnp.dot(x, w[c0:c1, f0:f1], preferred_element_type=f32)
                if p:
                    y = y + a[:, f0:f1]
                if not last:
                    a[:, f0:f1] = y
                    continue
                for k in range(nr):
                    gu_send[k, j, :, f0:f1] = y[k * part:(k + 1) * part].astype(bf16)
            if last:
                for k, device in mates:
                    send(gu_send.at[k, :, :, f0:f1], gu_recv.at[fme, :, :, f0:f1],
                         gusem.at[0, q, k], gusem.at[1, q, fme], device)
    ss = ss_send[fme]
    for k, device in mates:
        remote(ss_send.at[k], ss_recv.at[k], sssem.at[0, k], sssem.at[1, k], device).wait_recv()
        ss = ss + ss_recv[k]
    inv = lax.rsqrt(ss[:, 0:1] / D + epsilon)
    for q, (f0, f1) in enumerate(fparts):
        gate = gu_send[fme, 0, :, f0:f1].astype(f32)
        up = gu_send[fme, 1, :, f0:f1].astype(f32)
        for k, device in mates:
            remote(gu_send.at[k, :, :, f0:f1], gu_recv.at[k, :, :, f0:f1], gusem.at[0, q, k],
                   gusem.at[1, q, k], device).wait_recv()
            gate = gate + gu_recv[k, 0, :, f0:f1].astype(f32)
            up = up + gu_recv[k, 1, :, f0:f1].astype(f32)
        gate = gate * inv
        up = up * inv
        h = (gate / (1.0 + jnp.exp(-gate)) * up).astype(bf16)
        h_send[:, f0:f1] = h
        h_all[fme, :, f0:f1] = h
        for k, device in mates:
            send(h_send.at[:, f0:f1], h_all.at[fme, :, f0:f1], hsem.at[0, q, k],
                 hsem.at[1, q, fme], device)
    weights[3].wait()
    for q, (f0, f1) in enumerate(fparts):
        for k, device in mates:
            remote(h_send.at[:, f0:f1], h_all.at[k, :, f0:f1], hsem.at[0, q, k],
                   hsem.at[1, q, k], device).wait_recv()
        for k in range(nr):
            h_full[k * part:(k + 1) * part, f0:f1] = h_all[k, :, f0:f1].astype(f32)
        x = h_full[:, f0:f1].astype(bf16)
        last = q == len(fparts) - 1
        for p, (c0, c1) in enumerate(parts if last else [(0, dd)]):
            y = jnp.dot(x, wd[f0:f1, c0:c1], preferred_element_type=f32)
            if q:
                y = y + acc[:, c0:c1]
            if not last:
                acc[:, c0:c1] = y
                continue
            for k in range(n):
                piece = y[k * crows:(k + 1) * crows]
                dn[k, :, c0:c1] = piece
                dn_send[k, :, c0:c1] = piece.astype(bf16)
            for k in near[::-1]:
                send(dn_send.at[k, :, c0:c1], dn_recv.at[me, :, c0:c1], dnsem.at[0, p, k],
                     dnsem.at[1, p, me], {"ctx": k})
    drain()
    for p, (c0, c1) in enumerate(parts):
        result = resid[me, :, c0:c1] + dn[me, :, c0:c1]
        for k in near:
            remote(dn_send.at[k, :, c0:c1], dn_recv.at[k, :, c0:c1], dnsem.at[0, p, k],
                   dnsem.at[1, p, k], {"ctx": k}).wait_recv()
            result = result + dn_recv[k, :, c0:c1].astype(f32)
        out_ref[:, c0:c1] = result.astype(bf16)


def per_device(sizes, queries, cache, lengths, positions, value_up_weight, out_proj, residual,
               norm_gain, gate_weight, up_weight, down_weight):
    n, n_role, n_seq = sizes
    nr = n_role * n_seq
    rows, heads, width = queries.shape
    seqs, context = cache.shape[:2]
    rope = width - LATENT
    if heads % (8 * nr) or 2 * rope != 128 or n < 2 or nr < 2:
        return per_device_latents(
            sizes, queries, cache, lengths, positions, value_up_weight, out_proj, residual,
            norm_gain, gate_weight, up_weight, down_weight)
    hk = heads // nr
    span = rows * heads // seqs
    vdim = value_up_weight.shape[2]
    all_rows, dd = residual.shape
    ff = gate_weight.shape[1]
    part, crows = all_rows // nr, all_rows // n
    nf = -(-ff // 768)
    vmem = pl.BlockSpec(memory_space=pltpu.VMEM)
    smem = pl.BlockSpec(memory_space=pltpu.SMEM)
    hbm = pl.BlockSpec(memory_space=pl.ANY)
    V = pltpu.VMEM
    sems = lambda *k: pltpu.SemaphoreType.DMA(k)
    return pl.pallas_call(
        functools.partial(heads_kernel, n, n_role, n_seq),
        out_shape=jax.ShapeDtypeStruct((crows, dd), bf16),
        in_specs=[hbm, hbm, smem, smem] + [hbm] * 7,
        out_specs=vmem,
        scratch_shapes=[
            V((seqs, span, width), bf16),
            V((seqs, width + rope, context), bf16),
            V((hk, LATENT, vdim), bf16),
            V((all_rows, dd), bf16),
            V((1, dd), f32),
            V(out_proj.shape, bf16),
            V(gate_weight.shape, bf16),
            V(up_weight.shape, bf16),
            V(down_weight.shape, bf16),
            V((seqs, span, LATENT), bf16),
            V((seqs, span // 2, 2 * rope), bf16),
            V((n, seqs, span, LATENT), bf16),
            V((n, seqs, span // 2, 2 * rope), bf16),
            V((n, seqs, nr, MTP * hk, LATENT), bf16),
            V((n * nr, seqs, MTP * hk, LATENT), bf16),
            V((n, seqs, 1, 2 * span), f32),
            V((n * nr, seqs, 1, 2 * span), f32),
            V((seqs, span, 128), f32),
            V((hk, all_rows, LATENT), f32),
            V((all_rows, hk * vdim), bf16),
            V((nr, all_rows, hk * vdim), bf16),
            V((all_rows, dd), f32),
            V((all_rows, dd), bf16),
            V((n, all_rows, dd), bf16),
            V((n, crows, dd), f32),
            V((nr, part, 128), f32),
            V((nr, part, 128), f32),
            V((all_rows, ff), f32),
            V((all_rows, ff), f32),
            V((nr, 2, part, ff), bf16),
            V((nr, 2, part, ff), bf16),
            V((part, ff), bf16),
            V((nr, part, ff), bf16),
            V((all_rows, ff), f32),
            V((n, crows, dd), f32),
            V((n, crows, dd), bf16),
            V((n, crows, dd), bf16),
            sems(6),
            sems(4),
            sems(4, seqs, n, n),
            sems(2, nr),
            sems(2, seqs, n, nr),
            sems(2, seqs, n, nr),
            sems(2, nr),
            sems(2, 2, n),
            sems(2, nr),
            sems(2, nf, nr),
            sems(2, nf, nr),
            sems(2, 2, n),
        ],
        compiler_params=pltpu.CompilerParams(
            collective_id=0, has_side_effects=True, vmem_limit_bytes=VMEM_BYTES),
        name="layer",
    )(queries.reshape(seqs, span, width), cache.transpose(0, 2, 1), lengths, positions, value_up_weight,
      residual, norm_gain, out_proj, gate_weight, up_weight, down_weight)


def solution(mesh):
    placed = (
        P(("groups", "role", "seq"), "ctx", None),
        P(("groups", "role", "seq"), "ctx", None),
        P(("groups", "role", "seq")),
        P(("groups", "role", "seq")),
        P("ctx", ("role", "seq"), None),
        P("ctx", ("role", "seq")),
        P("groups", ("role", "seq")),
        P(("role", "seq")),
        P(("role", "seq"), "ctx"),
        P(("role", "seq"), "ctx"),
        P("ctx", ("role", "seq")),
    )
    sizes = (mesh.shape["ctx"], mesh.shape["role"], mesh.shape["seq"])
    return jax.shard_map(
        functools.partial(per_device, sizes),
        mesh=mesh,
        in_specs=placed,
        out_specs=P(("groups", "ctx"), ("role", "seq")),
        check_vma=False,
    )
```

```python
import functools

import jax
import jax.numpy as jnp
from jax import lax
from jax.experimental import pallas as pl
from jax.experimental.pallas import tpu as pltpu
from jax.sharding import PartitionSpec as P

D = 7168
LATENT = 512
MTP = 2

softmax_scale = 0.07216878364870323
epsilon = 1e-06
MESH = pl.DeviceIdType.MESH
VMEM_BYTES = 60 * 1024 * 1024
f32, bf16 = jnp.float32, jnp.bfloat16


def ctx_group(n):
    me = lax.axis_index("ctx")

    def peer(d):
        k = lax.rem(me + d, n)
        return k, {"ctx": k}

    return me, peer


def feature_group(n_role, n_seq):
    n = n_role * n_seq
    me = lax.axis_index("role") * n_seq + lax.axis_index("seq")

    def peer(d):
        k = lax.rem(me + d, n)
        return k, {"role": k // n_seq, "seq": lax.rem(k, n_seq)}

    return me, peer


def enter(groups):
    barrier = pltpu.get_barrier_semaphore()
    count = 0
    for n, peer in groups:
        for d in range(1, n):
            pl.semaphore_signal(barrier, inc=1, device_id=peer(d)[1], device_id_type=MESH)
            count += 1
    pl.semaphore_wait(barrier, count)


def remote(src, dst, send, recv, device):
    return pltpu.make_async_remote_copy(
        src_ref=src, dst_ref=dst, send_sem=send, recv_sem=recv,
        device_id=device, device_id_type=MESH,
    )


def attend(n, n_role, n_seq, q_ref, cache_ref, cache_copy, len_ref, pos_ref, out_ref,
           q_all, o_send, o_recv, s_send, s_recv, a_send, sems):
    nr = n_role * n_seq
    me, peer = ctx_group(n)
    fme, fpeer = feature_group(n_role, n_seq)
    seqs, _, context = cache_ref.shape
    rows = q_ref.shape[1]
    heads = rows // MTP

    q_copies = []
    for s in range(seqs):
        for d in range(1, n):
            c = remote(q_ref.at[s], q_all.at[me, s], sems.at[s, d], sems.at[seqs + s, d],
                       peer(d)[1])
            c.start()
            q_copies.append(c)

    places = me * context + lax.broadcasted_iota(jnp.int32, (rows, context), 1)
    first = lax.broadcasted_iota(jnp.int32, (rows, context), 0) < heads
    lives = []
    for s in range(seqs):
        limit = jnp.where(first, pos_ref[MTP * s], pos_ref[MTP * s + 1])
        lives.append((places < len_ref[s]) & (places <= limit))

    lane = lax.broadcasted_iota(jnp.int32, (rows, 128), 1)

    def block(q, s):
        keys = cache_ref[s]
        scores = jnp.dot(q, keys, preferred_element_type=f32) * softmax_scale
        live = lives[s]
        top = jnp.max(jnp.where(live, scores, -1e30), axis=1, keepdims=True)
        probs = jnp.exp(jnp.where(live, scores - top, -1e30)).astype(bf16)
        total = jnp.sum(probs.astype(f32), axis=1, keepdims=True)
        out = lax.dot_general(
            probs, keys[:LATENT], (((1,), (1,)), ((), ())), preferred_element_type=f32)
        return out, top, total

    cache_copy.wait()
    own = [block(q_ref[s], s) for s in range(seqs)]
    o_copies, s_copies = {}, {}
    for s in range(seqs):
        for d in range(1, n):
            src, device = peer(n - d)
            remote(q_ref.at[s], q_all.at[src, s], sems.at[s, d], sems.at[seqs + s, d],
                   device).wait_recv()
            o, top, total = block(q_all[src, s], s)
            o_send[d, s] = o.astype(bf16)
            s_send[d, s] = jnp.where(lane == 0, top, total).T[0:8]
            c = remote(o_send.at[d, s], o_recv.at[d, s], sems.at[2 * seqs + s, d],
                       sems.at[3 * seqs + s, d], device)
            c.start()
            o_copies[s, d] = c
            c = remote(s_send.at[d, s], s_recv.at[d, s], sems.at[4 * seqs + s, d],
                       sems.at[5 * seqs + s, d], device)
            c.start()
            s_copies[s, d] = c
    for c in q_copies:
        c.wait_send()

    heads = rows // MTP
    merged = []
    for s in range(seqs):
        own_o, top, total = own[s]
        tops, totals = [top], [total]
        for d in range(1, n):
            s_copies[s, d].wait()
            back = jnp.concatenate([s_recv[d, s]] * 16, axis=0).T
            tops.append(back[:, 0:1])
            totals.append(back[:, 1:2])
        highest = functools.reduce(jnp.maximum, tops)
        factors = [jnp.exp(t - highest) for t in tops]
        denom = sum(f * t for f, t in zip(factors, totals))
        numer = factors[0] * own_o
        for d in range(1, n):
            o_copies[s, d].wait()
            numer = numer + factors[d] * o_recv[d, s].astype(f32)
        merged.append((numer / denom).astype(bf16))

    part = LATENT // nr
    for k in range(nr):
        for r in range(seqs * MTP):
            t = r % MTP
            a_send[k, r] = merged[r // MTP][t * heads:(t + 1) * heads, k * part:(k + 1) * part]
    copies = []
    for d in range(1, nr):
        k, device = fpeer(d)
        c = remote(a_send.at[k], out_ref.at[fme], sems.at[6 * seqs, d], sems.at[7 * seqs, d], device)
        c.start()
        copies.append(c)
    out_ref[fme] = a_send[fme]
    for d in range(1, nr):
        k, device = fpeer(nr - d)
        copies[d - 1].wait_send()
        remote(a_send.at[k], out_ref.at[k], sems.at[6 * seqs, d], sems.at[7 * seqs, d],
               device).wait_recv()


def layer_kernel(n, n_role, n_seq, q_ref, cache_hbm, len_ref, pos_ref, vu_hbm, res_ref, gain_ref,
                 wo_hbm, wg_hbm, wu_hbm, wd_hbm,
                 out_ref, cache, vu, q_all, o_send, o_recv, s_send, s_recv, a_send, a_all, a_head,
                 mixed, pv_ref, wo, wg, wu, wd, pv_recv, v_send, v_all, v_full, acc, po_send,
                 po_recv, resid, xg_ref, g_acc, u_acc, gu_send, gu_recv, ss_send, ss_recv, h_send,
                 h_all, h_full, dn, dn_send, dn_recv, wsem, lsem, asems, sems):
    nr = n_role * n_seq
    me, peer = ctx_group(n)
    fme, fpeer = feature_group(n_role, n_seq)

    cache_copy = pltpu.make_async_copy(cache_hbm, cache, lsem.at[0])
    cache_copy.start()
    vu_copy = pltpu.make_async_copy(vu_hbm, vu, lsem.at[1])
    vu_copy.start()
    weights = []
    for which, (hbm, vmem) in enumerate(((wo_hbm, wo), (wg_hbm, wg), (wu_hbm, wu), (wd_hbm, wd))):
        depth = vmem.shape[1]

        def fetch(i, hbm=hbm, vmem=vmem, depth=depth, which=which):
            return pltpu.make_async_copy(
                hbm.at[pl.ds(i * depth, depth)], vmem.at[i], wsem.at[which, i])

        weights.append((fetch, vmem))
    for fetch, vmem in weights:
        for i in range(vmem.shape[0]):
            fetch(i).start()
    enter(((n, peer), (nr, fpeer)))
    attend(n, n_role, n_seq, q_ref, cache, cache_copy, len_ref, pos_ref, a_all,
           q_all, o_send, o_recv, s_send, s_recv, a_send, asems)
    rows, heads = a_all.shape[1:3]
    for j in range(nr):
        for r in range(rows):
            a_head[:, j * rows + r, :] = a_all[j, r].astype(f32)
    vu_copy.wait()
    vdim = vu.shape[2]
    for h in range(heads):
        mixed[:, h * vdim:(h + 1) * vdim] = jnp.dot(
            a_head[h].astype(bf16), vu[h], preferred_element_type=f32)
    for k in range(nr):
        pv_ref[k] = mixed[k * rows:(k + 1) * rows, :].astype(bf16)

    def matmul(x_ref, *pairs):
        chunks, depth, _ = weights[pairs[0][0]][1].shape
        for which, acc_ref in pairs:
            fetch, vmem = weights[which]
            fetch(0).wait()
            acc_ref[...] = jnp.dot(x_ref[:, :depth], vmem[0], preferred_element_type=f32)
        if chunks == 1:
            return

        @pl.loop(1, chunks)
        def _(i):
            x = x_ref[:, pl.ds(pl.multiple_of(i * depth, depth), depth)]
            for which, acc_ref in pairs:
                fetch, vmem = weights[which]
                fetch(i).wait()
                acc_ref[...] += jnp.dot(x, vmem[i], preferred_element_type=f32)

    def swap(size, peer_of, chunk, recv, row):
        copies = []
        for d in range(1, size):
            k, device = peer_of(d)
            c = remote(chunk(k), recv.at[d], sems.at[row, d], sems.at[row + 1, d], device)
            c.start()
            copies.append(c)
        return copies

    def gather(size, my, peer_of, send, full, row):
        copies = []
        for d in range(1, size):
            c = remote(send, full.at[my], sems.at[row, d], sems.at[row + 1, d], peer_of(d)[1])
            c.start()
            copies.append(c)
        full[my] = send[...]
        for d in range(1, size):
            k, device = peer_of(size - d)
            copies[d - 1].wait_send()
            remote(send, full.at[k], sems.at[row, d], sems.at[row + 1, d], device).wait_recv()

    part = res_ref.shape[0] // nr
    copies = swap(nr, fpeer, lambda k: pv_ref.at[k], pv_recv, 0)
    vals = pv_ref[fme].astype(f32)
    for d in range(1, nr):
        copies[d - 1].wait()
        vals = vals + pv_recv[d].astype(f32)
    v_send[...] = vals.astype(bf16)
    gather(nr, fme, fpeer, v_send, v_all, 2)
    for k in range(nr):
        acc_rows = v_all[k].astype(f32)
        v_full[k * part:(k + 1) * part, :] = acc_rows
    x_ref = xg_ref[0]
    x_ref[...] = v_full[...].astype(bf16)
    matmul(x_ref, (0, acc))

    po_send[...] = acc[...].astype(bf16)
    copies = swap(n, peer, lambda k: po_send, po_recv, 4)
    total = res_ref[...].astype(f32) + acc[...]
    for d in range(1, n):
        copies[d - 1].wait()
        total = total + po_recv[d].astype(f32)
    crows = res_ref.shape[0] // n
    for k in range(n):
        resid[k] = total[k * crows:(k + 1) * crows]
    sumsq = jnp.sum(total * total, axis=1, keepdims=True)
    sumsq = jnp.broadcast_to(sumsq, (total.shape[0], 128))
    for k in range(nr):
        ss_send[k] = sumsq[k * part:(k + 1) * part]
    s_copies = swap(nr, fpeer, lambda k: ss_send.at[k], ss_recv, 6)
    x_ref = xg_ref[1]
    x_ref[...] = (total * gain_ref[...]).astype(bf16)
    matmul(x_ref, (1, g_acc), (2, u_acc))

    for j, a in enumerate((g_acc, u_acc)):
        for k in range(nr):
            gu_send[k, j] = a[k * part:(k + 1) * part, :].astype(bf16)
    copies = swap(nr, fpeer, lambda k: gu_send.at[k], gu_recv, 8)
    ss = ss_send[fme]
    for d in range(1, nr):
        s_copies[d - 1].wait()
        ss = ss + ss_recv[d]
    inv = lax.rsqrt(ss[:, 0:1] / D + epsilon)
    gate = gu_send[fme, 0].astype(f32)
    up = gu_send[fme, 1].astype(f32)
    for d in range(1, nr):
        copies[d - 1].wait()
        gate = gate + gu_recv[d, 0].astype(f32)
        up = up + gu_recv[d, 1].astype(f32)
    gate = gate * inv
    up = up * inv
    h_send[...] = (gate / (1.0 + jnp.exp(-gate)) * up).astype(bf16)
    gather(nr, fme, fpeer, h_send, h_all, 10)
    for k in range(nr):
        h_full[k * part:(k + 1) * part, :] = h_all[k].astype(f32)
    x_ref = xg_ref[2]
    x_ref[...] = h_full[...].astype(bf16)
    matmul(x_ref, (3, acc))

    for k in range(n):
        piece = acc[k * crows:(k + 1) * crows, :]
        dn[k] = piece
        dn_send[k] = piece.astype(bf16)
    copies = swap(n, peer, lambda k: dn_send.at[k], dn_recv, 12)
    result = resid[me] + dn[me]
    for d in range(1, n):
        copies[d - 1].wait()
        result = result + dn_recv[d].astype(f32)
    out_ref[...] = result.astype(bf16)


def chunk_of(depth):
    for size in (1024, 768, 512, 256):
        if depth % size == 0:
            return size
    return depth


def per_device_latents(sizes, queries, cache, lengths, positions, value_up_weight, out_proj, residual,
               norm_gain, gate_weight, up_weight, down_weight):
    n, n_role, n_seq = sizes
    nr = n_role * n_seq
    rows, heads, width = queries.shape
    seqs = cache.shape[0]
    span = rows * heads // seqs
    lat = LATENT // nr
    vmem = pl.BlockSpec(memory_space=pltpu.VMEM)
    smem = pl.BlockSpec(memory_space=pltpu.SMEM)
    hbm = pl.BlockSpec(memory_space=pl.ANY)
    most = max(n, nr)
    sems = lambda k: pltpu.SemaphoreType.DMA((k, most))
    vwide = heads * value_up_weight.shape[2]
    all_rows, dd = residual.shape
    ff = gate_weight.shape[1]
    part, crows = all_rows // nr, all_rows // n

    def held(w):
        size = chunk_of(w.shape[0])
        return pltpu.VMEM((w.shape[0] // size, size, w.shape[1]), bf16)

    ws = (out_proj, gate_weight, up_weight, down_weight)
    most_chunks = max(w.shape[0] // chunk_of(w.shape[0]) for w in ws)
    V = pltpu.VMEM
    return pl.pallas_call(
        functools.partial(layer_kernel, n, n_role, n_seq),
        out_shape=jax.ShapeDtypeStruct((crows, dd), bf16),
        in_specs=[vmem, hbm, smem, smem, hbm, vmem, vmem] + [hbm] * 4,
        out_specs=vmem,
        scratch_shapes=[
            V((cache.shape[0], width, cache.shape[1]), bf16),
            V(value_up_weight.shape, bf16),
            V((n, seqs, span, width), bf16),
            V((n, seqs, span, LATENT), bf16),
            V((n, seqs, span, LATENT), bf16),
            V((n, seqs, 8, span), f32),
            V((n, seqs, 8, span), f32),
            V((nr, rows, heads, lat), bf16),
            V((nr, rows, heads, lat), bf16),
            V((heads, all_rows, lat), f32),
            V((all_rows, vwide), f32),
            V((nr, part, vwide), bf16),
            *[held(w) for w in ws],
            V((nr, part, vwide), bf16),
            V((part, vwide), bf16),
            V((nr, part, vwide), bf16),
            V((all_rows, vwide), f32),
            V((all_rows, dd), f32),
            V((all_rows, dd), bf16),
            V((n, all_rows, dd), bf16),
            V((n, crows, dd), f32),
            [V((all_rows, vwide), bf16), V((all_rows, dd), bf16), V((all_rows, ff), bf16)],
            V((all_rows, ff), f32),
            V((all_rows, ff), f32),
            V((nr, 2, part, ff), bf16),
            V((nr, 2, part, ff), bf16),
            V((nr, part, 128), f32),
            V((nr, part, 128), f32),
            V((part, ff), bf16),
            V((nr, part, ff), bf16),
            V((all_rows, ff), f32),
            V((n, crows, dd), f32),
            V((n, crows, dd), bf16),
            V((n, crows, dd), bf16),
            pltpu.SemaphoreType.DMA((4, most_chunks)),
            pltpu.SemaphoreType.DMA((2,)),
            sems(8 * seqs),
            sems(14),
        ],
        compiler_params=pltpu.CompilerParams(
            collective_id=0, has_side_effects=True, vmem_limit_bytes=VMEM_BYTES),
        name="layer",
    )(queries.reshape(seqs, span, width), cache.transpose(0, 2, 1), lengths, positions, value_up_weight,
      residual, norm_gain.reshape(1, dd), *ws)


LOG2E = 1.4426950408889634


def by_distance(n, me):
    found = []
    for i in range(n - 1):
        k = jnp.int32(0)
        for z in range(n):
            others = sorted((j for j in range(n) if j != z), key=lambda j: (abs(j - z), j))
            k = jnp.where(me == z, others[i], k)
        found.append(k)
    return found


def cut(width):
    unit = 256 if width % 256 == 0 else 128
    if width % unit or width < 2 * unit:
        return [(0, width)]
    first = -(-(width // unit) // 2) * unit
    return [(0, first), (first, width)]


def heads_kernel(n, n_role, n_seq, q_hbm, cache_hbm, len_ref, pos_ref, vu_hbm, res_hbm, gain_hbm,
                 wo_hbm, wg_hbm, wu_hbm, wd_hbm, out_ref,
                 q_ref, cache, vu, res_ref, gain_ref, wo, wg, wu, wd,
                 q_send, q_all, o_send, o_recv, st_send, st_recv, w_ref,
                 a_head, v_send, xv, acc, po_send, po_recv, resid, ss_send, ss_recv,
                 g_acc, u_acc, gu_send, gu_recv, h_send, h_all, h_full, dn, dn_send, dn_recv,
                 lsem, wsem, qsem, gone, osem, stsem, vsem, posem, gusem, hsem, dnsem, onesem):
    nr = n_role * n_seq
    me = lax.axis_index("ctx")
    role, seq = lax.axis_index("role"), lax.axis_index("seq")
    fme = role * n_seq + seq
    near = by_distance(n, me)
    mates = []
    for dr in range(n_role):
        for ds in range(n_seq):
            if dr or ds:
                r, s = lax.rem(role + dr, n_role), lax.rem(seq + ds, n_seq)
                mates.append((r * n_seq + s, {"role": r, "seq": s}))
    seqs, span, width = q_ref.shape
    context = cache.shape[2]
    heads = span // MTP
    hk = heads // nr
    rope = width - LATENT
    lat = LATENT // nr
    own = n - 1
    extra = span * rope // LATENT

    q_copy = pltpu.make_async_copy(q_hbm, q_ref, lsem.at[0])
    q_copy.start()
    cache_copies = [
        pltpu.make_async_copy(cache_hbm, cache.at[:, pl.ds(0, width), :], lsem.at[1]),
        pltpu.make_async_copy(cache_hbm.at[:, pl.ds(LATENT, rope), :],
                              cache.at[:, pl.ds(width, rope), :], lsem.at[2]),
    ]
    for c in cache_copies:
        c.start()
    barrier = pltpu.get_barrier_semaphore()
    for k in near:
        pl.semaphore_signal(barrier, inc=1, device_id={"ctx": k}, device_id_type=MESH)
    for _, device in mates:
        pl.semaphore_signal(barrier, inc=1, device_id=device, device_id_type=MESH)
    vu_own = pltpu.make_async_copy(
        vu_hbm.at[pl.ds(pl.multiple_of(fme * hk, hk), hk)],
        vu.at[:, pl.ds(pl.multiple_of(fme * lat, lat), lat), :], lsem.at[3])
    vu_own.start()
    res_copy = pltpu.make_async_copy(res_hbm, res_ref, lsem.at[4])
    res_copy.start()
    gain_copy = pltpu.make_async_copy(gain_hbm, gain_ref.at[0], lsem.at[5])
    gain_copy.start()

    q_copy.wait()
    for s in range(seqs):
        qn, qr = [], []
        for k in range(nr):
            for t in range(MTP):
                at = t * heads + k * hk
                rows = q_ref[s, at:at + hk, :].astype(f32)
                qn.append(rows[:, :LATENT])
                qr.append(rows[:, LATENT:])
        q_send[s, :span] = jnp.concatenate(qn, axis=0).astype(bf16)
        qr = jnp.concatenate(qr, axis=0)
        qr = jnp.concatenate([qr[:span // 2], qr[span // 2:]], axis=1)
        q_send[s, span:] = jnp.concatenate(
            [qr[i:i + extra] for i in range(0, span // 2, extra)], axis=1).astype(bf16)
    weights = []
    for which, (hbm, vmem) in enumerate(((wo_hbm, wo), (wg_hbm, wg), (wu_hbm, wu), (wd_hbm, wd))):
        weights.append(pltpu.make_async_copy(hbm, vmem, wsem.at[which]))
    for c in weights:
        c.start()
    pl.semaphore_wait(barrier, len(near) + len(mates))

    Q, RELAY, VU, O, ST, VAL, PO, SS, GU, H, DN = range(11)

    def send(src, dst, kind, recv_sem, device):
        remote(src, dst, gone.at[kind], recv_sem, device).start()

    def all_gone(kind, like):
        remote(like, like, gone.at[kind], gone.at[kind], {"ctx": near[0]}).wait_send()

    def all_here(like, recv_sem):
        remote(like, like, gone.at[0], recv_sem, {"ctx": near[0]}).wait_recv()

    def take(b, s):
        all_here(q_all.at[b, s], qsem.at[s, b])

    paired = n == 4
    if paired:
        beside = me + 1 - 2 * lax.rem(me, 2)
        across = 2 - me // 2
        beyond = 3 - 3 * (me // 2)
        inner = lax.rem((me + 1) // 2, 2)
        reach = [beside, across]
    else:
        reach = near[::-1]
    for s in range(seqs):
        for k in reach:
            send(q_send.at[s], q_all.at[me, s], Q, qsem.at[s, me], {"ctx": k})
    for k, device in mates:
        send(vu_hbm.at[pl.ds(pl.multiple_of(k * hk, hk), hk)],
             vu.at[:, pl.ds(pl.multiple_of(fme * lat, lat), lat), :], VU, onesem.at[0], device)

    column = lax.broadcasted_iota(jnp.int32, (span, context), 1)
    row = lax.broadcasted_iota(jnp.int32, (span, 1), 0)
    even = lax.rem(row, MTP * hk) < hk
    lane = lax.broadcasted_iota(jnp.int32, (span, 128), 1)
    half = lax.broadcasted_iota(jnp.int32, (span // 2, 2 * rope), 1) < rope
    ends = []
    for s in range(seqs):
        limit = jnp.where(even, pos_ref[MTP * s], pos_ref[MTP * s + 1]) + 1
        ends.append(jnp.minimum(limit, len_ref[s]) - me * context)

    def block(queries, s, slot):
        qn, qr = queries[:span], queries[span:].astype(f32)
        qr = jnp.concatenate([qr[:, i:i + 128] for i in range(0, LATENT, 128)], axis=0)
        zero = jnp.zeros_like(qr)
        q = jnp.concatenate(
            [qn, jnp.concatenate([jnp.where(half, qr, zero), jnp.where(half, zero, qr)],
                                 axis=0).astype(bf16)],
            axis=1)
        keys = cache[s]
        scores = jnp.dot(q, keys, preferred_element_type=f32) * (softmax_scale * LOG2E)
        scores = jnp.where(column < ends[s], scores, -1e30)
        top = jnp.maximum(jnp.max(scores, axis=1, keepdims=True), -1e29)
        probs = jnp.exp2(scores - top).astype(bf16)
        total = jnp.sum(probs.astype(f32), axis=1, keepdims=True)
        out = lax.dot_general(
            probs, keys[:LATENT], (((1,), (1,)), ((), ())), preferred_element_type=f32)
        out = out.astype(bf16)
        for k in range(nr):
            o_send[slot, s, k] = out[k * MTP * hk:(k + 1) * MTP * hk]
        stats = jnp.where(lane == 0, top, total).T
        st_send[slot, s] = jnp.concatenate([stats[0:1], stats[1:2]], axis=1)

    mine = me * nr + fme
    for c in cache_copies:
        c.wait()
    for s in range(seqs):
        block(q_send[s], s, own)
        for k, device in mates:
            send(o_send.at[own, s, k], o_recv.at[mine, s], O, osem.at[s], device)
            send(st_send.at[own, s], st_recv.at[mine, s], ST, stsem.at[s], device)
        for c in (
            pltpu.make_async_copy(o_send.at[own, s, fme], o_recv.at[mine, s], osem.at[s]),
            pltpu.make_async_copy(st_send.at[own, s], st_recv.at[mine, s], stsem.at[s]),
        ):
            c.start()

    def answer(b, s, slot):
        block(q_all[b, s], s, slot)
        for k in range(nr):
            device = {"ctx": b, "role": k // n_seq, "seq": k % n_seq}
            send(o_send.at[slot, s, k], o_recv.at[mine, s], O, osem.at[s], device)
            send(st_send.at[slot, s], st_recv.at[mine, s], ST, stsem.at[s], device)

    if paired:
        def relay(b, s):
            @pl.when(inner == 1)
            def _():
                take(b, s)
                send(q_all.at[b, s], q_all.at[b, s], RELAY, qsem.at[s, b], {"ctx": beside})

        def take_outer(b, s):
            @pl.when(inner == 0)
            def _():
                take(b, s)

        relay(across, 0)
        for s in range(seqs):
            take(beside, s)
            answer(beside, s, 0)
            if s == 0:
                relay(beyond, 0)
            take_outer(across, s)
            answer(across, s, 1)
            if s + 1 < seqs:
                relay(across, s + 1)
            take_outer(beyond, s)
            answer(beyond, s, 2)
            if s + 1 < seqs:
                relay(beyond, s + 1)
    else:
        for s in range(seqs):
            for i, b in enumerate(near):
                take(b, s)
                answer(b, s, i)

    rows = seqs * MTP
    all_rows = nr * rows
    mine_at = pl.ds(pl.multiple_of(fme * MTP * hk, MTP * hk), MTP * hk)
    for s in range(seqs):
        all_here(st_recv.at[:, s], stsem.at[s])
        tops, totals = [], []
        for b in range(n):
            stats = [st_recv[b * nr + j, s] for j in range(nr)]
            stats = jnp.concatenate(stats, axis=0)
            tops.append(stats[:, :span])
            totals.append(stats[:, span:])
        highest = functools.reduce(jnp.maximum, tops)
        factors = [jnp.exp2(t - highest) for t in tops]
        denom = sum(f * t for f, t in zip(factors, totals))
        shares = jnp.concatenate([f / denom for f in factors], axis=0)
        copies = -(-128 // (n * nr))
        shares = jnp.concatenate([shares] * copies, axis=0)[:128]
        w_ref[s] = shares.T
        share = w_ref[s, mine_at, :]
        all_here(o_recv.at[:, s], osem.at[s])
        for j in range(nr):
            mixed = None
            for b in range(n):
                i = b * nr + j
                term = share[:, i:i + 1] * o_recv[i, s].astype(f32)
                mixed = term if mixed is None else mixed + term
            for t in range(MTP):
                a_head[:, j * rows + s * MTP + t, :] = mixed[t * hk:(t + 1) * hk]

    vu_own.wait()
    others = len(mates)
    all_here(vu.at[:, :others * lat], onesem.at[0])
    vdim = vu.shape[2]
    for h in range(hk):
        v_send[:, h * vdim:(h + 1) * vdim] = jnp.dot(
            a_head[h].astype(bf16), vu[h], preferred_element_type=f32).astype(bf16)
    for k, device in mates:
        send(v_send, xv.at[fme], VAL, vsem.at[fme], device)
    weights[0].wait()
    deep = hk * vdim

    def wo_rows(k):
        return pl.ds(pl.multiple_of(k * deep, deep), deep)

    acc[...] = jnp.dot(v_send[...], wo[wo_rows(fme), :], preferred_element_type=f32)

    def arrived(k, device):
        all_here(xv.at[k], vsem.at[k])

    early, late = mates[:n_seq - 1], mates[n_seq - 1:]
    for k, device in early:
        arrived(k, device)
        acc[...] += jnp.dot(xv[k], wo[wo_rows(k), :], preferred_element_type=f32)
    for k, device in late:
        arrived(k, device)
    dd = acc.shape[1]
    parts = cut(dd)
    for p, (c0, c1) in enumerate(parts):
        total = acc[:, c0:c1]
        for k, device in late:
            total = total + jnp.dot(xv[k], wo[wo_rows(k), c0:c1], preferred_element_type=f32)
        acc[:, c0:c1] = total
        po_send[:, c0:c1] = total.astype(bf16)
        for k in near[::-1]:
            send(po_send.at[:, c0:c1], po_recv.at[me, :, c0:c1], PO, posem.at[p], {"ctx": k})
    all_gone(Q, q_all.at[:len(reach)])
    if paired:
        @pl.when(inner == 1)
        def _():
            all_gone(RELAY, q_all.at[:2])
    all_gone(VU, vu.at[:, :others * lat])
    all_gone(O, o_recv.at[:n * nr - 1])
    all_gone(ST, st_recv.at[:n * nr - 1])
    all_gone(VAL, xv.at[:others])
    res_copy.wait()
    gain_copy.wait()
    weights[1].wait()
    weights[2].wait()

    part, crows = all_rows // nr, all_rows // n
    ff = g_acc.shape[1]
    fparts = [(f, min(f + 768, ff)) for f in range(0, ff, 768)]
    sumsq = jnp.zeros((all_rows, 1), f32)
    for p, (c0, c1) in enumerate(parts):
        total = res_ref[:, c0:c1].astype(f32) + acc[:, c0:c1]
        all_here(po_recv.at[:n - 1, :, c0:c1], posem.at[p])
        for k in near:
            total = total + po_recv[k, :, c0:c1].astype(f32)
        for k in range(n):
            resid[k, :, c0:c1] = total[k * crows:(k + 1) * crows]
        sumsq = sumsq + jnp.sum(total * total, axis=1, keepdims=True)
        x = (total * gain_ref[:, c0:c1]).astype(bf16)
        last = p == len(parts) - 1
        if last:
            wide = jnp.broadcast_to(sumsq, (all_rows, 128))
            for k in range(nr):
                ss_send[k] = wide[k * part:(k + 1) * part]
            for k, device in mates:
                send(ss_send.at[k], ss_recv.at[fme], SS, onesem.at[1], device)
        for q, (f0, f1) in enumerate(fparts if last else [(0, ff)]):
            for j, (w, a) in enumerate(((wg, g_acc), (wu, u_acc))):
                y = jnp.dot(x, w[c0:c1, f0:f1], preferred_element_type=f32)
                if p:
                    y = y + a[:, f0:f1]
                if not last:
                    a[:, f0:f1] = y
                    continue
                for k in range(nr):
                    gu_send[k, j, :, f0:f1] = y[k * part:(k + 1) * part].astype(bf16)
            if last:
                for k, device in mates:
                    send(gu_send.at[k, :, :, f0:f1], gu_recv.at[fme, :, :, f0:f1],
                         GU, gusem.at[q], device)
    ss = ss_send[fme]
    all_here(ss_recv.at[:others], onesem.at[1])
    for k, device in mates:
        ss = ss + ss_recv[k]
    inv = lax.rsqrt(ss[:, 0:1] / D + epsilon)
    for q, (f0, f1) in enumerate(fparts):
        gate = gu_send[fme, 0, :, f0:f1].astype(f32)
        up = gu_send[fme, 1, :, f0:f1].astype(f32)
        all_here(gu_recv.at[:others, :, :, f0:f1], gusem.at[q])
        for k, device in mates:
            gate = gate + gu_recv[k, 0, :, f0:f1].astype(f32)
            up = up + gu_recv[k, 1, :, f0:f1].astype(f32)
        gate = gate * inv
        up = up * inv
        h = (gate / (1.0 + jnp.exp(-gate)) * up).astype(bf16)
        h_send[:, f0:f1] = h
        h_all[fme, :, f0:f1] = h
        for k, device in mates:
            send(h_send.at[:, f0:f1], h_all.at[fme, :, f0:f1], H, hsem.at[q], device)
    weights[3].wait()
    for q, (f0, f1) in enumerate(fparts):
        all_here(h_all.at[:others, :, f0:f1], hsem.at[q])
        for k in range(nr):
            h_full[k * part:(k + 1) * part, f0:f1] = h_all[k, :, f0:f1].astype(f32)
        x = h_full[:, f0:f1].astype(bf16)
        last = q == len(fparts) - 1
        for p, (c0, c1) in enumerate(parts if last else [(0, dd)]):
            y = jnp.dot(x, wd[f0:f1, c0:c1], preferred_element_type=f32)
            if q:
                y = y + acc[:, c0:c1]
            if not last:
                acc[:, c0:c1] = y
                continue
            for k in range(n):
                piece = y[k * crows:(k + 1) * crows]
                dn[k, :, c0:c1] = piece
                dn_send[k, :, c0:c1] = piece.astype(bf16)
            for k in near[::-1]:
                send(dn_send.at[k, :, c0:c1], dn_recv.at[me, :, c0:c1], DN, dnsem.at[p], {"ctx": k})
    all_gone(PO, po_recv.at[:n - 1])
    all_gone(SS, ss_recv.at[:others])
    all_gone(GU, gu_recv.at[:others])
    all_gone(H, h_all.at[:others])
    for p, (c0, c1) in enumerate(parts):
        result = resid[me, :, c0:c1] + dn[me, :, c0:c1]
        all_here(dn_recv.at[:n - 1, :, c0:c1], dnsem.at[p])
        for k in near:
            result = result + dn_recv[k, :, c0:c1].astype(f32)
        out_ref[:, c0:c1] = result.astype(bf16)
    all_gone(DN, dn_recv.at[:n - 1])


def per_device(sizes, queries, cache, lengths, positions, value_up_weight, out_proj, residual,
               norm_gain, gate_weight, up_weight, down_weight):
    n, n_role, n_seq = sizes
    nr = n_role * n_seq
    rows, heads, width = queries.shape
    seqs, context = cache.shape[:2]
    rope = width - LATENT
    if heads % (8 * nr) or 2 * rope != 128 or n < 2 or nr < 2:
        return per_device_latents(
            sizes, queries, cache, lengths, positions, value_up_weight, out_proj, residual,
            norm_gain, gate_weight, up_weight, down_weight)
    hk = heads // nr
    span = rows * heads // seqs
    extra = span * rope // LATENT
    vdim = value_up_weight.shape[2]
    all_rows, dd = residual.shape
    ff = gate_weight.shape[1]
    part, crows = all_rows // nr, all_rows // n
    nf = -(-ff // 768)
    vmem = pl.BlockSpec(memory_space=pltpu.VMEM)
    smem = pl.BlockSpec(memory_space=pltpu.SMEM)
    hbm = pl.BlockSpec(memory_space=pl.ANY)
    V = pltpu.VMEM
    sems = lambda *k: pltpu.SemaphoreType.DMA(k)
    return pl.pallas_call(
        functools.partial(heads_kernel, n, n_role, n_seq),
        out_shape=jax.ShapeDtypeStruct((crows, dd), bf16),
        in_specs=[hbm, hbm, smem, smem] + [hbm] * 7,
        out_specs=vmem,
        scratch_shapes=[
            V((seqs, span, width), bf16),
            V((seqs, width + rope, context), bf16),
            V((hk, LATENT, vdim), bf16),
            V((all_rows, dd), bf16),
            V((1, dd), f32),
            V(out_proj.shape, bf16),
            V(gate_weight.shape, bf16),
            V(up_weight.shape, bf16),
            V(down_weight.shape, bf16),
            V((seqs, span + extra, LATENT), bf16),
            V((n, seqs, span + extra, LATENT), bf16),
            V((n, seqs, nr, MTP * hk, LATENT), bf16),
            V((n * nr, seqs, MTP * hk, LATENT), bf16),
            V((n, seqs, 1, 2 * span), f32),
            V((n * nr, seqs, 1, 2 * span), f32),
            V((seqs, span, 128), f32),
            V((hk, all_rows, LATENT), f32),
            V((all_rows, hk * vdim), bf16),
            V((nr, all_rows, hk * vdim), bf16),
            V((all_rows, dd), f32),
            V((all_rows, dd), bf16),
            V((n, all_rows, dd), bf16),
            V((n, crows, dd), f32),
            V((nr, part, 128), f32),
            V((nr, part, 128), f32),
            V((all_rows, ff), f32),
            V((all_rows, ff), f32),
            V((nr, 2, part, ff), bf16),
            V((nr, 2, part, ff), bf16),
            V((part, ff), bf16),
            V((nr, part, ff), bf16),
            V((all_rows, ff), f32),
            V((n, crows, dd), f32),
            V((n, crows, dd), bf16),
            V((n, crows, dd), bf16),
            sems(6),
            sems(4),
            sems(seqs, n),
            sems(11),
            sems(seqs),
            sems(seqs),
            sems(nr),
            sems(2),
            sems(nf),
            sems(nf),
            sems(2),
            sems(2),
        ],
        compiler_params=pltpu.CompilerParams(
            collective_id=0, has_side_effects=True, vmem_limit_bytes=VMEM_BYTES),
        name="layer",
    )(queries.reshape(seqs, span, width), cache.transpose(0, 2, 1), lengths, positions, value_up_weight,
      residual, norm_gain, out_proj, gate_weight, up_weight, down_weight)


def solution(mesh):
    placed = (
        P(("groups", "role", "seq"), "ctx", None),
        P(("groups", "role", "seq"), "ctx", None),
        P(("groups", "role", "seq")),
        P(("groups", "role", "seq")),
        P("ctx", ("role", "seq"), None),
        P("ctx", ("role", "seq")),
        P("groups", ("role", "seq")),
        P(("role", "seq")),
        P(("role", "seq"), "ctx"),
        P(("role", "seq"), "ctx"),
        P("ctx", ("role", "seq")),
    )
    sizes = (mesh.shape["ctx"], mesh.shape["role"], mesh.shape["seq"])
    return jax.shard_map(
        functools.partial(per_device, sizes),
        mesh=mesh,
        in_specs=placed,
        out_specs=P(("groups", "ctx"), ("role", "seq")),
        check_vma=False,
    )
```

```python
import functools

import jax
import jax.numpy as jnp
from jax import lax
from jax.experimental import pallas as pl
from jax.experimental.pallas import tpu as pltpu
from jax.sharding import PartitionSpec as P

D = 7168
LATENT = 512
MTP = 2

softmax_scale = 0.07216878364870323
epsilon = 1e-06
MESH = pl.DeviceIdType.MESH
VMEM_BYTES = 60 * 1024 * 1024
f32, bf16 = jnp.float32, jnp.bfloat16


def ctx_group(n):
    me = lax.axis_index("ctx")

    def peer(d):
        k = lax.rem(me + d, n)
        return k, {"ctx": k}

    return me, peer


def feature_group(n_role, n_seq):
    n = n_role * n_seq
    me = lax.axis_index("role") * n_seq + lax.axis_index("seq")

    def peer(d):
        k = lax.rem(me + d, n)
        return k, {"role": k // n_seq, "seq": lax.rem(k, n_seq)}

    return me, peer


def enter(groups):
    barrier = pltpu.get_barrier_semaphore()
    count = 0
    for n, peer in groups:
        for d in range(1, n):
            pl.semaphore_signal(barrier, inc=1, device_id=peer(d)[1], device_id_type=MESH)
            count += 1
    pl.semaphore_wait(barrier, count)


def remote(src, dst, send, recv, device):
    return pltpu.make_async_remote_copy(
        src_ref=src, dst_ref=dst, send_sem=send, recv_sem=recv,
        device_id=device, device_id_type=MESH,
    )


def attend(n, n_role, n_seq, q_ref, cache_ref, cache_copy, len_ref, pos_ref, out_ref,
           q_all, o_send, o_recv, s_send, s_recv, a_send, sems):
    nr = n_role * n_seq
    me, peer = ctx_group(n)
    fme, fpeer = feature_group(n_role, n_seq)
    seqs, _, context = cache_ref.shape
    rows = q_ref.shape[1]
    heads = rows // MTP

    q_copies = []
    for s in range(seqs):
        for d in range(1, n):
            c = remote(q_ref.at[s], q_all.at[me, s], sems.at[s, d], sems.at[seqs + s, d],
                       peer(d)[1])
            c.start()
            q_copies.append(c)

    places = me * context + lax.broadcasted_iota(jnp.int32, (rows, context), 1)
    first = lax.broadcasted_iota(jnp.int32, (rows, context), 0) < heads
    lives = []
    for s in range(seqs):
        limit = jnp.where(first, pos_ref[MTP * s], pos_ref[MTP * s + 1])
        lives.append((places < len_ref[s]) & (places <= limit))

    lane = lax.broadcasted_iota(jnp.int32, (rows, 128), 1)

    def block(q, s):
        keys = cache_ref[s]
        scores = jnp.dot(q, keys, preferred_element_type=f32) * softmax_scale
        live = lives[s]
        top = jnp.max(jnp.where(live, scores, -1e30), axis=1, keepdims=True)
        probs = jnp.exp(jnp.where(live, scores - top, -1e30)).astype(bf16)
        total = jnp.sum(probs.astype(f32), axis=1, keepdims=True)
        out = lax.dot_general(
            probs, keys[:LATENT], (((1,), (1,)), ((), ())), preferred_element_type=f32)
        return out, top, total

    cache_copy.wait()
    own = [block(q_ref[s], s) for s in range(seqs)]
    o_copies, s_copies = {}, {}
    for s in range(seqs):
        for d in range(1, n):
            src, device = peer(n - d)
            remote(q_ref.at[s], q_all.at[src, s], sems.at[s, d], sems.at[seqs + s, d],
                   device).wait_recv()
            o, top, total = block(q_all[src, s], s)
            o_send[d, s] = o.astype(bf16)
            s_send[d, s] = jnp.where(lane == 0, top, total).T[0:8]
            c = remote(o_send.at[d, s], o_recv.at[d, s], sems.at[2 * seqs + s, d],
                       sems.at[3 * seqs + s, d], device)
            c.start()
            o_copies[s, d] = c
            c = remote(s_send.at[d, s], s_recv.at[d, s], sems.at[4 * seqs + s, d],
                       sems.at[5 * seqs + s, d], device)
            c.start()
            s_copies[s, d] = c
    for c in q_copies:
        c.wait_send()

    heads = rows // MTP
    merged = []
    for s in range(seqs):
        own_o, top, total = own[s]
        tops, totals = [top], [total]
        for d in range(1, n):
            s_copies[s, d].wait()
            back = jnp.concatenate([s_recv[d, s]] * 16, axis=0).T
            tops.append(back[:, 0:1])
            totals.append(back[:, 1:2])
        highest = functools.reduce(jnp.maximum, tops)
        factors = [jnp.exp(t - highest) for t in tops]
        denom = sum(f * t for f, t in zip(factors, totals))
        numer = factors[0] * own_o
        for d in range(1, n):
            o_copies[s, d].wait()
            numer = numer + factors[d] * o_recv[d, s].astype(f32)
        merged.append((numer / denom).astype(bf16))

    part = LATENT // nr
    for k in range(nr):
        for r in range(seqs * MTP):
            t = r % MTP
            a_send[k, r] = merged[r // MTP][t * heads:(t + 1) * heads, k * part:(k + 1) * part]
    copies = []
    for d in range(1, nr):
        k, device = fpeer(d)
        c = remote(a_send.at[k], out_ref.at[fme], sems.at[6 * seqs, d], sems.at[7 * seqs, d], device)
        c.start()
        copies.append(c)
    out_ref[fme] = a_send[fme]
    for d in range(1, nr):
        k, device = fpeer(nr - d)
        copies[d - 1].wait_send()
        remote(a_send.at[k], out_ref.at[k], sems.at[6 * seqs, d], sems.at[7 * seqs, d],
               device).wait_recv()


def layer_kernel(n, n_role, n_seq, q_ref, cache_hbm, len_ref, pos_ref, vu_hbm, res_ref, gain_ref,
                 wo_hbm, wg_hbm, wu_hbm, wd_hbm,
                 out_ref, cache, vu, q_all, o_send, o_recv, s_send, s_recv, a_send, a_all, a_head,
                 mixed, pv_ref, wo, wg, wu, wd, pv_recv, v_send, v_all, v_full, acc, po_send,
                 po_recv, resid, xg_ref, g_acc, u_acc, gu_send, gu_recv, ss_send, ss_recv, h_send,
                 h_all, h_full, dn, dn_send, dn_recv, wsem, lsem, asems, sems):
    nr = n_role * n_seq
    me, peer = ctx_group(n)
    fme, fpeer = feature_group(n_role, n_seq)

    cache_copy = pltpu.make_async_copy(cache_hbm, cache, lsem.at[0])
    cache_copy.start()
    vu_copy = pltpu.make_async_copy(vu_hbm, vu, lsem.at[1])
    vu_copy.start()
    weights = []
    for which, (hbm, vmem) in enumerate(((wo_hbm, wo), (wg_hbm, wg), (wu_hbm, wu), (wd_hbm, wd))):
        depth = vmem.shape[1]

        def fetch(i, hbm=hbm, vmem=vmem, depth=depth, which=which):
            return pltpu.make_async_copy(
                hbm.at[pl.ds(i * depth, depth)], vmem.at[i], wsem.at[which, i])

        weights.append((fetch, vmem))
    for fetch, vmem in weights:
        for i in range(vmem.shape[0]):
            fetch(i).start()
    enter(((n, peer), (nr, fpeer)))
    attend(n, n_role, n_seq, q_ref, cache, cache_copy, len_ref, pos_ref, a_all,
           q_all, o_send, o_recv, s_send, s_recv, a_send, asems)
    rows, heads = a_all.shape[1:3]
    for j in range(nr):
        for r in range(rows):
            a_head[:, j * rows + r, :] = a_all[j, r].astype(f32)
    vu_copy.wait()
    vdim = vu.shape[2]
    for h in range(heads):
        mixed[:, h * vdim:(h + 1) * vdim] = jnp.dot(
            a_head[h].astype(bf16), vu[h], preferred_element_type=f32)
    for k in range(nr):
        pv_ref[k] = mixed[k * rows:(k + 1) * rows, :].astype(bf16)

    def matmul(x_ref, *pairs):
        chunks, depth, _ = weights[pairs[0][0]][1].shape
        for which, acc_ref in pairs:
            fetch, vmem = weights[which]
            fetch(0).wait()
            acc_ref[...] = jnp.dot(x_ref[:, :depth], vmem[0], preferred_element_type=f32)
        if chunks == 1:
            return

        @pl.loop(1, chunks)
        def _(i):
            x = x_ref[:, pl.ds(pl.multiple_of(i * depth, depth), depth)]
            for which, acc_ref in pairs:
                fetch, vmem = weights[which]
                fetch(i).wait()
                acc_ref[...] += jnp.dot(x, vmem[i], preferred_element_type=f32)

    def swap(size, peer_of, chunk, recv, row):
        copies = []
        for d in range(1, size):
            k, device = peer_of(d)
            c = remote(chunk(k), recv.at[d], sems.at[row, d], sems.at[row + 1, d], device)
            c.start()
            copies.append(c)
        return copies

    def gather(size, my, peer_of, send, full, row):
        copies = []
        for d in range(1, size):
            c = remote(send, full.at[my], sems.at[row, d], sems.at[row + 1, d], peer_of(d)[1])
            c.start()
            copies.append(c)
        full[my] = send[...]
        for d in range(1, size):
            k, device = peer_of(size - d)
            copies[d - 1].wait_send()
            remote(send, full.at[k], sems.at[row, d], sems.at[row + 1, d], device).wait_recv()

    part = res_ref.shape[0] // nr
    copies = swap(nr, fpeer, lambda k: pv_ref.at[k], pv_recv, 0)
    vals = pv_ref[fme].astype(f32)
    for d in range(1, nr):
        copies[d - 1].wait()
        vals = vals + pv_recv[d].astype(f32)
    v_send[...] = vals.astype(bf16)
    gather(nr, fme, fpeer, v_send, v_all, 2)
    for k in range(nr):
        acc_rows = v_all[k].astype(f32)
        v_full[k * part:(k + 1) * part, :] = acc_rows
    x_ref = xg_ref[0]
    x_ref[...] = v_full[...].astype(bf16)
    matmul(x_ref, (0, acc))

    po_send[...] = acc[...].astype(bf16)
    copies = swap(n, peer, lambda k: po_send, po_recv, 4)
    total = res_ref[...].astype(f32) + acc[...]
    for d in range(1, n):
        copies[d - 1].wait()
        total = total + po_recv[d].astype(f32)
    crows = res_ref.shape[0] // n
    for k in range(n):
        resid[k] = total[k * crows:(k + 1) * crows]
    sumsq = jnp.sum(total * total, axis=1, keepdims=True)
    sumsq = jnp.broadcast_to(sumsq, (total.shape[0], 128))
    for k in range(nr):
        ss_send[k] = sumsq[k * part:(k + 1) * part]
    s_copies = swap(nr, fpeer, lambda k: ss_send.at[k], ss_recv, 6)
    x_ref = xg_ref[1]
    x_ref[...] = (total * gain_ref[...]).astype(bf16)
    matmul(x_ref, (1, g_acc), (2, u_acc))

    for j, a in enumerate((g_acc, u_acc)):
        for k in range(nr):
            gu_send[k, j] = a[k * part:(k + 1) * part, :].astype(bf16)
    copies = swap(nr, fpeer, lambda k: gu_send.at[k], gu_recv, 8)
    ss = ss_send[fme]
    for d in range(1, nr):
        s_copies[d - 1].wait()
        ss = ss + ss_recv[d]
    inv = lax.rsqrt(ss[:, 0:1] / D + epsilon)
    gate = gu_send[fme, 0].astype(f32)
    up = gu_send[fme, 1].astype(f32)
    for d in range(1, nr):
        copies[d - 1].wait()
        gate = gate + gu_recv[d, 0].astype(f32)
        up = up + gu_recv[d, 1].astype(f32)
    gate = gate * inv
    up = up * inv
    h_send[...] = (gate / (1.0 + jnp.exp(-gate)) * up).astype(bf16)
    gather(nr, fme, fpeer, h_send, h_all, 10)
    for k in range(nr):
        h_full[k * part:(k + 1) * part, :] = h_all[k].astype(f32)
    x_ref = xg_ref[2]
    x_ref[...] = h_full[...].astype(bf16)
    matmul(x_ref, (3, acc))

    for k in range(n):
        piece = acc[k * crows:(k + 1) * crows, :]
        dn[k] = piece
        dn_send[k] = piece.astype(bf16)
    copies = swap(n, peer, lambda k: dn_send.at[k], dn_recv, 12)
    result = resid[me] + dn[me]
    for d in range(1, n):
        copies[d - 1].wait()
        result = result + dn_recv[d].astype(f32)
    out_ref[...] = result.astype(bf16)


def chunk_of(depth):
    for size in (1024, 768, 512, 256):
        if depth % size == 0:
            return size
    return depth


def per_device_latents(sizes, queries, cache, lengths, positions, value_up_weight, out_proj, residual,
               norm_gain, gate_weight, up_weight, down_weight):
    n, n_role, n_seq = sizes
    nr = n_role * n_seq
    rows, heads, width = queries.shape
    seqs = cache.shape[0]
    span = rows * heads // seqs
    lat = LATENT // nr
    vmem = pl.BlockSpec(memory_space=pltpu.VMEM)
    smem = pl.BlockSpec(memory_space=pltpu.SMEM)
    hbm = pl.BlockSpec(memory_space=pl.ANY)
    most = max(n, nr)
    sems = lambda k: pltpu.SemaphoreType.DMA((k, most))
    vwide = heads * value_up_weight.shape[2]
    all_rows, dd = residual.shape
    ff = gate_weight.shape[1]
    part, crows = all_rows // nr, all_rows // n

    def held(w):
        size = chunk_of(w.shape[0])
        return pltpu.VMEM((w.shape[0] // size, size, w.shape[1]), bf16)

    ws = (out_proj, gate_weight, up_weight, down_weight)
    most_chunks = max(w.shape[0] // chunk_of(w.shape[0]) for w in ws)
    V = pltpu.VMEM
    return pl.pallas_call(
        functools.partial(layer_kernel, n, n_role, n_seq),
        out_shape=jax.ShapeDtypeStruct((crows, dd), bf16),
        in_specs=[vmem, hbm, smem, smem, hbm, vmem, vmem] + [hbm] * 4,
        out_specs=vmem,
        scratch_shapes=[
            V((cache.shape[0], width, cache.shape[1]), bf16),
            V(value_up_weight.shape, bf16),
            V((n, seqs, span, width), bf16),
            V((n, seqs, span, LATENT), bf16),
            V((n, seqs, span, LATENT), bf16),
            V((n, seqs, 8, span), f32),
            V((n, seqs, 8, span), f32),
            V((nr, rows, heads, lat), bf16),
            V((nr, rows, heads, lat), bf16),
            V((heads, all_rows, lat), f32),
            V((all_rows, vwide), f32),
            V((nr, part, vwide), bf16),
            *[held(w) for w in ws],
            V((nr, part, vwide), bf16),
            V((part, vwide), bf16),
            V((nr, part, vwide), bf16),
            V((all_rows, vwide), f32),
            V((all_rows, dd), f32),
            V((all_rows, dd), bf16),
            V((n, all_rows, dd), bf16),
            V((n, crows, dd), f32),
            [V((all_rows, vwide), bf16), V((all_rows, dd), bf16), V((all_rows, ff), bf16)],
            V((all_rows, ff), f32),
            V((all_rows, ff), f32),
            V((nr, 2, part, ff), bf16),
            V((nr, 2, part, ff), bf16),
            V((nr, part, 128), f32),
            V((nr, part, 128), f32),
            V((part, ff), bf16),
            V((nr, part, ff), bf16),
            V((all_rows, ff), f32),
            V((n, crows, dd), f32),
            V((n, crows, dd), bf16),
            V((n, crows, dd), bf16),
            pltpu.SemaphoreType.DMA((4, most_chunks)),
            pltpu.SemaphoreType.DMA((2,)),
            sems(8 * seqs),
            sems(14),
        ],
        compiler_params=pltpu.CompilerParams(
            collective_id=0, has_side_effects=True, vmem_limit_bytes=VMEM_BYTES),
        name="layer",
    )(queries.reshape(seqs, span, width), cache.transpose(0, 2, 1), lengths, positions, value_up_weight,
      residual, norm_gain.reshape(1, dd), *ws)


LOG2E = 1.4426950408889634


def by_distance(n, me):
    found = []
    for i in range(n - 1):
        k = jnp.int32(0)
        for z in range(n):
            others = sorted((j for j in range(n) if j != z), key=lambda j: (abs(j - z), j))
            k = jnp.where(me == z, others[i], k)
        found.append(k)
    return found


def cut(width):
    unit = 256 if width % 256 == 0 else 128
    if width % unit or width < 2 * unit:
        return [(0, width)]
    first = -(-(width // unit) // 2) * unit
    return [(0, first), (first, width)]


def heads_kernel(n, n_role, n_seq, q_hbm, cache_hbm, len_ref, pos_ref, vu_hbm, res_hbm, gain_hbm,
                 wo_hbm, wg_hbm, wu_hbm, wd_hbm, out_ref,
                 q_ref, cache, vu, res_ref, gain_ref, wo, wg, wu, wd,
                 q_send, q_all, o_send, o_recv, st_send, st_recv, w_ref,
                 a_head, v_send, xv, acc, po, po_send, po_recv, resid, ss_send, ss_recv,
                 g_acc, u_acc, gu_send, gu_recv, h_send, h_all, h_full, dn, dn_send, dn_recv,
                 lsem, wsem, qsem, gone, osem, stsem, vsem, posem, gusem, hsem, dnsem, onesem):
    nr = n_role * n_seq
    me = lax.axis_index("ctx")
    role, seq = lax.axis_index("role"), lax.axis_index("seq")
    fme = role * n_seq + seq
    near = by_distance(n, me)
    mates = []
    for dr in range(n_role):
        for ds in range(n_seq):
            if dr or ds:
                r, s = lax.rem(role + dr, n_role), lax.rem(seq + ds, n_seq)
                mates.append((r * n_seq + s, {"role": r, "seq": s}))
    seqs, span, width = q_ref.shape
    context = cache.shape[2]
    heads = span // MTP
    hk = heads // nr
    rope = width - LATENT
    lat = LATENT // nr
    own = n - 1
    extra = span * rope // LATENT

    paired = n == 4
    if paired:
        beside = me + 1 - 2 * lax.rem(me, 2)
        across = 2 - me // 2
        beyond = 3 - 3 * (me // 2)
        inner = lax.rem((me + 1) // 2, 2)
        reach = [beside, across]
    else:
        reach = near[::-1]

    q_copy = pltpu.make_async_copy(q_hbm, q_ref, lsem.at[0])
    q_copy.start()
    cache_copies = [
        pltpu.make_async_copy(cache_hbm, cache.at[:, pl.ds(0, width), :], lsem.at[1]),
        pltpu.make_async_copy(cache_hbm.at[:, pl.ds(LATENT, rope), :],
                              cache.at[:, pl.ds(width, rope), :], lsem.at[2]),
    ]
    for c in cache_copies:
        c.start()
    barrier = pltpu.get_barrier_semaphore()
    if paired:
        pl.semaphore_signal(barrier, inc=1, device_id={"ctx": beside}, device_id_type=MESH)

        @pl.when(inner == 1)
        def _():
            for k in (across, beyond):
                pl.semaphore_signal(barrier, inc=1, device_id={"ctx": k}, device_id_type=MESH)
    else:
        for k in near:
            pl.semaphore_signal(barrier, inc=1, device_id={"ctx": k}, device_id_type=MESH)
    for _, device in mates:
        pl.semaphore_signal(barrier, inc=1, device_id=device, device_id_type=MESH)
    vu_own = pltpu.make_async_copy(
        vu_hbm.at[pl.ds(pl.multiple_of(fme * hk, hk), hk)],
        vu.at[:, pl.ds(pl.multiple_of(fme * lat, lat), lat), :], lsem.at[3])
    vu_own.start()
    res_copy = pltpu.make_async_copy(res_hbm, res_ref, lsem.at[4])
    res_copy.start()
    gain_copy = pltpu.make_async_copy(gain_hbm, gain_ref.at[0], lsem.at[5])
    gain_copy.start()

    q_copy.wait()
    for s in range(seqs):
        qn, qr = [], []
        for k in range(nr):
            for t in range(MTP):
                at = t * heads + k * hk
                rows = q_ref[s, at:at + hk, :].astype(f32)
                qn.append(rows[:, :LATENT])
                qr.append(rows[:, LATENT:])
        q_send[s, :span] = jnp.concatenate(qn, axis=0).astype(bf16)
        qr = jnp.concatenate(qr, axis=0)
        qr = jnp.concatenate([qr[:span // 2], qr[span // 2:]], axis=1)
        q_send[s, span:] = jnp.concatenate(
            [qr[i:i + extra] for i in range(0, span // 2, extra)], axis=1).astype(bf16)
    weights = []
    for which, (hbm, vmem) in enumerate(((wo_hbm, wo), (wg_hbm, wg), (wu_hbm, wu), (wd_hbm, wd))):
        weights.append(pltpu.make_async_copy(hbm, vmem, wsem.at[which]))
    for c in weights:
        c.start()
    pl.semaphore_wait(barrier, len(reach) + len(mates))

    Q, RELAY, VU, O, ST, VAL, PO, SS, GU, H, DN = range(11)

    def send(src, dst, kind, recv_sem, device):
        remote(src, dst, gone.at[kind], recv_sem, device).start()

    def all_gone(kind, like):
        remote(like, like, gone.at[kind], gone.at[kind], {"ctx": near[0]}).wait_send()

    def all_here(like, recv_sem):
        remote(like, like, gone.at[0], recv_sem, {"ctx": near[0]}).wait_recv()

    def take(b, s):
        all_here(q_all.at[b, s], qsem.at[s, b])

    for s in range(seqs):
        for k in reach:
            send(q_send.at[s], q_all.at[me, s], Q, qsem.at[s, me], {"ctx": k})
    for k, device in mates:
        send(vu_hbm.at[pl.ds(pl.multiple_of(k * hk, hk), hk)],
             vu.at[:, pl.ds(pl.multiple_of(fme * lat, lat), lat), :], VU, onesem.at[0], device)

    column = lax.broadcasted_iota(jnp.int32, (span, context), 1)
    row = lax.broadcasted_iota(jnp.int32, (span, 1), 0)
    even = lax.rem(row, MTP * hk) < hk
    lane = lax.broadcasted_iota(jnp.int32, (span, 128), 1)
    half = lax.broadcasted_iota(jnp.int32, (span // 2, 2 * rope), 1) < rope
    ends = []
    for s in range(seqs):
        limit = jnp.where(even, pos_ref[MTP * s], pos_ref[MTP * s + 1]) + 1
        ends.append(jnp.minimum(limit, len_ref[s]) - me * context)

    def block(queries, s, slot):
        qn, qr = queries[:span], queries[span:].astype(f32)
        qr = jnp.concatenate([qr[:, i:i + 128] for i in range(0, LATENT, 128)], axis=0)
        zero = jnp.zeros_like(qr)
        q = jnp.concatenate(
            [qn, jnp.concatenate([jnp.where(half, qr, zero), jnp.where(half, zero, qr)],
                                 axis=0).astype(bf16)],
            axis=1)
        keys = cache[s]
        scores = jnp.dot(q, keys, preferred_element_type=f32) * (softmax_scale * LOG2E)
        scores = jnp.where(column < ends[s], scores, -1e30)
        top = jnp.maximum(jnp.max(scores, axis=1, keepdims=True), -1e29)
        probs = jnp.exp2(scores - top).astype(bf16)
        total = jnp.sum(probs.astype(f32), axis=1, keepdims=True)
        out = lax.dot_general(
            probs, keys[:LATENT], (((1,), (1,)), ((), ())), preferred_element_type=f32)
        out = out.astype(bf16)
        for k in range(nr):
            o_send[slot, s, k] = out[k * MTP * hk:(k + 1) * MTP * hk]
        stats = jnp.where(lane == 0, top, total).T
        st_send[slot, s] = jnp.concatenate([stats[0:1], stats[1:2]], axis=1)

    mine = me * nr + fme
    for c in cache_copies:
        c.wait()
    for s in range(seqs):
        block(q_send[s], s, own)
        for k, device in mates:
            send(o_send.at[own, s, k], o_recv.at[mine, s], O, osem.at[s], device)
            send(st_send.at[own, s], st_recv.at[mine, s], ST, stsem.at[s], device)
        for c in (
            pltpu.make_async_copy(o_send.at[own, s, fme], o_recv.at[mine, s], osem.at[s]),
            pltpu.make_async_copy(st_send.at[own, s], st_recv.at[mine, s], stsem.at[s]),
        ):
            c.start()

    def answer(b, s, slot):
        block(q_all[b, s], s, slot)
        for k in range(nr):
            device = {"ctx": b, "role": k // n_seq, "seq": k % n_seq}
            send(o_send.at[slot, s, k], o_recv.at[mine, s], O, osem.at[s], device)
            send(st_send.at[slot, s], st_recv.at[mine, s], ST, stsem.at[s], device)

    if paired:
        def relay(b, s):
            @pl.when(inner == 1)
            def _():
                take(b, s)
                send(q_all.at[b, s], q_all.at[b, s], RELAY, qsem.at[s, b], {"ctx": beside})

        def take_outer(b, s):
            @pl.when(inner == 0)
            def _():
                take(b, s)

        relay(across, 0)
        for s in range(seqs):
            take(beside, s)
            answer(beside, s, 0)
            if s == 0:
                relay(beyond, 0)
            take_outer(across, s)
            answer(across, s, 1)
            if s + 1 < seqs:
                relay(across, s + 1)
            take_outer(beyond, s)
            answer(beyond, s, 2)
            if s + 1 < seqs:
                relay(beyond, s + 1)
    else:
        for s in range(seqs):
            for i, b in enumerate(near):
                take(b, s)
                answer(b, s, i)

    rows = seqs * MTP
    all_rows = nr * rows
    mine_at = pl.ds(pl.multiple_of(fme * MTP * hk, MTP * hk), MTP * hk)
    vdim = vu.shape[2]
    deep = hk * vdim
    others = len(mates)

    def merge(s):
        all_here(st_recv.at[:, s], stsem.at[s])
        tops, totals = [], []
        for b in range(n):
            stats = jnp.concatenate([st_recv[b * nr + j, s] for j in range(nr)], axis=0)
            tops.append(stats[:, :span])
            totals.append(stats[:, span:])
        highest = functools.reduce(jnp.maximum, tops)
        factors = [jnp.exp2(t - highest) for t in tops]
        denom = sum(f * t for f, t in zip(factors, totals))
        shares = jnp.concatenate([f / denom for f in factors], axis=0)
        copies = -(-128 // (n * nr))
        shares = jnp.concatenate([shares] * copies, axis=0)[:128]
        w_ref[s] = shares.T
        share = w_ref[s, mine_at, :]
        all_here(o_recv.at[:, s], osem.at[s])
        for j in range(nr):
            mixed = None
            for b in range(n):
                i = b * nr + j
                term = share[:, i:i + 1] * o_recv[i, s].astype(f32)
                mixed = term if mixed is None else mixed + term
            for t in range(MTP):
                a_head[:, s, j * MTP + t, :] = mixed[t * hk:(t + 1) * hk]
        if s == 0:
            vu_own.wait()
            all_here(vu.at[:, :others * lat], onesem.at[0])
        for h in range(hk):
            v_send[s, :, h * vdim:(h + 1) * vdim] = jnp.dot(
                a_head[h, s].astype(bf16), vu[h], preferred_element_type=f32).astype(bf16)
        for k, device in mates:
            send(v_send.at[s], xv.at[s, fme], VAL, vsem.at[s, fme], device)

    early, late = mates[:n_seq - 1], mates[n_seq - 1:]
    dd = acc.shape[1]
    parts = cut(dd)

    def wo_rows(k):
        return pl.ds(pl.multiple_of(k * deep, deep), deep)

    def project(s):
        if s == 0:
            weights[0].wait()
        po[s] = jnp.dot(v_send[s], wo[wo_rows(fme), :], preferred_element_type=f32)
        for k, device in early:
            all_here(xv.at[s, k], vsem.at[s, k])
            po[s] += jnp.dot(xv[s, k], wo[wo_rows(k), :], preferred_element_type=f32)
        for k, device in late:
            all_here(xv.at[s, k], vsem.at[s, k])
        for p, (c0, c1) in enumerate(parts):
            total = po[s, :, c0:c1]
            for k, device in late:
                total = total + jnp.dot(xv[s, k], wo[wo_rows(k), c0:c1], preferred_element_type=f32)
            po[s, :, c0:c1] = total
            po_send[s, :, c0:c1] = total.astype(bf16)
            for k in near[::-1]:
                send(po_send.at[s, :, c0:c1], po_recv.at[s, me, :, c0:c1], PO, posem.at[s, p],
                     {"ctx": k})

    for s in range(seqs):
        merge(s)
        project(s)
    all_gone(Q, q_all.at[:len(reach)])
    if paired:
        @pl.when(inner == 1)
        def _():
            all_gone(RELAY, q_all.at[:2])
    all_gone(VU, vu.at[:, :others * lat])
    all_gone(O, o_recv.at[:n * nr - 1])
    all_gone(ST, st_recv.at[:n * nr - 1])
    all_gone(VAL, xv.at[:, :others])
    res_copy.wait()
    gain_copy.wait()
    weights[1].wait()
    weights[2].wait()

    part, crows = all_rows // nr, all_rows // n
    ff = g_acc.shape[1]
    fparts = [(f, min(f + 768, ff)) for f in range(0, ff, 768)]
    sumsq = jnp.zeros((all_rows, 1), f32)
    for p, (c0, c1) in enumerate(parts):
        for s in range(seqs):
            all_here(po_recv.at[s, :n - 1, :, c0:c1], posem.at[s, p])
            total = po[s, :, c0:c1]
            for k in near:
                total = total + po_recv[s, k, :, c0:c1].astype(f32)
            for j in range(nr):
                at = j * rows + s * MTP
                acc[at:at + MTP, c0:c1] = total[j * MTP:(j + 1) * MTP]
        total = res_ref[:, c0:c1].astype(f32) + acc[:, c0:c1]
        for k in range(n):
            resid[k, :, c0:c1] = total[k * crows:(k + 1) * crows]
        sumsq = sumsq + jnp.sum(total * total, axis=1, keepdims=True)
        x = (total * gain_ref[:, c0:c1]).astype(bf16)
        last = p == len(parts) - 1
        if last:
            wide = jnp.broadcast_to(sumsq, (all_rows, 128))
            for k in range(nr):
                ss_send[k] = wide[k * part:(k + 1) * part]
            for k, device in mates:
                send(ss_send.at[k], ss_recv.at[fme], SS, onesem.at[1], device)
        for q, (f0, f1) in enumerate(fparts if last else [(0, ff)]):
            for j, (w, a) in enumerate(((wg, g_acc), (wu, u_acc))):
                y = jnp.dot(x, w[c0:c1, f0:f1], preferred_element_type=f32)
                if p:
                    y = y + a[:, f0:f1]
                if not last:
                    a[:, f0:f1] = y
                    continue
                for k in range(nr):
                    gu_send[k, j, :, f0:f1] = y[k * part:(k + 1) * part].astype(bf16)
            if last:
                for k, device in mates:
                    send(gu_send.at[k, :, :, f0:f1], gu_recv.at[fme, :, :, f0:f1],
                         GU, gusem.at[q], device)
    ss = ss_send[fme]
    all_here(ss_recv.at[:others], onesem.at[1])
    for k, device in mates:
        ss = ss + ss_recv[k]
    inv = lax.rsqrt(ss[:, 0:1] / D + epsilon)
    for q, (f0, f1) in enumerate(fparts):
        gate = gu_send[fme, 0, :, f0:f1].astype(f32)
        up = gu_send[fme, 1, :, f0:f1].astype(f32)
        all_here(gu_recv.at[:others, :, :, f0:f1], gusem.at[q])
        for k, device in mates:
            gate = gate + gu_recv[k, 0, :, f0:f1].astype(f32)
            up = up + gu_recv[k, 1, :, f0:f1].astype(f32)
        gate = gate * inv
        up = up * inv
        h = (gate / (1.0 + jnp.exp(-gate)) * up).astype(bf16)
        h_send[:, f0:f1] = h
        h_all[fme, :, f0:f1] = h
        for k, device in mates:
            send(h_send.at[:, f0:f1], h_all.at[fme, :, f0:f1], H, hsem.at[q], device)
    weights[3].wait()
    for q, (f0, f1) in enumerate(fparts):
        all_here(h_all.at[:others, :, f0:f1], hsem.at[q])
        for k in range(nr):
            h_full[k * part:(k + 1) * part, f0:f1] = h_all[k, :, f0:f1].astype(f32)
        x = h_full[:, f0:f1].astype(bf16)
        last = q == len(fparts) - 1
        for p, (c0, c1) in enumerate(parts if last else [(0, dd)]):
            y = jnp.dot(x, wd[f0:f1, c0:c1], preferred_element_type=f32)
            if q:
                y = y + acc[:, c0:c1]
            if not last:
                acc[:, c0:c1] = y
                continue
            for k in range(n):
                piece = y[k * crows:(k + 1) * crows]
                dn[k, :, c0:c1] = piece
                dn_send[k, :, c0:c1] = piece.astype(bf16)
            for k in near[::-1]:
                send(dn_send.at[k, :, c0:c1], dn_recv.at[me, :, c0:c1], DN, dnsem.at[p], {"ctx": k})
    all_gone(PO, po_recv.at[:, :n - 1])
    all_gone(SS, ss_recv.at[:others])
    all_gone(GU, gu_recv.at[:others])
    all_gone(H, h_all.at[:others])
    for p, (c0, c1) in enumerate(parts):
        result = resid[me, :, c0:c1] + dn[me, :, c0:c1]
        all_here(dn_recv.at[:n - 1, :, c0:c1], dnsem.at[p])
        for k in near:
            result = result + dn_recv[k, :, c0:c1].astype(f32)
        out_ref[:, c0:c1] = result.astype(bf16)
    all_gone(DN, dn_recv.at[:n - 1])


def per_device(sizes, queries, cache, lengths, positions, value_up_weight, out_proj, residual,
               norm_gain, gate_weight, up_weight, down_weight):
    n, n_role, n_seq = sizes
    nr = n_role * n_seq
    rows, heads, width = queries.shape
    seqs, context = cache.shape[:2]
    rope = width - LATENT
    if heads % (8 * nr) or 2 * rope != 128 or n < 2 or nr < 2:
        return per_device_latents(
            sizes, queries, cache, lengths, positions, value_up_weight, out_proj, residual,
            norm_gain, gate_weight, up_weight, down_weight)
    hk = heads // nr
    span = rows * heads // seqs
    extra = span * rope // LATENT
    vdim = value_up_weight.shape[2]
    all_rows, dd = residual.shape
    ff = gate_weight.shape[1]
    part, crows = all_rows // nr, all_rows // n
    nf = -(-ff // 768)
    vmem = pl.BlockSpec(memory_space=pltpu.VMEM)
    smem = pl.BlockSpec(memory_space=pltpu.SMEM)
    hbm = pl.BlockSpec(memory_space=pl.ANY)
    V = pltpu.VMEM
    sems = lambda *k: pltpu.SemaphoreType.DMA(k)
    return pl.pallas_call(
        functools.partial(heads_kernel, n, n_role, n_seq),
        out_shape=pltpu.VMEM((crows, dd), bf16),
        in_specs=[hbm, hbm, smem, smem] + [hbm] * 7,
        out_specs=vmem,
        scratch_shapes=[
            V((seqs, span, width), bf16),
            V((seqs, width + rope, context), bf16),
            V((hk, LATENT, vdim), bf16),
            V((all_rows, dd), bf16),
            V((1, dd), f32),
            V(out_proj.shape, bf16),
            V(gate_weight.shape, bf16),
            V(up_weight.shape, bf16),
            V(down_weight.shape, bf16),
            V((seqs, span + extra, LATENT), bf16),
            V((n, seqs, span + extra, LATENT), bf16),
            V((n, seqs, nr, MTP * hk, LATENT), bf16),
            V((n * nr, seqs, MTP * hk, LATENT), bf16),
            V((n, seqs, 1, 2 * span), f32),
            V((n * nr, seqs, 1, 2 * span), f32),
            V((seqs, span, 128), f32),
            V((hk, seqs, all_rows // seqs, LATENT), f32),
            V((seqs, all_rows // seqs, hk * vdim), bf16),
            V((seqs, nr, all_rows // seqs, hk * vdim), bf16),
            V((all_rows, dd), f32),
            V((seqs, all_rows // seqs, dd), f32),
            V((seqs, all_rows // seqs, dd), bf16),
            V((seqs, n, all_rows // seqs, dd), bf16),
            V((n, crows, dd), f32),
            V((nr, part, 128), f32),
            V((nr, part, 128), f32),
            V((all_rows, ff), f32),
            V((all_rows, ff), f32),
            V((nr, 2, part, ff), bf16),
            V((nr, 2, part, ff), bf16),
            V((part, ff), bf16),
            V((nr, part, ff), bf16),
            V((all_rows, ff), f32),
            V((n, crows, dd), f32),
            V((n, crows, dd), bf16),
            V((n, crows, dd), bf16),
            sems(6),
            sems(4),
            sems(seqs, n),
            sems(11),
            sems(seqs),
            sems(seqs),
            sems(seqs, nr),
            sems(seqs, 2),
            sems(nf),
            sems(nf),
            sems(2),
            sems(2),
        ],
        compiler_params=pltpu.CompilerParams(
            collective_id=0, has_side_effects=True, vmem_limit_bytes=VMEM_BYTES),
        name="layer",
    )(queries.reshape(seqs, span, width), cache.transpose(0, 2, 1), lengths, positions, value_up_weight,
      residual, norm_gain, out_proj, gate_weight, up_weight, down_weight)


def solution(mesh):
    placed = (
        P(("groups", "role", "seq"), "ctx", None),
        P(("groups", "role", "seq"), "ctx", None),
        P(("groups", "role", "seq")),
        P(("groups", "role", "seq")),
        P("ctx", ("role", "seq"), None),
        P("ctx", ("role", "seq")),
        P("groups", ("role", "seq")),
        P(("role", "seq")),
        P(("role", "seq"), "ctx"),
        P(("role", "seq"), "ctx"),
        P("ctx", ("role", "seq")),
    )
    sizes = (mesh.shape["ctx"], mesh.shape["role"], mesh.shape["seq"])
    return jax.shard_map(
        functools.partial(per_device, sizes),
        mesh=mesh,
        in_specs=placed,
        out_specs=P(("groups", "ctx"), ("role", "seq")),
        check_vma=False,
    )
```

```python
import functools

import jax
import jax.numpy as jnp
from jax import lax
from jax.experimental import pallas as pl
from jax.experimental.pallas import tpu as pltpu
from jax.sharding import PartitionSpec as P

D = 7168
LATENT = 512
MTP = 2

softmax_scale = 0.07216878364870323
epsilon = 1e-06
MESH = pl.DeviceIdType.MESH
VMEM_BYTES = 60 * 1024 * 1024
f32, bf16 = jnp.float32, jnp.bfloat16


def ctx_group(n):
    me = lax.axis_index("ctx")

    def peer(d):
        k = lax.rem(me + d, n)
        return k, {"ctx": k}

    return me, peer


def feature_group(n_role, n_seq):
    n = n_role * n_seq
    me = lax.axis_index("role") * n_seq + lax.axis_index("seq")

    def peer(d):
        k = lax.rem(me + d, n)
        return k, {"role": k // n_seq, "seq": lax.rem(k, n_seq)}

    return me, peer


def enter(groups):
    barrier = pltpu.get_barrier_semaphore()
    count = 0
    for n, peer in groups:
        for d in range(1, n):
            pl.semaphore_signal(barrier, inc=1, device_id=peer(d)[1], device_id_type=MESH)
            count += 1
    pl.semaphore_wait(barrier, count)


def remote(src, dst, send, recv, device):
    return pltpu.make_async_remote_copy(
        src_ref=src, dst_ref=dst, send_sem=send, recv_sem=recv,
        device_id=device, device_id_type=MESH,
    )


def attend(n, n_role, n_seq, q_ref, cache_ref, cache_copy, len_ref, pos_ref, out_ref,
           q_all, o_send, o_recv, s_send, s_recv, a_send, sems):
    nr = n_role * n_seq
    me, peer = ctx_group(n)
    fme, fpeer = feature_group(n_role, n_seq)
    seqs, _, context = cache_ref.shape
    rows = q_ref.shape[1]
    heads = rows // MTP

    q_copies = []
    for s in range(seqs):
        for d in range(1, n):
            c = remote(q_ref.at[s], q_all.at[me, s], sems.at[s, d], sems.at[seqs + s, d],
                       peer(d)[1])
            c.start()
            q_copies.append(c)

    places = me * context + lax.broadcasted_iota(jnp.int32, (rows, context), 1)
    first = lax.broadcasted_iota(jnp.int32, (rows, context), 0) < heads
    lives = []
    for s in range(seqs):
        limit = jnp.where(first, pos_ref[MTP * s], pos_ref[MTP * s + 1])
        lives.append((places < len_ref[s]) & (places <= limit))

    lane = lax.broadcasted_iota(jnp.int32, (rows, 128), 1)

    def block(q, s):
        keys = cache_ref[s]
        scores = jnp.dot(q, keys, preferred_element_type=f32) * softmax_scale
        live = lives[s]
        top = jnp.max(jnp.where(live, scores, -1e30), axis=1, keepdims=True)
        probs = jnp.exp(jnp.where(live, scores - top, -1e30)).astype(bf16)
        total = jnp.sum(probs.astype(f32), axis=1, keepdims=True)
        out = lax.dot_general(
            probs, keys[:LATENT], (((1,), (1,)), ((), ())), preferred_element_type=f32)
        return out, top, total

    cache_copy.wait()
    own = [block(q_ref[s], s) for s in range(seqs)]
    o_copies, s_copies = {}, {}
    for s in range(seqs):
        for d in range(1, n):
            src, device = peer(n - d)
            remote(q_ref.at[s], q_all.at[src, s], sems.at[s, d], sems.at[seqs + s, d],
                   device).wait_recv()
            o, top, total = block(q_all[src, s], s)
            o_send[d, s] = o.astype(bf16)
            s_send[d, s] = jnp.where(lane == 0, top, total).T[0:8]
            c = remote(o_send.at[d, s], o_recv.at[d, s], sems.at[2 * seqs + s, d],
                       sems.at[3 * seqs + s, d], device)
            c.start()
            o_copies[s, d] = c
            c = remote(s_send.at[d, s], s_recv.at[d, s], sems.at[4 * seqs + s, d],
                       sems.at[5 * seqs + s, d], device)
            c.start()
            s_copies[s, d] = c
    for c in q_copies:
        c.wait_send()

    heads = rows // MTP
    merged = []
    for s in range(seqs):
        own_o, top, total = own[s]
        tops, totals = [top], [total]
        for d in range(1, n):
            s_copies[s, d].wait()
            back = jnp.concatenate([s_recv[d, s]] * 16, axis=0).T
            tops.append(back[:, 0:1])
            totals.append(back[:, 1:2])
        highest = functools.reduce(jnp.maximum, tops)
        factors = [jnp.exp(t - highest) for t in tops]
        denom = sum(f * t for f, t in zip(factors, totals))
        numer = factors[0] * own_o
        for d in range(1, n):
            o_copies[s, d].wait()
            numer = numer + factors[d] * o_recv[d, s].astype(f32)
        merged.append((numer / denom).astype(bf16))

    part = LATENT // nr
    for k in range(nr):
        for r in range(seqs * MTP):
            t = r % MTP
            a_send[k, r] = merged[r // MTP][t * heads:(t + 1) * heads, k * part:(k + 1) * part]
    copies = []
    for d in range(1, nr):
        k, device = fpeer(d)
        c = remote(a_send.at[k], out_ref.at[fme], sems.at[6 * seqs, d], sems.at[7 * seqs, d], device)
        c.start()
        copies.append(c)
    out_ref[fme] = a_send[fme]
    for d in range(1, nr):
        k, device = fpeer(nr - d)
        copies[d - 1].wait_send()
        remote(a_send.at[k], out_ref.at[k], sems.at[6 * seqs, d], sems.at[7 * seqs, d],
               device).wait_recv()


def layer_kernel(n, n_role, n_seq, q_ref, cache_hbm, len_ref, pos_ref, vu_hbm, res_ref, gain_ref,
                 wo_hbm, wg_hbm, wu_hbm, wd_hbm,
                 out_ref, cache, vu, q_all, o_send, o_recv, s_send, s_recv, a_send, a_all, a_head,
                 mixed, pv_ref, wo, wg, wu, wd, pv_recv, v_send, v_all, v_full, acc, po_send,
                 po_recv, resid, xg_ref, g_acc, u_acc, gu_send, gu_recv, ss_send, ss_recv, h_send,
                 h_all, h_full, dn, dn_send, dn_recv, wsem, lsem, asems, sems):
    nr = n_role * n_seq
    me, peer = ctx_group(n)
    fme, fpeer = feature_group(n_role, n_seq)

    cache_copy = pltpu.make_async_copy(cache_hbm, cache, lsem.at[0])
    cache_copy.start()
    vu_copy = pltpu.make_async_copy(vu_hbm, vu, lsem.at[1])
    vu_copy.start()
    weights = []
    for which, (hbm, vmem) in enumerate(((wo_hbm, wo), (wg_hbm, wg), (wu_hbm, wu), (wd_hbm, wd))):
        depth = vmem.shape[1]

        def fetch(i, hbm=hbm, vmem=vmem, depth=depth, which=which):
            return pltpu.make_async_copy(
                hbm.at[pl.ds(i * depth, depth)], vmem.at[i], wsem.at[which, i])

        weights.append((fetch, vmem))
    for fetch, vmem in weights:
        for i in range(vmem.shape[0]):
            fetch(i).start()
    enter(((n, peer), (nr, fpeer)))
    attend(n, n_role, n_seq, q_ref, cache, cache_copy, len_ref, pos_ref, a_all,
           q_all, o_send, o_recv, s_send, s_recv, a_send, asems)
    rows, heads = a_all.shape[1:3]
    for j in range(nr):
        for r in range(rows):
            a_head[:, j * rows + r, :] = a_all[j, r].astype(f32)
    vu_copy.wait()
    vdim = vu.shape[2]
    for h in range(heads):
        mixed[:, h * vdim:(h + 1) * vdim] = jnp.dot(
            a_head[h].astype(bf16), vu[h], preferred_element_type=f32)
    for k in range(nr):
        pv_ref[k] = mixed[k * rows:(k + 1) * rows, :].astype(bf16)

    def matmul(x_ref, *pairs):
        chunks, depth, _ = weights[pairs[0][0]][1].shape
        for which, acc_ref in pairs:
            fetch, vmem = weights[which]
            fetch(0).wait()
            acc_ref[...] = jnp.dot(x_ref[:, :depth], vmem[0], preferred_element_type=f32)
        if chunks == 1:
            return

        @pl.loop(1, chunks)
        def _(i):
            x = x_ref[:, pl.ds(pl.multiple_of(i * depth, depth), depth)]
            for which, acc_ref in pairs:
                fetch, vmem = weights[which]
                fetch(i).wait()
                acc_ref[...] += jnp.dot(x, vmem[i], preferred_element_type=f32)

    def swap(size, peer_of, chunk, recv, row):
        copies = []
        for d in range(1, size):
            k, device = peer_of(d)
            c = remote(chunk(k), recv.at[d], sems.at[row, d], sems.at[row + 1, d], device)
            c.start()
            copies.append(c)
        return copies

    def gather(size, my, peer_of, send, full, row):
        copies = []
        for d in range(1, size):
            c = remote(send, full.at[my], sems.at[row, d], sems.at[row + 1, d], peer_of(d)[1])
            c.start()
            copies.append(c)
        full[my] = send[...]
        for d in range(1, size):
            k, device = peer_of(size - d)
            copies[d - 1].wait_send()
            remote(send, full.at[k], sems.at[row, d], sems.at[row + 1, d], device).wait_recv()

    part = res_ref.shape[0] // nr
    copies = swap(nr, fpeer, lambda k: pv_ref.at[k], pv_recv, 0)
    vals = pv_ref[fme].astype(f32)
    for d in range(1, nr):
        copies[d - 1].wait()
        vals = vals + pv_recv[d].astype(f32)
    v_send[...] = vals.astype(bf16)
    gather(nr, fme, fpeer, v_send, v_all, 2)
    for k in range(nr):
        acc_rows = v_all[k].astype(f32)
        v_full[k * part:(k + 1) * part, :] = acc_rows
    x_ref = xg_ref[0]
    x_ref[...] = v_full[...].astype(bf16)
    matmul(x_ref, (0, acc))

    po_send[...] = acc[...].astype(bf16)
    copies = swap(n, peer, lambda k: po_send, po_recv, 4)
    total = res_ref[...].astype(f32) + acc[...]
    for d in range(1, n):
        copies[d - 1].wait()
        total = total + po_recv[d].astype(f32)
    crows = res_ref.shape[0] // n
    for k in range(n):
        resid[k] = total[k * crows:(k + 1) * crows]
    sumsq = jnp.sum(total * total, axis=1, keepdims=True)
    sumsq = jnp.broadcast_to(sumsq, (total.shape[0], 128))
    for k in range(nr):
        ss_send[k] = sumsq[k * part:(k + 1) * part]
    s_copies = swap(nr, fpeer, lambda k: ss_send.at[k], ss_recv, 6)
    x_ref = xg_ref[1]
    x_ref[...] = (total * gain_ref[...]).astype(bf16)
    matmul(x_ref, (1, g_acc), (2, u_acc))

    for j, a in enumerate((g_acc, u_acc)):
        for k in range(nr):
            gu_send[k, j] = a[k * part:(k + 1) * part, :].astype(bf16)
    copies = swap(nr, fpeer, lambda k: gu_send.at[k], gu_recv, 8)
    ss = ss_send[fme]
    for d in range(1, nr):
        s_copies[d - 1].wait()
        ss = ss + ss_recv[d]
    inv = lax.rsqrt(ss[:, 0:1] / D + epsilon)
    gate = gu_send[fme, 0].astype(f32)
    up = gu_send[fme, 1].astype(f32)
    for d in range(1, nr):
        copies[d - 1].wait()
        gate = gate + gu_recv[d, 0].astype(f32)
        up = up + gu_recv[d, 1].astype(f32)
    gate = gate * inv
    up = up * inv
    h_send[...] = (gate / (1.0 + jnp.exp(-gate)) * up).astype(bf16)
    gather(nr, fme, fpeer, h_send, h_all, 10)
    for k in range(nr):
        h_full[k * part:(k + 1) * part, :] = h_all[k].astype(f32)
    x_ref = xg_ref[2]
    x_ref[...] = h_full[...].astype(bf16)
    matmul(x_ref, (3, acc))

    for k in range(n):
        piece = acc[k * crows:(k + 1) * crows, :]
        dn[k] = piece
        dn_send[k] = piece.astype(bf16)
    copies = swap(n, peer, lambda k: dn_send.at[k], dn_recv, 12)
    result = resid[me] + dn[me]
    for d in range(1, n):
        copies[d - 1].wait()
        result = result + dn_recv[d].astype(f32)
    out_ref[...] = result.astype(bf16)


def chunk_of(depth):
    for size in (1024, 768, 512, 256):
        if depth % size == 0:
            return size
    return depth


def per_device_latents(sizes, queries, cache, lengths, positions, value_up_weight, out_proj, residual,
               norm_gain, gate_weight, up_weight, down_weight):
    n, n_role, n_seq = sizes
    nr = n_role * n_seq
    rows, heads, width = queries.shape
    seqs = cache.shape[0]
    span = rows * heads // seqs
    lat = LATENT // nr
    vmem = pl.BlockSpec(memory_space=pltpu.VMEM)
    smem = pl.BlockSpec(memory_space=pltpu.SMEM)
    hbm = pl.BlockSpec(memory_space=pl.ANY)
    most = max(n, nr)
    sems = lambda k: pltpu.SemaphoreType.DMA((k, most))
    vwide = heads * value_up_weight.shape[2]
    all_rows, dd = residual.shape
    ff = gate_weight.shape[1]
    part, crows = all_rows // nr, all_rows // n

    def held(w):
        size = chunk_of(w.shape[0])
        return pltpu.VMEM((w.shape[0] // size, size, w.shape[1]), bf16)

    ws = (out_proj, gate_weight, up_weight, down_weight)
    most_chunks = max(w.shape[0] // chunk_of(w.shape[0]) for w in ws)
    V = pltpu.VMEM
    return pl.pallas_call(
        functools.partial(layer_kernel, n, n_role, n_seq),
        out_shape=jax.ShapeDtypeStruct((crows, dd), bf16),
        in_specs=[vmem, hbm, smem, smem, hbm, vmem, vmem] + [hbm] * 4,
        out_specs=vmem,
        scratch_shapes=[
            V((cache.shape[0], width, cache.shape[1]), bf16),
            V(value_up_weight.shape, bf16),
            V((n, seqs, span, width), bf16),
            V((n, seqs, span, LATENT), bf16),
            V((n, seqs, span, LATENT), bf16),
            V((n, seqs, 8, span), f32),
            V((n, seqs, 8, span), f32),
            V((nr, rows, heads, lat), bf16),
            V((nr, rows, heads, lat), bf16),
            V((heads, all_rows, lat), f32),
            V((all_rows, vwide), f32),
            V((nr, part, vwide), bf16),
            *[held(w) for w in ws],
            V((nr, part, vwide), bf16),
            V((part, vwide), bf16),
            V((nr, part, vwide), bf16),
            V((all_rows, vwide), f32),
            V((all_rows, dd), f32),
            V((all_rows, dd), bf16),
            V((n, all_rows, dd), bf16),
            V((n, crows, dd), f32),
            [V((all_rows, vwide), bf16), V((all_rows, dd), bf16), V((all_rows, ff), bf16)],
            V((all_rows, ff), f32),
            V((all_rows, ff), f32),
            V((nr, 2, part, ff), bf16),
            V((nr, 2, part, ff), bf16),
            V((nr, part, 128), f32),
            V((nr, part, 128), f32),
            V((part, ff), bf16),
            V((nr, part, ff), bf16),
            V((all_rows, ff), f32),
            V((n, crows, dd), f32),
            V((n, crows, dd), bf16),
            V((n, crows, dd), bf16),
            pltpu.SemaphoreType.DMA((4, most_chunks)),
            pltpu.SemaphoreType.DMA((2,)),
            sems(8 * seqs),
            sems(14),
        ],
        compiler_params=pltpu.CompilerParams(
            collective_id=0, has_side_effects=True, vmem_limit_bytes=VMEM_BYTES),
        name="layer",
    )(queries.reshape(seqs, span, width), cache.transpose(0, 2, 1), lengths, positions, value_up_weight,
      residual, norm_gain.reshape(1, dd), *ws)


LOG2E = 1.4426950408889634


def by_distance(n, me):
    found = []
    for i in range(n - 1):
        k = jnp.int32(0)
        for z in range(n):
            others = sorted((j for j in range(n) if j != z), key=lambda j: (abs(j - z), j))
            k = jnp.where(me == z, others[i], k)
        found.append(k)
    return found


def cut(width):
    unit = 256 if width % 256 == 0 else 128
    if width % unit or width < 2 * unit:
        return [(0, width)]
    first = width // unit // 2 * unit
    return [(0, first), (first, width)]


def heads_kernel(n, n_role, n_seq, q_hbm, cache_hbm, len_ref, pos_ref, vu_hbm, res_hbm, gain_hbm,
                 wo_hbm, wg_hbm, wu_hbm, wd_hbm, out_ref,
                 q_ref, cache, vu, res_ref, gain_ref, wo, wg, wu, wd,
                 q_send, q_all, o_send, o_recv, st_send, st_recv, w_ref,
                 a_head, v_send, xv, acc, po, po_send, po_recv, resid, ss_send, ss_recv,
                 g_acc, u_acc, gu_send, gu_recv, h_send, h_all, h_full, dn, dn_send, dn_recv,
                 lsem, wsem, qsem, gone, osem, stsem, vsem, posem, gusem, hsem, dnsem, onesem):
    nr = n_role * n_seq
    me = lax.axis_index("ctx")
    role, seq = lax.axis_index("role"), lax.axis_index("seq")
    fme = role * n_seq + seq
    near = by_distance(n, me)
    mates = []
    for dr in range(n_role):
        for ds in range(n_seq):
            if dr or ds:
                r, s = lax.rem(role + dr, n_role), lax.rem(seq + ds, n_seq)
                mates.append((r * n_seq + s, {"role": r, "seq": s}))
    seqs, span, width = q_ref.shape
    context = cache.shape[2]
    heads = span // MTP
    hk = heads // nr
    rope = width - LATENT
    lat = LATENT // nr
    own = n - 1
    extra = span * rope // LATENT

    paired = n == 4
    if paired:
        beside = me + 1 - 2 * lax.rem(me, 2)
        across = 2 - me // 2
        beyond = 3 - 3 * (me // 2)
        inner = lax.rem((me + 1) // 2, 2)
        reach = [beside, across]
    else:
        reach = near[::-1]

    q_copy = pltpu.make_async_copy(q_hbm, q_ref, lsem.at[0])
    q_copy.start()
    cache_copies = [
        pltpu.make_async_copy(cache_hbm, cache.at[:, pl.ds(0, width), :], lsem.at[1]),
        pltpu.make_async_copy(cache_hbm.at[:, pl.ds(LATENT, rope), :],
                              cache.at[:, pl.ds(width, rope), :], lsem.at[2]),
    ]
    for c in cache_copies:
        c.start()
    barrier = pltpu.get_barrier_semaphore()
    if paired:
        pl.semaphore_signal(barrier, inc=1, device_id={"ctx": beside}, device_id_type=MESH)

        @pl.when(inner == 1)
        def _():
            for k in (across, beyond):
                pl.semaphore_signal(barrier, inc=1, device_id={"ctx": k}, device_id_type=MESH)
    else:
        for k in near:
            pl.semaphore_signal(barrier, inc=1, device_id={"ctx": k}, device_id_type=MESH)
    for _, device in mates:
        pl.semaphore_signal(barrier, inc=1, device_id=device, device_id_type=MESH)
    vu_own = pltpu.make_async_copy(
        vu_hbm.at[pl.ds(pl.multiple_of(fme * hk, hk), hk)],
        vu.at[:, pl.ds(pl.multiple_of(fme * lat, lat), lat), :], lsem.at[3])
    vu_own.start()
    res_copy = pltpu.make_async_copy(res_hbm, res_ref, lsem.at[4])
    res_copy.start()
    gain_copy = pltpu.make_async_copy(gain_hbm, gain_ref.at[0], lsem.at[5])
    gain_copy.start()

    q_copy.wait()
    for s in range(seqs):
        qn, qr = [], []
        for k in range(nr):
            for t in range(MTP):
                at = t * heads + k * hk
                rows = q_ref[s, at:at + hk, :].astype(f32)
                qn.append(rows[:, :LATENT])
                qr.append(rows[:, LATENT:])
        q_send[s, :span] = jnp.concatenate(qn, axis=0).astype(bf16)
        qr = jnp.concatenate(qr, axis=0)
        qr = jnp.concatenate([qr[:span // 2], qr[span // 2:]], axis=1)
        q_send[s, span:] = jnp.concatenate(
            [qr[i:i + extra] for i in range(0, span // 2, extra)], axis=1).astype(bf16)
    weights = []
    for which, (hbm, vmem) in enumerate(((wo_hbm, wo), (wg_hbm, wg), (wu_hbm, wu), (wd_hbm, wd))):
        weights.append(pltpu.make_async_copy(hbm, vmem, wsem.at[which]))
    for c in weights:
        c.start()
    pl.semaphore_wait(barrier, len(reach) + len(mates))

    Q, RELAY, VU, O, ST, VAL, PO, SS, GU, H, DN = range(11)

    def send(src, dst, kind, recv_sem, device):
        remote(src, dst, gone.at[kind], recv_sem, device).start()

    def all_gone(kind, like):
        remote(like, like, gone.at[kind], gone.at[kind], {"ctx": near[0]}).wait_send()

    def all_here(like, recv_sem):
        remote(like, like, gone.at[0], recv_sem, {"ctx": near[0]}).wait_recv()

    def take(b, s):
        all_here(q_all.at[b, s], qsem.at[s, b])

    for s in range(seqs):
        for k in reach:
            send(q_send.at[s], q_all.at[me, s], Q, qsem.at[s, me], {"ctx": k})
    for k, device in mates:
        send(vu_hbm.at[pl.ds(pl.multiple_of(k * hk, hk), hk)],
             vu.at[:, pl.ds(pl.multiple_of(fme * lat, lat), lat), :], VU, onesem.at[0], device)

    column = lax.broadcasted_iota(jnp.int32, (span, context), 1)
    row = lax.broadcasted_iota(jnp.int32, (span, 1), 0)
    even = lax.rem(row, MTP * hk) < hk
    lane = lax.broadcasted_iota(jnp.int32, (span, 128), 1)
    half = lax.broadcasted_iota(jnp.int32, (span // 2, 2 * rope), 1) < rope
    ends = []
    for s in range(seqs):
        limit = jnp.where(even, pos_ref[MTP * s], pos_ref[MTP * s + 1]) + 1
        ends.append(jnp.minimum(limit, len_ref[s]) - me * context)

    def block(queries, s, slot):
        qn, qr = queries[:span], queries[span:].astype(f32)
        qr = jnp.concatenate([qr[:, i:i + 128] for i in range(0, LATENT, 128)], axis=0)
        zero = jnp.zeros_like(qr)
        q = jnp.concatenate(
            [qn, jnp.concatenate([jnp.where(half, qr, zero), jnp.where(half, zero, qr)],
                                 axis=0).astype(bf16)],
            axis=1)
        keys = cache[s]
        scores = jnp.dot(q, keys, preferred_element_type=f32) * (softmax_scale * LOG2E)
        scores = jnp.where(column < ends[s], scores, -1e30)
        top = jnp.maximum(jnp.max(scores, axis=1, keepdims=True), -1e29)
        probs = jnp.exp2(scores - top).astype(bf16)
        total = jnp.sum(probs.astype(f32), axis=1, keepdims=True)
        out = lax.dot_general(
            probs, keys[:LATENT], (((1,), (1,)), ((), ())), preferred_element_type=f32)
        out = out.astype(bf16)
        for k in range(nr):
            o_send[slot, s, k] = out[k * MTP * hk:(k + 1) * MTP * hk]
        stats = jnp.where(lane == 0, top, total).T
        st_send[slot, s] = jnp.concatenate([stats[0:1], stats[1:2]], axis=1)

    mine = me * nr + fme
    for c in cache_copies:
        c.wait()
    def home(s):
        block(q_send[s], s, own)
        for k, device in mates:
            send(o_send.at[own, s, k], o_recv.at[mine, s], O, osem.at[s], device)
            send(st_send.at[own, s], st_recv.at[mine, s], ST, stsem.at[s], device)
        for c in (
            pltpu.make_async_copy(o_send.at[own, s, fme], o_recv.at[mine, s], osem.at[s]),
            pltpu.make_async_copy(st_send.at[own, s], st_recv.at[mine, s], stsem.at[s]),
        ):
            c.start()

    def answer(b, s, slot):
        block(q_all[b, s], s, slot)
        for k in range(nr):
            device = {"ctx": b, "role": k // n_seq, "seq": k % n_seq}
            send(o_send.at[slot, s, k], o_recv.at[mine, s], O, osem.at[s], device)
            send(st_send.at[slot, s], st_recv.at[mine, s], ST, stsem.at[s], device)

    if paired:
        def relay(b, s):
            @pl.when(inner == 1)
            def _():
                take(b, s)
                send(q_all.at[b, s], q_all.at[b, s], RELAY, qsem.at[s, b], {"ctx": beside})

        def take_outer(b, s):
            @pl.when(inner == 0)
            def _():
                take(b, s)

        home(0)
        relay(across, 0)
        for s in range(seqs):
            take(beside, s)
            answer(beside, s, 0)
            if s == 0:
                relay(beyond, 0)
            if s + 1 < seqs:
                relay(across, s + 1)
            take_outer(across, s)
            answer(across, s, 1)
            if s + 1 < seqs:
                relay(beyond, s + 1)
            take_outer(beyond, s)
            answer(beyond, s, 2)
        for s in range(1, seqs):
            home(s)
    else:
        for s in range(seqs):
            home(s)
            for i, b in enumerate(near):
                take(b, s)
                answer(b, s, i)

    rows = seqs * MTP
    all_rows = nr * rows
    mine_at = pl.ds(pl.multiple_of(fme * MTP * hk, MTP * hk), MTP * hk)
    vdim = vu.shape[2]
    deep = hk * vdim
    others = len(mates)

    def merge(s):
        all_here(st_recv.at[:, s], stsem.at[s])
        tops, totals = [], []
        for b in range(n):
            stats = jnp.concatenate([st_recv[b * nr + j, s] for j in range(nr)], axis=0)
            tops.append(stats[:, :span])
            totals.append(stats[:, span:])
        highest = functools.reduce(jnp.maximum, tops)
        factors = [jnp.exp2(t - highest) for t in tops]
        denom = sum(f * t for f, t in zip(factors, totals))
        shares = jnp.concatenate([f / denom for f in factors], axis=0)
        copies = -(-128 // (n * nr))
        shares = jnp.concatenate([shares] * copies, axis=0)[:128]
        w_ref[s] = shares.T
        share = w_ref[s, mine_at, :]
        all_here(o_recv.at[:, s], osem.at[s])
        for j in range(nr):
            mixed = None
            for b in range(n):
                i = b * nr + j
                term = share[:, i:i + 1] * o_recv[i, s].astype(f32)
                mixed = term if mixed is None else mixed + term
            for t in range(MTP):
                a_head[:, s, j * MTP + t, :] = mixed[t * hk:(t + 1) * hk]
        if s == 0:
            vu_own.wait()
            all_here(vu.at[:, :others * lat], onesem.at[0])
        for h in range(hk):
            v_send[s, :, h * vdim:(h + 1) * vdim] = jnp.dot(
                a_head[h, s].astype(bf16), vu[h], preferred_element_type=f32).astype(bf16)
        for k, device in mates:
            send(v_send.at[s], xv.at[s, fme], VAL, vsem.at[s, fme], device)

    early, late = mates[:n_seq - 1], mates[n_seq - 1:]
    dd = acc.shape[1]
    parts = cut(dd)

    def wo_rows(k):
        return pl.ds(pl.multiple_of(k * deep, deep), deep)

    def project(s):
        if s == 0:
            weights[0].wait()
        po[s] = jnp.dot(v_send[s], wo[wo_rows(fme), :], preferred_element_type=f32)
        for k, device in early:
            all_here(xv.at[s, k], vsem.at[s, k])
            po[s] += jnp.dot(xv[s, k], wo[wo_rows(k), :], preferred_element_type=f32)
        for k, device in late:
            all_here(xv.at[s, k], vsem.at[s, k])
        for p, (c0, c1) in enumerate(parts):
            total = po[s, :, c0:c1]
            for k, device in late:
                total = total + jnp.dot(xv[s, k], wo[wo_rows(k), c0:c1], preferred_element_type=f32)
            po[s, :, c0:c1] = total
            po_send[s, :, c0:c1] = total.astype(bf16)
            for k in near[::-1]:
                send(po_send.at[s, :, c0:c1], po_recv.at[s, me, :, c0:c1], PO, posem.at[s, p],
                     {"ctx": k})

    for s in range(seqs):
        merge(s)
        project(s)
    all_gone(Q, q_all.at[:len(reach)])
    if paired:
        @pl.when(inner == 1)
        def _():
            all_gone(RELAY, q_all.at[:2])
    all_gone(VU, vu.at[:, :others * lat])
    all_gone(O, o_recv.at[:n * nr - 1])
    all_gone(ST, st_recv.at[:n * nr - 1])
    all_gone(VAL, xv.at[:, :others])
    res_copy.wait()
    gain_copy.wait()
    weights[1].wait()
    weights[2].wait()

    part, crows = all_rows // nr, all_rows // n
    ff = g_acc.shape[1]
    fparts = [(f, min(f + 768, ff)) for f in range(0, ff, 768)]
    sumsq = jnp.zeros((all_rows, 1), f32)
    for p, (c0, c1) in enumerate(parts):
        for s in range(seqs):
            all_here(po_recv.at[s, :n - 1, :, c0:c1], posem.at[s, p])
            total = po[s, :, c0:c1]
            for k in near:
                total = total + po_recv[s, k, :, c0:c1].astype(f32)
            for j in range(nr):
                at = j * rows + s * MTP
                acc[at:at + MTP, c0:c1] = total[j * MTP:(j + 1) * MTP]
        total = res_ref[:, c0:c1].astype(f32) + acc[:, c0:c1]
        for k in range(n):
            resid[k, :, c0:c1] = total[k * crows:(k + 1) * crows]
        sumsq = sumsq + jnp.sum(total * total, axis=1, keepdims=True)
        x = (total * gain_ref[:, c0:c1]).astype(bf16)
        last = p == len(parts) - 1
        if last:
            wide = jnp.broadcast_to(sumsq, (all_rows, 128))
            for k in range(nr):
                ss_send[k] = wide[k * part:(k + 1) * part]
            for k, device in mates:
                send(ss_send.at[k], ss_recv.at[fme], SS, onesem.at[1], device)
        for q, (f0, f1) in enumerate(fparts if last else [(0, ff)]):
            for j, (w, a) in enumerate(((wg, g_acc), (wu, u_acc))):
                y = jnp.dot(x, w[c0:c1, f0:f1], preferred_element_type=f32)
                if p:
                    y = y + a[:, f0:f1]
                if not last:
                    a[:, f0:f1] = y
                    continue
                for k in range(nr):
                    gu_send[k, j, :, f0:f1] = y[k * part:(k + 1) * part].astype(bf16)
            if last:
                for k, device in mates:
                    send(gu_send.at[k, :, :, f0:f1], gu_recv.at[fme, :, :, f0:f1],
                         GU, gusem.at[q], device)
    ss = ss_send[fme]
    all_here(ss_recv.at[:others], onesem.at[1])
    for k, device in mates:
        ss = ss + ss_recv[k]
    inv = lax.rsqrt(ss[:, 0:1] / D + epsilon)
    for q, (f0, f1) in enumerate(fparts):
        gate = gu_send[fme, 0, :, f0:f1].astype(f32)
        up = gu_send[fme, 1, :, f0:f1].astype(f32)
        all_here(gu_recv.at[:others, :, :, f0:f1], gusem.at[q])
        for k, device in mates:
            gate = gate + gu_recv[k, 0, :, f0:f1].astype(f32)
            up = up + gu_recv[k, 1, :, f0:f1].astype(f32)
        gate = gate * inv
        up = up * inv
        h = (gate / (1.0 + jnp.exp(-gate)) * up).astype(bf16)
        h_send[:, f0:f1] = h
        h_all[fme, :, f0:f1] = h
        for k, device in mates:
            send(h_send.at[:, f0:f1], h_all.at[fme, :, f0:f1], H, hsem.at[q], device)
    weights[3].wait()
    for q, (f0, f1) in enumerate(fparts):
        all_here(h_all.at[:others, :, f0:f1], hsem.at[q])
        for k in range(nr):
            h_full[k * part:(k + 1) * part, f0:f1] = h_all[k, :, f0:f1].astype(f32)
        x = h_full[:, f0:f1].astype(bf16)
        last = q == len(fparts) - 1
        for p, (c0, c1) in enumerate(parts if last else [(0, dd)]):
            y = jnp.dot(x, wd[f0:f1, c0:c1], preferred_element_type=f32)
            if q:
                y = y + acc[:, c0:c1]
            if not last:
                acc[:, c0:c1] = y
                continue
            for k in range(n):
                piece = y[k * crows:(k + 1) * crows]
                dn[k, :, c0:c1] = piece
                dn_send[k, :, c0:c1] = piece.astype(bf16)
            for k in near[::-1]:
                send(dn_send.at[k, :, c0:c1], dn_recv.at[me, :, c0:c1], DN, dnsem.at[p], {"ctx": k})
    all_gone(PO, po_recv.at[:, :n - 1])
    all_gone(SS, ss_recv.at[:others])
    all_gone(GU, gu_recv.at[:others])
    all_gone(H, h_all.at[:others])
    for p, (c0, c1) in enumerate(parts):
        result = resid[me, :, c0:c1] + dn[me, :, c0:c1]
        all_here(dn_recv.at[:n - 1, :, c0:c1], dnsem.at[p])
        for k in near:
            result = result + dn_recv[k, :, c0:c1].astype(f32)
        out_ref[:, c0:c1] = result.astype(bf16)
    all_gone(DN, dn_recv.at[:n - 1])


def per_device(sizes, queries, cache, lengths, positions, value_up_weight, out_proj, residual,
               norm_gain, gate_weight, up_weight, down_weight):
    n, n_role, n_seq = sizes
    nr = n_role * n_seq
    rows, heads, width = queries.shape
    seqs, context = cache.shape[:2]
    rope = width - LATENT
    if heads % (8 * nr) or 2 * rope != 128 or n < 2 or nr < 2:
        return per_device_latents(
            sizes, queries, cache, lengths, positions, value_up_weight, out_proj, residual,
            norm_gain, gate_weight, up_weight, down_weight)
    hk = heads // nr
    span = rows * heads // seqs
    extra = span * rope // LATENT
    vdim = value_up_weight.shape[2]
    all_rows, dd = residual.shape
    ff = gate_weight.shape[1]
    part, crows = all_rows // nr, all_rows // n
    nf = -(-ff // 768)
    vmem = pl.BlockSpec(memory_space=pltpu.VMEM)
    smem = pl.BlockSpec(memory_space=pltpu.SMEM)
    hbm = pl.BlockSpec(memory_space=pl.ANY)
    V = pltpu.VMEM
    sems = lambda *k: pltpu.SemaphoreType.DMA(k)
    return pl.pallas_call(
        functools.partial(heads_kernel, n, n_role, n_seq),
        out_shape=pltpu.VMEM((crows, dd), bf16),
        in_specs=[hbm, hbm, smem, smem] + [hbm] * 7,
        out_specs=vmem,
        scratch_shapes=[
            V((seqs, span, width), bf16),
            V((seqs, width + rope, context), bf16),
            V((hk, LATENT, vdim), bf16),
            V((all_rows, dd), bf16),
            V((1, dd), f32),
            V(out_proj.shape, bf16),
            V(gate_weight.shape, bf16),
            V(up_weight.shape, bf16),
            V(down_weight.shape, bf16),
            V((seqs, span + extra, LATENT), bf16),
            V((n, seqs, span + extra, LATENT), bf16),
            V((n, seqs, nr, MTP * hk, LATENT), bf16),
            V((n * nr, seqs, MTP * hk, LATENT), bf16),
            V((n, seqs, 1, 2 * span), f32),
            V((n * nr, seqs, 1, 2 * span), f32),
            V((seqs, span, 128), f32),
            V((hk, seqs, all_rows // seqs, LATENT), f32),
            V((seqs, all_rows // seqs, hk * vdim), bf16),
            V((seqs, nr, all_rows // seqs, hk * vdim), bf16),
            V((all_rows, dd), f32),
            V((seqs, all_rows // seqs, dd), f32),
            V((seqs, all_rows // seqs, dd), bf16),
            V((seqs, n, all_rows // seqs, dd), bf16),
            V((n, crows, dd), f32),
            V((nr, part, 128), f32),
            V((nr, part, 128), f32),
            V((all_rows, ff), f32),
            V((all_rows, ff), f32),
            V((nr, 2, part, ff), bf16),
            V((nr, 2, part, ff), bf16),
            V((part, ff), bf16),
            V((nr, part, ff), bf16),
            V((all_rows, ff), f32),
            V((n, crows, dd), f32),
            V((n, crows, dd), bf16),
            V((n, crows, dd), bf16),
            sems(6),
            sems(4),
            sems(seqs, n),
            sems(11),
            sems(seqs),
            sems(seqs),
            sems(seqs, nr),
            sems(seqs, 2),
            sems(nf),
            sems(nf),
            sems(2),
            sems(2),
        ],
        compiler_params=pltpu.CompilerParams(
            collective_id=0, has_side_effects=True, vmem_limit_bytes=VMEM_BYTES),
        name="layer",
    )(queries.reshape(seqs, span, width), cache.transpose(0, 2, 1), lengths, positions, value_up_weight,
      residual, norm_gain, out_proj, gate_weight, up_weight, down_weight)


def solution(mesh):
    placed = (
        P(("groups", "role", "seq"), "ctx", None),
        P(("groups", "role", "seq"), "ctx", None),
        P(("groups", "role", "seq")),
        P(("groups", "role", "seq")),
        P("ctx", ("role", "seq"), None),
        P("ctx", ("role", "seq")),
        P("groups", ("role", "seq")),
        P(("role", "seq")),
        P(("role", "seq"), "ctx"),
        P(("role", "seq"), "ctx"),
        P("ctx", ("role", "seq")),
    )
    sizes = (mesh.shape["ctx"], mesh.shape["role"], mesh.shape["seq"])
    return jax.shard_map(
        functools.partial(per_device, sizes),
        mesh=mesh,
        in_specs=placed,
        out_specs=P(("groups", "ctx"), ("role", "seq")),
        check_vma=False,
    )
```

```python
import functools

import jax
import jax.numpy as jnp
from jax import lax
from jax.experimental import pallas as pl
from jax.experimental.pallas import tpu as pltpu
from jax.sharding import PartitionSpec as P

D = 7168
LATENT = 512
MTP = 2

softmax_scale = 0.07216878364870323
epsilon = 1e-06
MESH = pl.DeviceIdType.MESH
VMEM_BYTES = 60 * 1024 * 1024
f32, bf16 = jnp.float32, jnp.bfloat16


def ctx_group(n):
    me = lax.axis_index("ctx")

    def peer(d):
        k = lax.rem(me + d, n)
        return k, {"ctx": k}

    return me, peer


def feature_group(n_role, n_seq):
    n = n_role * n_seq
    me = lax.axis_index("role") * n_seq + lax.axis_index("seq")

    def peer(d):
        k = lax.rem(me + d, n)
        return k, {"role": k // n_seq, "seq": lax.rem(k, n_seq)}

    return me, peer


def enter(groups):
    barrier = pltpu.get_barrier_semaphore()
    count = 0
    for n, peer in groups:
        for d in range(1, n):
            pl.semaphore_signal(barrier, inc=1, device_id=peer(d)[1], device_id_type=MESH)
            count += 1
    pl.semaphore_wait(barrier, count)


def remote(src, dst, send, recv, device):
    return pltpu.make_async_remote_copy(
        src_ref=src, dst_ref=dst, send_sem=send, recv_sem=recv,
        device_id=device, device_id_type=MESH,
    )


def attend(n, n_role, n_seq, q_ref, cache_ref, cache_copy, len_ref, pos_ref, out_ref,
           q_all, o_send, o_recv, s_send, s_recv, a_send, sems):
    nr = n_role * n_seq
    me, peer = ctx_group(n)
    fme, fpeer = feature_group(n_role, n_seq)
    seqs, _, context = cache_ref.shape
    rows = q_ref.shape[1]
    heads = rows // MTP

    q_copies = []
    for s in range(seqs):
        for d in range(1, n):
            c = remote(q_ref.at[s], q_all.at[me, s], sems.at[s, d], sems.at[seqs + s, d],
                       peer(d)[1])
            c.start()
            q_copies.append(c)

    places = me * context + lax.broadcasted_iota(jnp.int32, (rows, context), 1)
    first = lax.broadcasted_iota(jnp.int32, (rows, context), 0) < heads
    lives = []
    for s in range(seqs):
        limit = jnp.where(first, pos_ref[MTP * s], pos_ref[MTP * s + 1])
        lives.append((places < len_ref[s]) & (places <= limit))

    lane = lax.broadcasted_iota(jnp.int32, (rows, 128), 1)

    def block(q, s):
        keys = cache_ref[s]
        scores = jnp.dot(q, keys, preferred_element_type=f32) * softmax_scale
        live = lives[s]
        top = jnp.max(jnp.where(live, scores, -1e30), axis=1, keepdims=True)
        probs = jnp.exp(jnp.where(live, scores - top, -1e30)).astype(bf16)
        total = jnp.sum(probs.astype(f32), axis=1, keepdims=True)
        out = lax.dot_general(
            probs, keys[:LATENT], (((1,), (1,)), ((), ())), preferred_element_type=f32)
        return out, top, total

    cache_copy.wait()
    own = [block(q_ref[s], s) for s in range(seqs)]
    o_copies, s_copies = {}, {}
    for s in range(seqs):
        for d in range(1, n):
            src, device = peer(n - d)
            remote(q_ref.at[s], q_all.at[src, s], sems.at[s, d], sems.at[seqs + s, d],
                   device).wait_recv()
            o, top, total = block(q_all[src, s], s)
            o_send[d, s] = o.astype(bf16)
            s_send[d, s] = jnp.where(lane == 0, top, total).T[0:8]
            c = remote(o_send.at[d, s], o_recv.at[d, s], sems.at[2 * seqs + s, d],
                       sems.at[3 * seqs + s, d], device)
            c.start()
            o_copies[s, d] = c
            c = remote(s_send.at[d, s], s_recv.at[d, s], sems.at[4 * seqs + s, d],
                       sems.at[5 * seqs + s, d], device)
            c.start()
            s_copies[s, d] = c
    for c in q_copies:
        c.wait_send()

    heads = rows // MTP
    merged = []
    for s in range(seqs):
        own_o, top, total = own[s]
        tops, totals = [top], [total]
        for d in range(1, n):
            s_copies[s, d].wait()
            back = jnp.concatenate([s_recv[d, s]] * 16, axis=0).T
            tops.append(back[:, 0:1])
            totals.append(back[:, 1:2])
        highest = functools.reduce(jnp.maximum, tops)
        factors = [jnp.exp(t - highest) for t in tops]
        denom = sum(f * t for f, t in zip(factors, totals))
        numer = factors[0] * own_o
        for d in range(1, n):
            o_copies[s, d].wait()
            numer = numer + factors[d] * o_recv[d, s].astype(f32)
        merged.append((numer / denom).astype(bf16))

    part = LATENT // nr
    for k in range(nr):
        for r in range(seqs * MTP):
            t = r % MTP
            a_send[k, r] = merged[r // MTP][t * heads:(t + 1) * heads, k * part:(k + 1) * part]
    copies = []
    for d in range(1, nr):
        k, device = fpeer(d)
        c = remote(a_send.at[k], out_ref.at[fme], sems.at[6 * seqs, d], sems.at[7 * seqs, d], device)
        c.start()
        copies.append(c)
    out_ref[fme] = a_send[fme]
    for d in range(1, nr):
        k, device = fpeer(nr - d)
        copies[d - 1].wait_send()
        remote(a_send.at[k], out_ref.at[k], sems.at[6 * seqs, d], sems.at[7 * seqs, d],
               device).wait_recv()


def layer_kernel(n, n_role, n_seq, q_ref, cache_hbm, len_ref, pos_ref, vu_hbm, res_ref, gain_ref,
                 wo_hbm, wg_hbm, wu_hbm, wd_hbm,
                 out_ref, cache, vu, q_all, o_send, o_recv, s_send, s_recv, a_send, a_all, a_head,
                 mixed, pv_ref, wo, wg, wu, wd, pv_recv, v_send, v_all, v_full, acc, po_send,
                 po_recv, resid, xg_ref, g_acc, u_acc, gu_send, gu_recv, ss_send, ss_recv, h_send,
                 h_all, h_full, dn, dn_send, dn_recv, wsem, lsem, asems, sems):
    nr = n_role * n_seq
    me, peer = ctx_group(n)
    fme, fpeer = feature_group(n_role, n_seq)

    cache_copy = pltpu.make_async_copy(cache_hbm, cache, lsem.at[0])
    cache_copy.start()
    vu_copy = pltpu.make_async_copy(vu_hbm, vu, lsem.at[1])
    vu_copy.start()
    weights = []
    for which, (hbm, vmem) in enumerate(((wo_hbm, wo), (wg_hbm, wg), (wu_hbm, wu), (wd_hbm, wd))):
        depth = vmem.shape[1]

        def fetch(i, hbm=hbm, vmem=vmem, depth=depth, which=which):
            return pltpu.make_async_copy(
                hbm.at[pl.ds(i * depth, depth)], vmem.at[i], wsem.at[which, i])

        weights.append((fetch, vmem))
    for fetch, vmem in weights:
        for i in range(vmem.shape[0]):
            fetch(i).start()
    enter(((n, peer), (nr, fpeer)))
    attend(n, n_role, n_seq, q_ref, cache, cache_copy, len_ref, pos_ref, a_all,
           q_all, o_send, o_recv, s_send, s_recv, a_send, asems)
    rows, heads = a_all.shape[1:3]
    for j in range(nr):
        for r in range(rows):
            a_head[:, j * rows + r, :] = a_all[j, r].astype(f32)
    vu_copy.wait()
    vdim = vu.shape[2]
    for h in range(heads):
        mixed[:, h * vdim:(h + 1) * vdim] = jnp.dot(
            a_head[h].astype(bf16), vu[h], preferred_element_type=f32)
    for k in range(nr):
        pv_ref[k] = mixed[k * rows:(k + 1) * rows, :].astype(bf16)

    def matmul(x_ref, *pairs):
        chunks, depth, _ = weights[pairs[0][0]][1].shape
        for which, acc_ref in pairs:
            fetch, vmem = weights[which]
            fetch(0).wait()
            acc_ref[...] = jnp.dot(x_ref[:, :depth], vmem[0], preferred_element_type=f32)
        if chunks == 1:
            return

        @pl.loop(1, chunks)
        def _(i):
            x = x_ref[:, pl.ds(pl.multiple_of(i * depth, depth), depth)]
            for which, acc_ref in pairs:
                fetch, vmem = weights[which]
                fetch(i).wait()
                acc_ref[...] += jnp.dot(x, vmem[i], preferred_element_type=f32)

    def swap(size, peer_of, chunk, recv, row):
        copies = []
        for d in range(1, size):
            k, device = peer_of(d)
            c = remote(chunk(k), recv.at[d], sems.at[row, d], sems.at[row + 1, d], device)
            c.start()
            copies.append(c)
        return copies

    def gather(size, my, peer_of, send, full, row):
        copies = []
        for d in range(1, size):
            c = remote(send, full.at[my], sems.at[row, d], sems.at[row + 1, d], peer_of(d)[1])
            c.start()
            copies.append(c)
        full[my] = send[...]
        for d in range(1, size):
            k, device = peer_of(size - d)
            copies[d - 1].wait_send()
            remote(send, full.at[k], sems.at[row, d], sems.at[row + 1, d], device).wait_recv()

    part = res_ref.shape[0] // nr
    copies = swap(nr, fpeer, lambda k: pv_ref.at[k], pv_recv, 0)
    vals = pv_ref[fme].astype(f32)
    for d in range(1, nr):
        copies[d - 1].wait()
        vals = vals + pv_recv[d].astype(f32)
    v_send[...] = vals.astype(bf16)
    gather(nr, fme, fpeer, v_send, v_all, 2)
    for k in range(nr):
        acc_rows = v_all[k].astype(f32)
        v_full[k * part:(k + 1) * part, :] = acc_rows
    x_ref = xg_ref[0]
    x_ref[...] = v_full[...].astype(bf16)
    matmul(x_ref, (0, acc))

    po_send[...] = acc[...].astype(bf16)
    copies = swap(n, peer, lambda k: po_send, po_recv, 4)
    total = res_ref[...].astype(f32) + acc[...]
    for d in range(1, n):
        copies[d - 1].wait()
        total = total + po_recv[d].astype(f32)
    crows = res_ref.shape[0] // n
    for k in range(n):
        resid[k] = total[k * crows:(k + 1) * crows]
    sumsq = jnp.sum(total * total, axis=1, keepdims=True)
    sumsq = jnp.broadcast_to(sumsq, (total.shape[0], 128))
    for k in range(nr):
        ss_send[k] = sumsq[k * part:(k + 1) * part]
    s_copies = swap(nr, fpeer, lambda k: ss_send.at[k], ss_recv, 6)
    x_ref = xg_ref[1]
    x_ref[...] = (total * gain_ref[...]).astype(bf16)
    matmul(x_ref, (1, g_acc), (2, u_acc))

    for j, a in enumerate((g_acc, u_acc)):
        for k in range(nr):
            gu_send[k, j] = a[k * part:(k + 1) * part, :].astype(bf16)
    copies = swap(nr, fpeer, lambda k: gu_send.at[k], gu_recv, 8)
    ss = ss_send[fme]
    for d in range(1, nr):
        s_copies[d - 1].wait()
        ss = ss + ss_recv[d]
    inv = lax.rsqrt(ss[:, 0:1] / D + epsilon)
    gate = gu_send[fme, 0].astype(f32)
    up = gu_send[fme, 1].astype(f32)
    for d in range(1, nr):
        copies[d - 1].wait()
        gate = gate + gu_recv[d, 0].astype(f32)
        up = up + gu_recv[d, 1].astype(f32)
    gate = gate * inv
    up = up * inv
    h_send[...] = (gate / (1.0 + jnp.exp(-gate)) * up).astype(bf16)
    gather(nr, fme, fpeer, h_send, h_all, 10)
    for k in range(nr):
        h_full[k * part:(k + 1) * part, :] = h_all[k].astype(f32)
    x_ref = xg_ref[2]
    x_ref[...] = h_full[...].astype(bf16)
    matmul(x_ref, (3, acc))

    for k in range(n):
        piece = acc[k * crows:(k + 1) * crows, :]
        dn[k] = piece
        dn_send[k] = piece.astype(bf16)
    copies = swap(n, peer, lambda k: dn_send.at[k], dn_recv, 12)
    result = resid[me] + dn[me]
    for d in range(1, n):
        copies[d - 1].wait()
        result = result + dn_recv[d].astype(f32)
    out_ref[...] = result.astype(bf16)


def chunk_of(depth):
    for size in (1024, 768, 512, 256):
        if depth % size == 0:
            return size
    return depth


def per_device_latents(sizes, queries, cache, lengths, positions, value_up_weight, out_proj, residual,
               norm_gain, gate_weight, up_weight, down_weight):
    n, n_role, n_seq = sizes
    nr = n_role * n_seq
    rows, heads, width = queries.shape
    seqs = cache.shape[0]
    span = rows * heads // seqs
    lat = LATENT // nr
    vmem = pl.BlockSpec(memory_space=pltpu.VMEM)
    smem = pl.BlockSpec(memory_space=pltpu.SMEM)
    hbm = pl.BlockSpec(memory_space=pl.ANY)
    most = max(n, nr)
    sems = lambda k: pltpu.SemaphoreType.DMA((k, most))
    vwide = heads * value_up_weight.shape[2]
    all_rows, dd = residual.shape
    ff = gate_weight.shape[1]
    part, crows = all_rows // nr, all_rows // n

    def held(w):
        size = chunk_of(w.shape[0])
        return pltpu.VMEM((w.shape[0] // size, size, w.shape[1]), bf16)

    ws = (out_proj, gate_weight, up_weight, down_weight)
    most_chunks = max(w.shape[0] // chunk_of(w.shape[0]) for w in ws)
    V = pltpu.VMEM
    return pl.pallas_call(
        functools.partial(layer_kernel, n, n_role, n_seq),
        out_shape=jax.ShapeDtypeStruct((crows, dd), bf16),
        in_specs=[vmem, hbm, smem, smem, hbm, vmem, vmem] + [hbm] * 4,
        out_specs=vmem,
        scratch_shapes=[
            V((cache.shape[0], width, cache.shape[1]), bf16),
            V(value_up_weight.shape, bf16),
            V((n, seqs, span, width), bf16),
            V((n, seqs, span, LATENT), bf16),
            V((n, seqs, span, LATENT), bf16),
            V((n, seqs, 8, span), f32),
            V((n, seqs, 8, span), f32),
            V((nr, rows, heads, lat), bf16),
            V((nr, rows, heads, lat), bf16),
            V((heads, all_rows, lat), f32),
            V((all_rows, vwide), f32),
            V((nr, part, vwide), bf16),
            *[held(w) for w in ws],
            V((nr, part, vwide), bf16),
            V((part, vwide), bf16),
            V((nr, part, vwide), bf16),
            V((all_rows, vwide), f32),
            V((all_rows, dd), f32),
            V((all_rows, dd), bf16),
            V((n, all_rows, dd), bf16),
            V((n, crows, dd), f32),
            [V((all_rows, vwide), bf16), V((all_rows, dd), bf16), V((all_rows, ff), bf16)],
            V((all_rows, ff), f32),
            V((all_rows, ff), f32),
            V((nr, 2, part, ff), bf16),
            V((nr, 2, part, ff), bf16),
            V((nr, part, 128), f32),
            V((nr, part, 128), f32),
            V((part, ff), bf16),
            V((nr, part, ff), bf16),
            V((all_rows, ff), f32),
            V((n, crows, dd), f32),
            V((n, crows, dd), bf16),
            V((n, crows, dd), bf16),
            pltpu.SemaphoreType.DMA((4, most_chunks)),
            pltpu.SemaphoreType.DMA((2,)),
            sems(8 * seqs),
            sems(14),
        ],
        compiler_params=pltpu.CompilerParams(
            collective_id=0, has_side_effects=True, vmem_limit_bytes=VMEM_BYTES),
        name="layer",
    )(queries.reshape(seqs, span, width), cache.transpose(0, 2, 1), lengths, positions, value_up_weight,
      residual, norm_gain.reshape(1, dd), *ws)


LOG2E = 1.4426950408889634


def by_distance(n, me):
    found = []
    for i in range(n - 1):
        k = jnp.int32(0)
        for z in range(n):
            others = sorted((j for j in range(n) if j != z), key=lambda j: (abs(j - z), j))
            k = jnp.where(me == z, others[i], k)
        found.append(k)
    return found


def cut(width):
    unit = 256 if width % 256 == 0 else 128
    if width % unit or width < 2 * unit:
        return [(0, width)]
    first = width // unit // 2 * unit
    return [(0, first), (first, width)]


def heads_kernel(n, n_role, n_seq, q_hbm, cache_hbm, len_ref, pos_ref, vu_hbm, res_hbm, gain_hbm,
                 wo_hbm, wg_hbm, wu_hbm, wd_hbm, out_ref,
                 q_ref, cache, vu, res_ref, gain_ref, wo, wg, wu, wd,
                 q_send, q_all, o_send, o_recv, st_send, st_recv, w_ref,
                 a_head, v_send, xv, acc, po, po_send, po_recv, resid, ss_send, ss_recv,
                 g_acc, u_acc, gu_send, gu_recv, h_send, h_all, h_full, dn, dn_send, dn_recv,
                 lsem, wsem, qsem, gone, osem, stsem, vsem, posem, gusem, hsem, dnsem, onesem):
    nr = n_role * n_seq
    me = lax.axis_index("ctx")
    role, seq = lax.axis_index("role"), lax.axis_index("seq")
    fme = role * n_seq + seq
    near = by_distance(n, me)
    mates = []
    for dr in range(n_role):
        for ds in range(n_seq):
            if dr or ds:
                r, s = lax.rem(role + dr, n_role), lax.rem(seq + ds, n_seq)
                mates.append((r * n_seq + s, {"role": r, "seq": s}))
    seqs, span, width = q_ref.shape
    context = cache.shape[2]
    heads = span // MTP
    hk = heads // nr
    rope = width - LATENT
    lat = LATENT // nr
    own = n - 1
    extra = span * rope // LATENT

    paired = n == 4
    if paired:
        beside = me + 1 - 2 * lax.rem(me, 2)
        across = 2 - me // 2
        beyond = 3 - 3 * (me // 2)
        inner = lax.rem((me + 1) // 2, 2)
        reach = [beside, across]
    else:
        reach = near[::-1]

    q_copy = pltpu.make_async_copy(q_hbm, q_ref, lsem.at[0])
    q_copy.start()
    cache_copies = [
        pltpu.make_async_copy(cache_hbm, cache.at[:, pl.ds(0, width), :], lsem.at[1]),
        pltpu.make_async_copy(cache_hbm.at[:, pl.ds(LATENT, rope), :],
                              cache.at[:, pl.ds(width, rope), :], lsem.at[2]),
    ]
    for c in cache_copies:
        c.start()
    barrier = pltpu.get_barrier_semaphore()
    if paired:
        pl.semaphore_signal(barrier, inc=1, device_id={"ctx": beside}, device_id_type=MESH)

        @pl.when(inner == 1)
        def _():
            for k in (across, beyond):
                pl.semaphore_signal(barrier, inc=1, device_id={"ctx": k}, device_id_type=MESH)
    else:
        for k in near:
            pl.semaphore_signal(barrier, inc=1, device_id={"ctx": k}, device_id_type=MESH)
    for _, device in mates:
        pl.semaphore_signal(barrier, inc=1, device_id=device, device_id_type=MESH)
    vu_own = pltpu.make_async_copy(
        vu_hbm.at[pl.ds(pl.multiple_of(fme * hk, hk), hk)],
        vu.at[:, pl.ds(pl.multiple_of(fme * lat, lat), lat), :], lsem.at[3])
    vu_own.start()
    res_copy = pltpu.make_async_copy(res_hbm, res_ref, lsem.at[4])
    res_copy.start()
    gain_copy = pltpu.make_async_copy(gain_hbm, gain_ref.at[0], lsem.at[5])
    gain_copy.start()

    q_copy.wait()
    for s in range(seqs):
        qn, qr = [], []
        for k in range(nr):
            for t in range(MTP):
                at = t * heads + k * hk
                rows = q_ref[s, at:at + hk, :].astype(f32)
                qn.append(rows[:, :LATENT])
                qr.append(rows[:, LATENT:])
        q_send[s, :span] = jnp.concatenate(qn, axis=0).astype(bf16)
        qr = jnp.concatenate(qr, axis=0)
        qr = jnp.concatenate([qr[:span // 2], qr[span // 2:]], axis=1)
        q_send[s, span:] = jnp.concatenate(
            [qr[i:i + extra] for i in range(0, span // 2, extra)], axis=1).astype(bf16)
    weights = []
    for which, (hbm, vmem) in enumerate(((wo_hbm, wo), (wg_hbm, wg), (wu_hbm, wu), (wd_hbm, wd))):
        weights.append(pltpu.make_async_copy(hbm, vmem, wsem.at[which]))
    for c in weights:
        c.start()
    pl.semaphore_wait(barrier, len(reach) + len(mates))

    Q, RELAY, VU, O, ST, VAL, PO, SS, GU, H, DN = range(11)

    def send(src, dst, kind, recv_sem, device):
        remote(src, dst, gone.at[kind], recv_sem, device).start()

    def all_gone(kind, like):
        remote(like, like, gone.at[kind], gone.at[kind], {"ctx": near[0]}).wait_send()

    def all_here(like, recv_sem):
        remote(like, like, gone.at[0], recv_sem, {"ctx": near[0]}).wait_recv()

    def take(b, s):
        all_here(q_all.at[b, s], qsem.at[s, b])

    for s in range(seqs):
        for k in reach:
            send(q_send.at[s], q_all.at[me, s], Q, qsem.at[s, me], {"ctx": k})
    for k, device in mates:
        send(vu_hbm.at[pl.ds(pl.multiple_of(k * hk, hk), hk)],
             vu.at[:, pl.ds(pl.multiple_of(fme * lat, lat), lat), :], VU, onesem.at[0], device)

    column = lax.broadcasted_iota(jnp.int32, (span, context), 1)
    row = lax.broadcasted_iota(jnp.int32, (span, 1), 0)
    even = lax.rem(row, MTP * hk) < hk
    lane = lax.broadcasted_iota(jnp.int32, (span, 128), 1)
    half = lax.broadcasted_iota(jnp.int32, (span // 2, 2 * rope), 1) < rope
    ends = []
    for s in range(seqs):
        limit = jnp.where(even, pos_ref[MTP * s], pos_ref[MTP * s + 1]) + 1
        ends.append(jnp.minimum(limit, len_ref[s]) - me * context)

    def block(queries, s, slot):
        qn, qr = queries[:span], queries[span:].astype(f32)
        qr = jnp.concatenate([qr[:, i:i + 128] for i in range(0, LATENT, 128)], axis=0)
        zero = jnp.zeros_like(qr)
        q = jnp.concatenate(
            [qn, jnp.concatenate([jnp.where(half, qr, zero), jnp.where(half, zero, qr)],
                                 axis=0).astype(bf16)],
            axis=1)
        keys = cache[s]
        scores = jnp.dot(q, keys, preferred_element_type=f32) * (softmax_scale * LOG2E)
        scores = jnp.where(column < ends[s], scores, -1e30)
        top = jnp.maximum(jnp.max(scores, axis=1, keepdims=True), -1e29)
        probs = jnp.exp2(scores - top).astype(bf16)
        total = jnp.sum(probs.astype(f32), axis=1, keepdims=True)
        out = lax.dot_general(
            probs, keys[:LATENT], (((1,), (1,)), ((), ())), preferred_element_type=f32)
        out = out.astype(bf16)
        for k in range(nr):
            o_send[slot, s, k] = out[k * MTP * hk:(k + 1) * MTP * hk]
        stats = jnp.where(lane == 0, top, total).T
        st_send[slot, s] = jnp.concatenate([stats[0:1], stats[1:2]], axis=1)

    mine = me * nr + fme
    for c in cache_copies:
        c.wait()
    def home(s):
        block(q_send[s], s, own)
        for k, device in mates:
            send(o_send.at[own, s, k], o_recv.at[mine, s], O, osem.at[s], device)
            send(st_send.at[own, s], st_recv.at[mine, s], ST, stsem.at[s], device)
        for c in (
            pltpu.make_async_copy(o_send.at[own, s, fme], o_recv.at[mine, s], osem.at[s]),
            pltpu.make_async_copy(st_send.at[own, s], st_recv.at[mine, s], stsem.at[s]),
        ):
            c.start()

    def answer(b, s, slot):
        block(q_all[b, s], s, slot)
        for k in range(nr):
            device = {"ctx": b, "role": k // n_seq, "seq": k % n_seq}
            send(o_send.at[slot, s, k], o_recv.at[mine, s], O, osem.at[s], device)
            send(st_send.at[slot, s], st_recv.at[mine, s], ST, stsem.at[s], device)

    if paired:
        def relay(b, s):
            @pl.when(inner == 1)
            def _():
                take(b, s)
                send(q_all.at[b, s], q_all.at[b, s], RELAY, qsem.at[s, b], {"ctx": beside})

        def take_outer(b, s):
            @pl.when(inner == 0)
            def _():
                take(b, s)

        home(0)
        relay(across, 0)
        for s in range(seqs):
            take(beside, s)
            answer(beside, s, 0)
            if s == 0:
                relay(beyond, 0)
            if s + 1 < seqs:
                relay(across, s + 1)
            take_outer(across, s)
            answer(across, s, 1)
            if s + 1 < seqs:
                relay(beyond, s + 1)
            take_outer(beyond, s)
            answer(beyond, s, 2)
        for s in range(1, seqs):
            home(s)
    else:
        for s in range(seqs):
            home(s)
            for i, b in enumerate(near):
                take(b, s)
                answer(b, s, i)

    rows = seqs * MTP
    all_rows = nr * rows
    mine_at = pl.ds(pl.multiple_of(fme * MTP * hk, MTP * hk), MTP * hk)
    vdim = vu.shape[2]
    deep = hk * vdim
    others = len(mates)

    def merge(s):
        all_here(st_recv.at[:, s], stsem.at[s])
        tops, totals = [], []
        for b in range(n):
            stats = jnp.concatenate([st_recv[b * nr + j, s] for j in range(nr)], axis=0)
            tops.append(stats[:, :span])
            totals.append(stats[:, span:])
        highest = functools.reduce(jnp.maximum, tops)
        factors = [jnp.exp2(t - highest) for t in tops]
        denom = sum(f * t for f, t in zip(factors, totals))
        shares = jnp.concatenate([f / denom for f in factors], axis=0)
        copies = -(-128 // (n * nr))
        shares = jnp.concatenate([shares] * copies, axis=0)[:128]
        w_ref[s] = shares.T
        share = w_ref[s, mine_at, :]
        all_here(o_recv.at[:, s], osem.at[s])
        for j in range(nr):
            mixed = None
            for b in range(n):
                i = b * nr + j
                term = share[:, i:i + 1] * o_recv[i, s].astype(f32)
                mixed = term if mixed is None else mixed + term
            for t in range(MTP):
                a_head[:, s, j * MTP + t, :] = mixed[t * hk:(t + 1) * hk]
        if s == 0:
            vu_own.wait()
            all_here(vu.at[:, :others * lat], onesem.at[0])
        for h in range(hk):
            v_send[s, :, h * vdim:(h + 1) * vdim] = jnp.dot(
                a_head[h, s].astype(bf16), vu[h], preferred_element_type=f32).astype(bf16)
        for k, device in mates:
            send(v_send.at[s], xv.at[s, fme], VAL, vsem.at[s, fme], device)

    early, late = mates[:n_seq - 1], mates[n_seq - 1:]
    dd = acc.shape[1]
    parts = cut(dd)

    def wo_rows(k):
        return pl.ds(pl.multiple_of(k * deep, deep), deep)

    def begin(s):
        if s == 0:
            weights[0].wait()
        po[s] = jnp.dot(v_send[s], wo[wo_rows(fme), :], preferred_element_type=f32)
        for k, device in early:
            all_here(xv.at[s, k], vsem.at[s, k])
            po[s] += jnp.dot(xv[s, k], wo[wo_rows(k), :], preferred_element_type=f32)

    def finish(s):
        for k, device in late:
            all_here(xv.at[s, k], vsem.at[s, k])
        for p, (c0, c1) in enumerate(parts):
            total = po[s, :, c0:c1]
            for k, device in late:
                total = total + jnp.dot(xv[s, k], wo[wo_rows(k), c0:c1], preferred_element_type=f32)
            po[s, :, c0:c1] = total
            po_send[s, :, c0:c1] = total.astype(bf16)
            for k in near[::-1]:
                send(po_send.at[s, :, c0:c1], po_recv.at[s, me, :, c0:c1], PO, posem.at[s, p],
                     {"ctx": k})

    for s in range(seqs):
        merge(s)
        if s:
            finish(s - 1)
        begin(s)
    finish(seqs - 1)
    all_gone(Q, q_all.at[:len(reach)])
    if paired:
        @pl.when(inner == 1)
        def _():
            all_gone(RELAY, q_all.at[:2])
    all_gone(VU, vu.at[:, :others * lat])
    all_gone(O, o_recv.at[:n * nr - 1])
    all_gone(ST, st_recv.at[:n * nr - 1])
    all_gone(VAL, xv.at[:, :others])
    res_copy.wait()
    gain_copy.wait()
    weights[1].wait()
    weights[2].wait()

    part, crows = all_rows // nr, all_rows // n
    ff = g_acc.shape[1]
    fparts = [(f, min(f + 768, ff)) for f in range(0, ff, 768)]
    sumsq = jnp.zeros((all_rows, 1), f32)
    for p, (c0, c1) in enumerate(parts):
        for s in range(seqs):
            all_here(po_recv.at[s, :n - 1, :, c0:c1], posem.at[s, p])
            total = po[s, :, c0:c1]
            for k in near:
                total = total + po_recv[s, k, :, c0:c1].astype(f32)
            for j in range(nr):
                at = j * rows + s * MTP
                acc[at:at + MTP, c0:c1] = total[j * MTP:(j + 1) * MTP]
        total = res_ref[:, c0:c1].astype(f32) + acc[:, c0:c1]
        for k in range(n):
            resid[k, :, c0:c1] = total[k * crows:(k + 1) * crows]
        sumsq = sumsq + jnp.sum(total * total, axis=1, keepdims=True)
        x = (total * gain_ref[:, c0:c1]).astype(bf16)
        last = p == len(parts) - 1
        if last:
            wide = jnp.broadcast_to(sumsq, (all_rows, 128))
            for k in range(nr):
                ss_send[k] = wide[k * part:(k + 1) * part]
            for k, device in mates:
                send(ss_send.at[k], ss_recv.at[fme], SS, onesem.at[1], device)
        for q, (f0, f1) in enumerate(fparts if last else [(0, ff)]):
            for j, (w, a) in enumerate(((wg, g_acc), (wu, u_acc))):
                y = jnp.dot(x, w[c0:c1, f0:f1], preferred_element_type=f32)
                if p:
                    y = y + a[:, f0:f1]
                if not last:
                    a[:, f0:f1] = y
                    continue
                for k in range(nr):
                    gu_send[k, j, :, f0:f1] = y[k * part:(k + 1) * part].astype(bf16)
            if last:
                for k, device in mates:
                    send(gu_send.at[k, :, :, f0:f1], gu_recv.at[fme, :, :, f0:f1],
                         GU, gusem.at[q], device)
    ss = ss_send[fme]
    all_here(ss_recv.at[:others], onesem.at[1])
    for k, device in mates:
        ss = ss + ss_recv[k]
    inv = lax.rsqrt(ss[:, 0:1] / D + epsilon)
    for q, (f0, f1) in enumerate(fparts):
        gate = gu_send[fme, 0, :, f0:f1].astype(f32)
        up = gu_send[fme, 1, :, f0:f1].astype(f32)
        all_here(gu_recv.at[:others, :, :, f0:f1], gusem.at[q])
        for k, device in mates:
            gate = gate + gu_recv[k, 0, :, f0:f1].astype(f32)
            up = up + gu_recv[k, 1, :, f0:f1].astype(f32)
        gate = gate * inv
        up = up * inv
        h = (gate / (1.0 + jnp.exp(-gate)) * up).astype(bf16)
        h_send[:, f0:f1] = h
        h_all[fme, :, f0:f1] = h
        for k, device in mates:
            send(h_send.at[:, f0:f1], h_all.at[fme, :, f0:f1], H, hsem.at[q], device)
    weights[3].wait()
    for q, (f0, f1) in enumerate(fparts):
        all_here(h_all.at[:others, :, f0:f1], hsem.at[q])
        for k in range(nr):
            h_full[k * part:(k + 1) * part, f0:f1] = h_all[k, :, f0:f1].astype(f32)
        x = h_full[:, f0:f1].astype(bf16)
        last = q == len(fparts) - 1
        for p, (c0, c1) in enumerate(parts if last else [(0, dd)]):
            y = jnp.dot(x, wd[f0:f1, c0:c1], preferred_element_type=f32)
            if q:
                y = y + acc[:, c0:c1]
            if not last:
                acc[:, c0:c1] = y
                continue
            for k in range(n):
                piece = y[k * crows:(k + 1) * crows]
                dn[k, :, c0:c1] = piece
                dn_send[k, :, c0:c1] = piece.astype(bf16)
            for k in near[::-1]:
                send(dn_send.at[k, :, c0:c1], dn_recv.at[me, :, c0:c1], DN, dnsem.at[p], {"ctx": k})
    all_gone(PO, po_recv.at[:, :n - 1])
    all_gone(SS, ss_recv.at[:others])
    all_gone(GU, gu_recv.at[:others])
    all_gone(H, h_all.at[:others])
    for p, (c0, c1) in enumerate(parts):
        result = resid[me, :, c0:c1] + dn[me, :, c0:c1]
        all_here(dn_recv.at[:n - 1, :, c0:c1], dnsem.at[p])
        for k in near:
            result = result + dn_recv[k, :, c0:c1].astype(f32)
        out_ref[:, c0:c1] = result.astype(bf16)
    all_gone(DN, dn_recv.at[:n - 1])


def per_device(sizes, queries, cache, lengths, positions, value_up_weight, out_proj, residual,
               norm_gain, gate_weight, up_weight, down_weight):
    n, n_role, n_seq = sizes
    nr = n_role * n_seq
    rows, heads, width = queries.shape
    seqs, context = cache.shape[:2]
    rope = width - LATENT
    if heads % (8 * nr) or 2 * rope != 128 or n < 2 or nr < 2:
        return per_device_latents(
            sizes, queries, cache, lengths, positions, value_up_weight, out_proj, residual,
            norm_gain, gate_weight, up_weight, down_weight)
    hk = heads // nr
    span = rows * heads // seqs
    extra = span * rope // LATENT
    vdim = value_up_weight.shape[2]
    all_rows, dd = residual.shape
    ff = gate_weight.shape[1]
    part, crows = all_rows // nr, all_rows // n
    nf = -(-ff // 768)
    vmem = pl.BlockSpec(memory_space=pltpu.VMEM)
    smem = pl.BlockSpec(memory_space=pltpu.SMEM)
    hbm = pl.BlockSpec(memory_space=pl.ANY)
    V = pltpu.VMEM
    sems = lambda *k: pltpu.SemaphoreType.DMA(k)
    return pl.pallas_call(
        functools.partial(heads_kernel, n, n_role, n_seq),
        out_shape=pltpu.VMEM((crows, dd), bf16),
        in_specs=[hbm, hbm, smem, smem] + [hbm] * 7,
        out_specs=vmem,
        scratch_shapes=[
            V((seqs, span, width), bf16),
            V((seqs, width + rope, context), bf16),
            V((hk, LATENT, vdim), bf16),
            V((all_rows, dd), bf16),
            V((1, dd), f32),
            V(out_proj.shape, bf16),
            V(gate_weight.shape, bf16),
            V(up_weight.shape, bf16),
            V(down_weight.shape, bf16),
            V((seqs, span + extra, LATENT), bf16),
            V((n, seqs, span + extra, LATENT), bf16),
            V((n, seqs, nr, MTP * hk, LATENT), bf16),
            V((n * nr, seqs, MTP * hk, LATENT), bf16),
            V((n, seqs, 1, 2 * span), f32),
            V((n * nr, seqs, 1, 2 * span), f32),
            V((seqs, span, 128), f32),
            V((hk, seqs, all_rows // seqs, LATENT), f32),
            V((seqs, all_rows // seqs, hk * vdim), bf16),
            V((seqs, nr, all_rows // seqs, hk * vdim), bf16),
            V((all_rows, dd), f32),
            V((seqs, all_rows // seqs, dd), f32),
            V((seqs, all_rows // seqs, dd), bf16),
            V((seqs, n, all_rows // seqs, dd), bf16),
            V((n, crows, dd), f32),
            V((nr, part, 128), f32),
            V((nr, part, 128), f32),
            V((all_rows, ff), f32),
            V((all_rows, ff), f32),
            V((nr, 2, part, ff), bf16),
            V((nr, 2, part, ff), bf16),
            V((part, ff), bf16),
            V((nr, part, ff), bf16),
            V((all_rows, ff), f32),
            V((n, crows, dd), f32),
            V((n, crows, dd), bf16),
            V((n, crows, dd), bf16),
            sems(6),
            sems(4),
            sems(seqs, n),
            sems(11),
            sems(seqs),
            sems(seqs),
            sems(seqs, nr),
            sems(seqs, 2),
            sems(nf),
            sems(nf),
            sems(2),
            sems(2),
        ],
        compiler_params=pltpu.CompilerParams(
            collective_id=0, has_side_effects=True, vmem_limit_bytes=VMEM_BYTES),
        name="layer",
    )(queries.reshape(seqs, span, width), cache.transpose(0, 2, 1), lengths, positions, value_up_weight,
      residual, norm_gain, out_proj, gate_weight, up_weight, down_weight)


def solution(mesh):
    placed = (
        P(("groups", "role", "seq"), "ctx", None),
        P(("groups", "role", "seq"), "ctx", None),
        P(("groups", "role", "seq")),
        P(("groups", "role", "seq")),
        P("ctx", ("role", "seq"), None),
        P("ctx", ("role", "seq")),
        P("groups", ("role", "seq")),
        P(("role", "seq")),
        P(("role", "seq"), "ctx"),
        P(("role", "seq"), "ctx"),
        P("ctx", ("role", "seq")),
    )
    sizes = (mesh.shape["ctx"], mesh.shape["role"], mesh.shape["seq"])
    return jax.shard_map(
        functools.partial(per_device, sizes),
        mesh=mesh,
        in_specs=placed,
        out_specs=P(("groups", "ctx"), ("role", "seq")),
        check_vma=False,
    )
```

```python
import functools

import jax
import jax.numpy as jnp
from jax import lax
from jax.experimental import pallas as pl
from jax.experimental.pallas import tpu as pltpu
from jax.sharding import PartitionSpec as P

D = 7168
LATENT = 512
MTP = 2

softmax_scale = 0.07216878364870323
epsilon = 1e-06
MESH = pl.DeviceIdType.MESH
VMEM_BYTES = 60 * 1024 * 1024
f32, bf16 = jnp.float32, jnp.bfloat16


def ctx_group(n):
    me = lax.axis_index("ctx")

    def peer(d):
        k = lax.rem(me + d, n)
        return k, {"ctx": k}

    return me, peer


def feature_group(n_role, n_seq):
    n = n_role * n_seq
    me = lax.axis_index("role") * n_seq + lax.axis_index("seq")

    def peer(d):
        k = lax.rem(me + d, n)
        return k, {"role": k // n_seq, "seq": lax.rem(k, n_seq)}

    return me, peer


def enter(groups):
    barrier = pltpu.get_barrier_semaphore()
    count = 0
    for n, peer in groups:
        for d in range(1, n):
            pl.semaphore_signal(barrier, inc=1, device_id=peer(d)[1], device_id_type=MESH)
            count += 1
    pl.semaphore_wait(barrier, count)


def remote(src, dst, send, recv, device):
    return pltpu.make_async_remote_copy(
        src_ref=src, dst_ref=dst, send_sem=send, recv_sem=recv,
        device_id=device, device_id_type=MESH,
    )


def attend(n, n_role, n_seq, q_ref, cache_ref, cache_copy, len_ref, pos_ref, out_ref,
           q_all, o_send, o_recv, s_send, s_recv, a_send, sems):
    nr = n_role * n_seq
    me, peer = ctx_group(n)
    fme, fpeer = feature_group(n_role, n_seq)
    seqs, _, context = cache_ref.shape
    rows = q_ref.shape[1]
    heads = rows // MTP

    q_copies = []
    for s in range(seqs):
        for d in range(1, n):
            c = remote(q_ref.at[s], q_all.at[me, s], sems.at[s, d], sems.at[seqs + s, d],
                       peer(d)[1])
            c.start()
            q_copies.append(c)

    places = me * context + lax.broadcasted_iota(jnp.int32, (rows, context), 1)
    first = lax.broadcasted_iota(jnp.int32, (rows, context), 0) < heads
    lives = []
    for s in range(seqs):
        limit = jnp.where(first, pos_ref[MTP * s], pos_ref[MTP * s + 1])
        lives.append((places < len_ref[s]) & (places <= limit))

    lane = lax.broadcasted_iota(jnp.int32, (rows, 128), 1)

    def block(q, s):
        keys = cache_ref[s]
        scores = jnp.dot(q, keys, preferred_element_type=f32) * softmax_scale
        live = lives[s]
        top = jnp.max(jnp.where(live, scores, -1e30), axis=1, keepdims=True)
        probs = jnp.exp(jnp.where(live, scores - top, -1e30)).astype(bf16)
        total = jnp.sum(probs.astype(f32), axis=1, keepdims=True)
        out = lax.dot_general(
            probs, keys[:LATENT], (((1,), (1,)), ((), ())), preferred_element_type=f32)
        return out, top, total

    cache_copy.wait()
    own = [block(q_ref[s], s) for s in range(seqs)]
    o_copies, s_copies = {}, {}
    for s in range(seqs):
        for d in range(1, n):
            src, device = peer(n - d)
            remote(q_ref.at[s], q_all.at[src, s], sems.at[s, d], sems.at[seqs + s, d],
                   device).wait_recv()
            o, top, total = block(q_all[src, s], s)
            o_send[d, s] = o.astype(bf16)
            s_send[d, s] = jnp.where(lane == 0, top, total).T[0:8]
            c = remote(o_send.at[d, s], o_recv.at[d, s], sems.at[2 * seqs + s, d],
                       sems.at[3 * seqs + s, d], device)
            c.start()
            o_copies[s, d] = c
            c = remote(s_send.at[d, s], s_recv.at[d, s], sems.at[4 * seqs + s, d],
                       sems.at[5 * seqs + s, d], device)
            c.start()
            s_copies[s, d] = c
    for c in q_copies:
        c.wait_send()

    heads = rows // MTP
    merged = []
    for s in range(seqs):
        own_o, top, total = own[s]
        tops, totals = [top], [total]
        for d in range(1, n):
            s_copies[s, d].wait()
            back = jnp.concatenate([s_recv[d, s]] * 16, axis=0).T
            tops.append(back[:, 0:1])
            totals.append(back[:, 1:2])
        highest = functools.reduce(jnp.maximum, tops)
        factors = [jnp.exp(t - highest) for t in tops]
        denom = sum(f * t for f, t in zip(factors, totals))
        numer = factors[0] * own_o
        for d in range(1, n):
            o_copies[s, d].wait()
            numer = numer + factors[d] * o_recv[d, s].astype(f32)
        merged.append((numer / denom).astype(bf16))

    part = LATENT // nr
    for k in range(nr):
        for r in range(seqs * MTP):
            t = r % MTP
            a_send[k, r] = merged[r // MTP][t * heads:(t + 1) * heads, k * part:(k + 1) * part]
    copies = []
    for d in range(1, nr):
        k, device = fpeer(d)
        c = remote(a_send.at[k], out_ref.at[fme], sems.at[6 * seqs, d], sems.at[7 * seqs, d], device)
        c.start()
        copies.append(c)
    out_ref[fme] = a_send[fme]
    for d in range(1, nr):
        k, device = fpeer(nr - d)
        copies[d - 1].wait_send()
        remote(a_send.at[k], out_ref.at[k], sems.at[6 * seqs, d], sems.at[7 * seqs, d],
               device).wait_recv()


def layer_kernel(n, n_role, n_seq, q_ref, cache_hbm, len_ref, pos_ref, vu_hbm, res_ref, gain_ref,
                 wo_hbm, wg_hbm, wu_hbm, wd_hbm,
                 out_ref, cache, vu, q_all, o_send, o_recv, s_send, s_recv, a_send, a_all, a_head,
                 mixed, pv_ref, wo, wg, wu, wd, pv_recv, v_send, v_all, v_full, acc, po_send,
                 po_recv, resid, xg_ref, g_acc, u_acc, gu_send, gu_recv, ss_send, ss_recv, h_send,
                 h_all, h_full, dn, dn_send, dn_recv, wsem, lsem, asems, sems):
    nr = n_role * n_seq
    me, peer = ctx_group(n)
    fme, fpeer = feature_group(n_role, n_seq)

    cache_copy = pltpu.make_async_copy(cache_hbm, cache, lsem.at[0])
    cache_copy.start()
    vu_copy = pltpu.make_async_copy(vu_hbm, vu, lsem.at[1])
    vu_copy.start()
    weights = []
    for which, (hbm, vmem) in enumerate(((wo_hbm, wo), (wg_hbm, wg), (wu_hbm, wu), (wd_hbm, wd))):
        depth = vmem.shape[1]

        def fetch(i, hbm=hbm, vmem=vmem, depth=depth, which=which):
            return pltpu.make_async_copy(
                hbm.at[pl.ds(i * depth, depth)], vmem.at[i], wsem.at[which, i])

        weights.append((fetch, vmem))
    for fetch, vmem in weights:
        for i in range(vmem.shape[0]):
            fetch(i).start()
    enter(((n, peer), (nr, fpeer)))
    attend(n, n_role, n_seq, q_ref, cache, cache_copy, len_ref, pos_ref, a_all,
           q_all, o_send, o_recv, s_send, s_recv, a_send, asems)
    rows, heads = a_all.shape[1:3]
    for j in range(nr):
        for r in range(rows):
            a_head[:, j * rows + r, :] = a_all[j, r].astype(f32)
    vu_copy.wait()
    vdim = vu.shape[2]
    for h in range(heads):
        mixed[:, h * vdim:(h + 1) * vdim] = jnp.dot(
            a_head[h].astype(bf16), vu[h], preferred_element_type=f32)
    for k in range(nr):
        pv_ref[k] = mixed[k * rows:(k + 1) * rows, :].astype(bf16)

    def matmul(x_ref, *pairs):
        chunks, depth, _ = weights[pairs[0][0]][1].shape
        for which, acc_ref in pairs:
            fetch, vmem = weights[which]
            fetch(0).wait()
            acc_ref[...] = jnp.dot(x_ref[:, :depth], vmem[0], preferred_element_type=f32)
        if chunks == 1:
            return

        @pl.loop(1, chunks)
        def _(i):
            x = x_ref[:, pl.ds(pl.multiple_of(i * depth, depth), depth)]
            for which, acc_ref in pairs:
                fetch, vmem = weights[which]
                fetch(i).wait()
                acc_ref[...] += jnp.dot(x, vmem[i], preferred_element_type=f32)

    def swap(size, peer_of, chunk, recv, row):
        copies = []
        for d in range(1, size):
            k, device = peer_of(d)
            c = remote(chunk(k), recv.at[d], sems.at[row, d], sems.at[row + 1, d], device)
            c.start()
            copies.append(c)
        return copies

    def gather(size, my, peer_of, send, full, row):
        copies = []
        for d in range(1, size):
            c = remote(send, full.at[my], sems.at[row, d], sems.at[row + 1, d], peer_of(d)[1])
            c.start()
            copies.append(c)
        full[my] = send[...]
        for d in range(1, size):
            k, device = peer_of(size - d)
            copies[d - 1].wait_send()
            remote(send, full.at[k], sems.at[row, d], sems.at[row + 1, d], device).wait_recv()

    part = res_ref.shape[0] // nr
    copies = swap(nr, fpeer, lambda k: pv_ref.at[k], pv_recv, 0)
    vals = pv_ref[fme].astype(f32)
    for d in range(1, nr):
        copies[d - 1].wait()
        vals = vals + pv_recv[d].astype(f32)
    v_send[...] = vals.astype(bf16)
    gather(nr, fme, fpeer, v_send, v_all, 2)
    for k in range(nr):
        acc_rows = v_all[k].astype(f32)
        v_full[k * part:(k + 1) * part, :] = acc_rows
    x_ref = xg_ref[0]
    x_ref[...] = v_full[...].astype(bf16)
    matmul(x_ref, (0, acc))

    po_send[...] = acc[...].astype(bf16)
    copies = swap(n, peer, lambda k: po_send, po_recv, 4)
    total = res_ref[...].astype(f32) + acc[...]
    for d in range(1, n):
        copies[d - 1].wait()
        total = total + po_recv[d].astype(f32)
    crows = res_ref.shape[0] // n
    for k in range(n):
        resid[k] = total[k * crows:(k + 1) * crows]
    sumsq = jnp.sum(total * total, axis=1, keepdims=True)
    sumsq = jnp.broadcast_to(sumsq, (total.shape[0], 128))
    for k in range(nr):
        ss_send[k] = sumsq[k * part:(k + 1) * part]
    s_copies = swap(nr, fpeer, lambda k: ss_send.at[k], ss_recv, 6)
    x_ref = xg_ref[1]
    x_ref[...] = (total * gain_ref[...]).astype(bf16)
    matmul(x_ref, (1, g_acc), (2, u_acc))

    for j, a in enumerate((g_acc, u_acc)):
        for k in range(nr):
            gu_send[k, j] = a[k * part:(k + 1) * part, :].astype(bf16)
    copies = swap(nr, fpeer, lambda k: gu_send.at[k], gu_recv, 8)
    ss = ss_send[fme]
    for d in range(1, nr):
        s_copies[d - 1].wait()
        ss = ss + ss_recv[d]
    inv = lax.rsqrt(ss[:, 0:1] / D + epsilon)
    gate = gu_send[fme, 0].astype(f32)
    up = gu_send[fme, 1].astype(f32)
    for d in range(1, nr):
        copies[d - 1].wait()
        gate = gate + gu_recv[d, 0].astype(f32)
        up = up + gu_recv[d, 1].astype(f32)
    gate = gate * inv
    up = up * inv
    h_send[...] = (gate / (1.0 + jnp.exp(-gate)) * up).astype(bf16)
    gather(nr, fme, fpeer, h_send, h_all, 10)
    for k in range(nr):
        h_full[k * part:(k + 1) * part, :] = h_all[k].astype(f32)
    x_ref = xg_ref[2]
    x_ref[...] = h_full[...].astype(bf16)
    matmul(x_ref, (3, acc))

    for k in range(n):
        piece = acc[k * crows:(k + 1) * crows, :]
        dn[k] = piece
        dn_send[k] = piece.astype(bf16)
    copies = swap(n, peer, lambda k: dn_send.at[k], dn_recv, 12)
    result = resid[me] + dn[me]
    for d in range(1, n):
        copies[d - 1].wait()
        result = result + dn_recv[d].astype(f32)
    out_ref[...] = result.astype(bf16)


def chunk_of(depth):
    for size in (1024, 768, 512, 256):
        if depth % size == 0:
            return size
    return depth


def per_device_latents(sizes, queries, cache, lengths, positions, value_up_weight, out_proj, residual,
               norm_gain, gate_weight, up_weight, down_weight):
    n, n_role, n_seq = sizes
    nr = n_role * n_seq
    rows, heads, width = queries.shape
    seqs = cache.shape[0]
    span = rows * heads // seqs
    lat = LATENT // nr
    vmem = pl.BlockSpec(memory_space=pltpu.VMEM)
    smem = pl.BlockSpec(memory_space=pltpu.SMEM)
    hbm = pl.BlockSpec(memory_space=pl.ANY)
    most = max(n, nr)
    sems = lambda k: pltpu.SemaphoreType.DMA((k, most))
    vwide = heads * value_up_weight.shape[2]
    all_rows, dd = residual.shape
    ff = gate_weight.shape[1]
    part, crows = all_rows // nr, all_rows // n

    def held(w):
        size = chunk_of(w.shape[0])
        return pltpu.VMEM((w.shape[0] // size, size, w.shape[1]), bf16)

    ws = (out_proj, gate_weight, up_weight, down_weight)
    most_chunks = max(w.shape[0] // chunk_of(w.shape[0]) for w in ws)
    V = pltpu.VMEM
    return pl.pallas_call(
        functools.partial(layer_kernel, n, n_role, n_seq),
        out_shape=jax.ShapeDtypeStruct((crows, dd), bf16),
        in_specs=[vmem, hbm, smem, smem, hbm, vmem, vmem] + [hbm] * 4,
        out_specs=vmem,
        scratch_shapes=[
            V((cache.shape[0], width, cache.shape[1]), bf16),
            V(value_up_weight.shape, bf16),
            V((n, seqs, span, width), bf16),
            V((n, seqs, span, LATENT), bf16),
            V((n, seqs, span, LATENT), bf16),
            V((n, seqs, 8, span), f32),
            V((n, seqs, 8, span), f32),
            V((nr, rows, heads, lat), bf16),
            V((nr, rows, heads, lat), bf16),
            V((heads, all_rows, lat), f32),
            V((all_rows, vwide), f32),
            V((nr, part, vwide), bf16),
            *[held(w) for w in ws],
            V((nr, part, vwide), bf16),
            V((part, vwide), bf16),
            V((nr, part, vwide), bf16),
            V((all_rows, vwide), f32),
            V((all_rows, dd), f32),
            V((all_rows, dd), bf16),
            V((n, all_rows, dd), bf16),
            V((n, crows, dd), f32),
            [V((all_rows, vwide), bf16), V((all_rows, dd), bf16), V((all_rows, ff), bf16)],
            V((all_rows, ff), f32),
            V((all_rows, ff), f32),
            V((nr, 2, part, ff), bf16),
            V((nr, 2, part, ff), bf16),
            V((nr, part, 128), f32),
            V((nr, part, 128), f32),
            V((part, ff), bf16),
            V((nr, part, ff), bf16),
            V((all_rows, ff), f32),
            V((n, crows, dd), f32),
            V((n, crows, dd), bf16),
            V((n, crows, dd), bf16),
            pltpu.SemaphoreType.DMA((4, most_chunks)),
            pltpu.SemaphoreType.DMA((2,)),
            sems(8 * seqs),
            sems(14),
        ],
        compiler_params=pltpu.CompilerParams(
            collective_id=0, has_side_effects=True, vmem_limit_bytes=VMEM_BYTES),
        name="layer",
    )(queries.reshape(seqs, span, width), cache.transpose(0, 2, 1), lengths, positions, value_up_weight,
      residual, norm_gain.reshape(1, dd), *ws)


LOG2E = 1.4426950408889634


def by_distance(n, me):
    found = []
    for i in range(n - 1):
        k = jnp.int32(0)
        for z in range(n):
            others = sorted((j for j in range(n) if j != z), key=lambda j: (abs(j - z), j))
            k = jnp.where(me == z, others[i], k)
        found.append(k)
    return found


def cut(width):
    unit = 256 if width % 256 == 0 else 128
    if width % unit or width < 2 * unit:
        return [(0, width)]
    first = width // unit // 2 * unit
    return [(0, first), (first, width)]


def heads_kernel(n, n_role, n_seq, q_hbm, cache_hbm, len_ref, pos_ref, vu_hbm, res_hbm, gain_hbm,
                 wo_hbm, wg_hbm, wu_hbm, wd_hbm, out_ref,
                 q_ref, cache, vu, res_ref, gain_ref, wo, wg, wu, wd,
                 q_send, q_all, o_send, o_recv, st_send, st_recv, w_ref,
                 a_head, v_send, xv, acc, po, po_send, po_recv, resid, ss_send, ss_recv,
                 g_acc, u_acc, gu_send, gu_recv, h_send, h_all, h_full, dn, dn_send, dn_recv,
                 lsem, wsem, qsem, gone, osem, stsem, vsem, posem, gusem, hsem, dnsem, onesem):
    nr = n_role * n_seq
    me = lax.axis_index("ctx")
    role, seq = lax.axis_index("role"), lax.axis_index("seq")
    fme = role * n_seq + seq
    near = by_distance(n, me)
    mates = []
    for dr in range(n_role):
        for ds in range(n_seq):
            if dr or ds:
                r, s = lax.rem(role + dr, n_role), lax.rem(seq + ds, n_seq)
                mates.append((r * n_seq + s, {"role": r, "seq": s}))
    seqs, span, width = q_ref.shape
    context = cache.shape[2]
    heads = span // MTP
    hk = heads // nr
    rope = width - LATENT
    lat = LATENT // nr
    own = n - 1
    extra = span * rope // LATENT

    paired = n == 4
    if paired:
        beside = me + 1 - 2 * lax.rem(me, 2)
        across = 2 - me // 2
        beyond = 3 - 3 * (me // 2)
        inner = lax.rem((me + 1) // 2, 2)
        reach = [beside, across]
    else:
        reach = near[::-1]

    q_copy = pltpu.make_async_copy(q_hbm, q_ref, lsem.at[0])
    q_copy.start()
    cache_copies = [
        pltpu.make_async_copy(cache_hbm, cache.at[:, pl.ds(0, width), :], lsem.at[1]),
        pltpu.make_async_copy(cache_hbm.at[:, pl.ds(LATENT, rope), :],
                              cache.at[:, pl.ds(width, rope), :], lsem.at[2]),
    ]
    for c in cache_copies:
        c.start()
    barrier = pltpu.get_barrier_semaphore()
    if paired:
        pl.semaphore_signal(barrier, inc=1, device_id={"ctx": beside}, device_id_type=MESH)

        @pl.when(inner == 1)
        def _():
            for k in (across, beyond):
                pl.semaphore_signal(barrier, inc=1, device_id={"ctx": k}, device_id_type=MESH)
    else:
        for k in near:
            pl.semaphore_signal(barrier, inc=1, device_id={"ctx": k}, device_id_type=MESH)
    for _, device in mates:
        pl.semaphore_signal(barrier, inc=1, device_id=device, device_id_type=MESH)
    vu_own = pltpu.make_async_copy(
        vu_hbm.at[pl.ds(pl.multiple_of(fme * hk, hk), hk)],
        vu.at[:, pl.ds(pl.multiple_of(fme * lat, lat), lat), :], lsem.at[3])
    vu_own.start()
    res_copy = pltpu.make_async_copy(res_hbm, res_ref, lsem.at[4])
    res_copy.start()
    gain_copy = pltpu.make_async_copy(gain_hbm, gain_ref.at[0], lsem.at[5])
    gain_copy.start()

    q_copy.wait()
    for s in range(seqs):
        qn, qr = [], []
        for k in range(nr):
            for t in range(MTP):
                at = t * heads + k * hk
                rows = q_ref[s, at:at + hk, :].astype(f32)
                qn.append(rows[:, :LATENT])
                qr.append(rows[:, LATENT:])
        q_send[s, :span] = jnp.concatenate(qn, axis=0).astype(bf16)
        qr = jnp.concatenate(qr, axis=0)
        qr = jnp.concatenate([qr[:span // 2], qr[span // 2:]], axis=1)
        q_send[s, span:] = jnp.concatenate(
            [qr[i:i + extra] for i in range(0, span // 2, extra)], axis=1).astype(bf16)
    weights = []
    for which, (hbm, vmem) in enumerate(((wo_hbm, wo), (wg_hbm, wg), (wu_hbm, wu), (wd_hbm, wd))):
        weights.append(pltpu.make_async_copy(hbm, vmem, wsem.at[which]))
    for c in weights:
        c.start()
    pl.semaphore_wait(barrier, len(reach) + len(mates))

    Q, RELAY, VU, O, ST, VAL, PO, SS, GU, H, DN = range(11)

    def send(src, dst, kind, recv_sem, device):
        remote(src, dst, gone.at[kind], recv_sem, device).start()

    def all_gone(kind, like):
        remote(like, like, gone.at[kind], gone.at[kind], {"ctx": near[0]}).wait_send()

    def all_here(like, recv_sem):
        remote(like, like, gone.at[0], recv_sem, {"ctx": near[0]}).wait_recv()

    def take(b, s):
        all_here(q_all.at[b, s], qsem.at[s, b])

    for s in range(seqs):
        for k in reach:
            send(q_send.at[s], q_all.at[me, s], Q, qsem.at[s, me], {"ctx": k})
    for k, device in mates:
        send(vu_hbm.at[pl.ds(pl.multiple_of(k * hk, hk), hk)],
             vu.at[:, pl.ds(pl.multiple_of(fme * lat, lat), lat), :], VU, onesem.at[0], device)

    column = lax.broadcasted_iota(jnp.int32, (span, context), 1)
    row = lax.broadcasted_iota(jnp.int32, (span, 1), 0)
    even = lax.rem(row, MTP * hk) < hk
    lane = lax.broadcasted_iota(jnp.int32, (span, 128), 1)
    half = lax.broadcasted_iota(jnp.int32, (span // 2, 2 * rope), 1) < rope
    ends = []
    for s in range(seqs):
        limit = jnp.where(even, pos_ref[MTP * s], pos_ref[MTP * s + 1]) + 1
        ends.append(jnp.minimum(limit, len_ref[s]) - me * context)

    def block(queries, s, slot):
        qn, qr = queries[:span], queries[span:].astype(f32)
        qr = jnp.concatenate([qr[:, i:i + 128] for i in range(0, LATENT, 128)], axis=0)
        zero = jnp.zeros_like(qr)
        q = jnp.concatenate(
            [qn, jnp.concatenate([jnp.where(half, qr, zero), jnp.where(half, zero, qr)],
                                 axis=0).astype(bf16)],
            axis=1)
        keys = cache[s]
        scores = jnp.dot(q, keys, preferred_element_type=f32) * (softmax_scale * LOG2E)
        scores = jnp.where(column < ends[s], scores, -1e30)
        top = jnp.maximum(jnp.max(scores, axis=1, keepdims=True), -1e29)
        probs = jnp.exp2(scores - top).astype(bf16)
        total = jnp.sum(probs.astype(f32), axis=1, keepdims=True)
        out = lax.dot_general(
            probs, keys[:LATENT], (((1,), (1,)), ((), ())), preferred_element_type=f32)
        out = out.astype(bf16)
        for k in range(nr):
            o_send[slot, s, k] = out[k * MTP * hk:(k + 1) * MTP * hk]
        stats = jnp.where(lane == 0, top, total).T
        st_send[slot, s] = jnp.concatenate([stats[0:1], stats[1:2]], axis=1)

    mine = me * nr + fme
    for c in cache_copies:
        c.wait()
    def home(s):
        block(q_send[s], s, own)
        for k, device in mates:
            send(o_send.at[own, s, k], o_recv.at[mine, s], O, osem.at[s], device)
            send(st_send.at[own, s], st_recv.at[mine, s], ST, stsem.at[s], device)
        for c in (
            pltpu.make_async_copy(o_send.at[own, s, fme], o_recv.at[mine, s], osem.at[s]),
            pltpu.make_async_copy(st_send.at[own, s], st_recv.at[mine, s], stsem.at[s]),
        ):
            c.start()

    def answer(b, s, slot):
        block(q_all[b, s], s, slot)
        for k in range(nr):
            device = {"ctx": b, "role": k // n_seq, "seq": k % n_seq}
            send(o_send.at[slot, s, k], o_recv.at[mine, s], O, osem.at[s], device)
            send(st_send.at[slot, s], st_recv.at[mine, s], ST, stsem.at[s], device)

    if paired:
        def relay(b, s):
            @pl.when(inner == 1)
            def _():
                take(b, s)
                send(q_all.at[b, s], q_all.at[b, s], RELAY, qsem.at[s, b], {"ctx": beside})

        def take_outer(b, s):
            @pl.when(inner == 0)
            def _():
                take(b, s)

        home(0)
        relay(across, 0)
        for s in range(seqs):
            take(beside, s)
            answer(beside, s, 0)
            if s == 0:
                relay(beyond, 0)
            if s + 1 < seqs:
                relay(across, s + 1)
            take_outer(across, s)
            answer(across, s, 1)
            if s + 1 < seqs:
                relay(beyond, s + 1)
            take_outer(beyond, s)
            answer(beyond, s, 2)
        for s in range(1, seqs):
            home(s)
    else:
        for s in range(seqs):
            home(s)
            for i, b in enumerate(near):
                take(b, s)
                answer(b, s, i)

    rows = seqs * MTP
    all_rows = nr * rows
    mine_at = pl.ds(pl.multiple_of(fme * MTP * hk, MTP * hk), MTP * hk)
    vdim = vu.shape[2]
    deep = hk * vdim
    others = len(mates)

    def merge(s):
        all_here(st_recv.at[:, s], stsem.at[s])
        tops, totals = [], []
        for b in range(n):
            stats = jnp.concatenate([st_recv[b * nr + j, s] for j in range(nr)], axis=0)
            tops.append(stats[:, :span])
            totals.append(stats[:, span:])
        highest = functools.reduce(jnp.maximum, tops)
        factors = [jnp.exp2(t - highest) for t in tops]
        denom = sum(f * t for f, t in zip(factors, totals))
        shares = jnp.concatenate([f / denom for f in factors], axis=0)
        copies = -(-128 // (n * nr))
        shares = jnp.concatenate([shares] * copies, axis=0)[:128]
        w_ref[s] = shares.T
        share = w_ref[s, mine_at, :]
        all_here(o_recv.at[:, s], osem.at[s])
        for j in range(nr):
            mixed = None
            for b in range(n):
                i = b * nr + j
                term = share[:, i:i + 1] * o_recv[i, s].astype(f32)
                mixed = term if mixed is None else mixed + term
            for t in range(MTP):
                a_head[:, s, j * MTP + t, :] = mixed[t * hk:(t + 1) * hk]
        if s == 0:
            vu_own.wait()
            all_here(vu.at[:, :others * lat], onesem.at[0])
        for h in range(hk):
            v_send[s, :, h * vdim:(h + 1) * vdim] = jnp.dot(
                a_head[h, s].astype(bf16), vu[h], preferred_element_type=f32).astype(bf16)
        for k, device in mates:
            send(v_send.at[s], xv.at[s, fme], VAL, vsem.at[s, fme], device)

    early, late = mates[:n_seq - 1], mates[n_seq - 1:]
    dd = acc.shape[1]
    parts = cut(dd)

    def wo_rows(k):
        return pl.ds(pl.multiple_of(k * deep, deep), deep)

    def begin(s):
        if s == 0:
            weights[0].wait()
        po[s] = jnp.dot(v_send[s], wo[wo_rows(fme), :], preferred_element_type=f32)
        for k, device in early:
            all_here(xv.at[s, k], vsem.at[s, k])
            po[s] += jnp.dot(xv[s, k], wo[wo_rows(k), :], preferred_element_type=f32)

    def finish(s):
        for k, device in late:
            all_here(xv.at[s, k], vsem.at[s, k])
        for p, (c0, c1) in enumerate(parts):
            total = po[s, :, c0:c1]
            for k, device in late:
                total = total + jnp.dot(xv[s, k], wo[wo_rows(k), c0:c1], preferred_element_type=f32)
            po[s, :, c0:c1] = total
            po_send[s, :, c0:c1] = total.astype(bf16)
            if s == seqs - 1:
                for k in near[::-1]:
                    send(po_send.at[s, :, c0:c1], po_recv.at[s, me, :, c0:c1], PO, posem.at[s, p],
                         {"ctx": k})
        if s < seqs - 1:
            for k in near[::-1]:
                send(po_send.at[s], po_recv.at[s, me], PO, posem.at[s, 0], {"ctx": k})

    for s in range(seqs):
        merge(s)
        if s:
            finish(s - 1)
        begin(s)
    finish(seqs - 1)
    all_gone(Q, q_all.at[:len(reach)])
    if paired:
        @pl.when(inner == 1)
        def _():
            all_gone(RELAY, q_all.at[:2])
    all_gone(VU, vu.at[:, :others * lat])
    all_gone(O, o_recv.at[:n * nr - 1])
    all_gone(ST, st_recv.at[:n * nr - 1])
    all_gone(VAL, xv.at[:, :others])
    res_copy.wait()
    gain_copy.wait()
    weights[1].wait()
    weights[2].wait()

    part, crows = all_rows // nr, all_rows // n
    ff = g_acc.shape[1]
    fparts = [(f, min(f + 768, ff)) for f in range(0, ff, 768)]
    sumsq = jnp.zeros((all_rows, 1), f32)
    for p, (c0, c1) in enumerate(parts):
        for s in range(seqs):
            if s == seqs - 1:
                all_here(po_recv.at[s, :n - 1, :, c0:c1], posem.at[s, p])
            elif p == 0:
                all_here(po_recv.at[s, :n - 1], posem.at[s, 0])
            total = po[s, :, c0:c1]
            for k in near:
                total = total + po_recv[s, k, :, c0:c1].astype(f32)
            for j in range(nr):
                at = j * rows + s * MTP
                acc[at:at + MTP, c0:c1] = total[j * MTP:(j + 1) * MTP]
        total = res_ref[:, c0:c1].astype(f32) + acc[:, c0:c1]
        for k in range(n):
            resid[k, :, c0:c1] = total[k * crows:(k + 1) * crows]
        sumsq = sumsq + jnp.sum(total * total, axis=1, keepdims=True)
        x = (total * gain_ref[:, c0:c1]).astype(bf16)
        last = p == len(parts) - 1
        if last:
            wide = jnp.broadcast_to(sumsq, (all_rows, 128))
            for k in range(nr):
                ss_send[k] = wide[k * part:(k + 1) * part]
            for k, device in mates:
                send(ss_send.at[k], ss_recv.at[fme], SS, onesem.at[1], device)
        for q, (f0, f1) in enumerate(fparts if last else [(0, ff)]):
            for j, (w, a) in enumerate(((wg, g_acc), (wu, u_acc))):
                y = jnp.dot(x, w[c0:c1, f0:f1], preferred_element_type=f32)
                if p:
                    y = y + a[:, f0:f1]
                if not last:
                    a[:, f0:f1] = y
                    continue
                for k in range(nr):
                    gu_send[k, j, :, f0:f1] = y[k * part:(k + 1) * part].astype(bf16)
            if last:
                for k, device in mates:
                    send(gu_send.at[k, :, :, f0:f1], gu_recv.at[fme, :, :, f0:f1],
                         GU, gusem.at[q], device)
    ss = ss_send[fme]
    all_here(ss_recv.at[:others], onesem.at[1])
    for k, device in mates:
        ss = ss + ss_recv[k]
    inv = lax.rsqrt(ss[:, 0:1] / D + epsilon)
    for q, (f0, f1) in enumerate(fparts):
        gate = gu_send[fme, 0, :, f0:f1].astype(f32)
        up = gu_send[fme, 1, :, f0:f1].astype(f32)
        all_here(gu_recv.at[:others, :, :, f0:f1], gusem.at[q])
        for k, device in mates:
            gate = gate + gu_recv[k, 0, :, f0:f1].astype(f32)
            up = up + gu_recv[k, 1, :, f0:f1].astype(f32)
        gate = gate * inv
        up = up * inv
        h = (gate / (1.0 + jnp.exp(-gate)) * up).astype(bf16)
        h_send[:, f0:f1] = h
        h_all[fme, :, f0:f1] = h
        for k, device in mates:
            send(h_send.at[:, f0:f1], h_all.at[fme, :, f0:f1], H, hsem.at[q], device)
    weights[3].wait()
    for q, (f0, f1) in enumerate(fparts):
        all_here(h_all.at[:others, :, f0:f1], hsem.at[q])
        for k in range(nr):
            h_full[k * part:(k + 1) * part, f0:f1] = h_all[k, :, f0:f1].astype(f32)
        x = h_full[:, f0:f1].astype(bf16)
        last = q == len(fparts) - 1
        for p, (c0, c1) in enumerate(parts if last else [(0, dd)]):
            y = jnp.dot(x, wd[f0:f1, c0:c1], preferred_element_type=f32)
            if q:
                y = y + acc[:, c0:c1]
            if not last:
                acc[:, c0:c1] = y
                continue
            for k in range(n):
                piece = y[k * crows:(k + 1) * crows]
                dn[k, :, c0:c1] = piece
                dn_send[k, :, c0:c1] = piece.astype(bf16)
            for k in near[::-1]:
                send(dn_send.at[k, :, c0:c1], dn_recv.at[me, :, c0:c1], DN, dnsem.at[p], {"ctx": k})
    all_gone(PO, po_recv.at[:, :n - 1])
    all_gone(SS, ss_recv.at[:others])
    all_gone(GU, gu_recv.at[:others])
    all_gone(H, h_all.at[:others])
    for p, (c0, c1) in enumerate(parts):
        result = resid[me, :, c0:c1] + dn[me, :, c0:c1]
        all_here(dn_recv.at[:n - 1, :, c0:c1], dnsem.at[p])
        for k in near:
            result = result + dn_recv[k, :, c0:c1].astype(f32)
        out_ref[:, c0:c1] = result.astype(bf16)
    all_gone(DN, dn_recv.at[:n - 1])


def per_device(sizes, queries, cache, lengths, positions, value_up_weight, out_proj, residual,
               norm_gain, gate_weight, up_weight, down_weight):
    n, n_role, n_seq = sizes
    nr = n_role * n_seq
    rows, heads, width = queries.shape
    seqs, context = cache.shape[:2]
    rope = width - LATENT
    if heads % (8 * nr) or 2 * rope != 128 or n < 2 or nr < 2:
        return per_device_latents(
            sizes, queries, cache, lengths, positions, value_up_weight, out_proj, residual,
            norm_gain, gate_weight, up_weight, down_weight)
    hk = heads // nr
    span = rows * heads // seqs
    extra = span * rope // LATENT
    vdim = value_up_weight.shape[2]
    all_rows, dd = residual.shape
    ff = gate_weight.shape[1]
    part, crows = all_rows // nr, all_rows // n
    nf = -(-ff // 768)
    vmem = pl.BlockSpec(memory_space=pltpu.VMEM)
    smem = pl.BlockSpec(memory_space=pltpu.SMEM)
    hbm = pl.BlockSpec(memory_space=pl.ANY)
    V = pltpu.VMEM
    sems = lambda *k: pltpu.SemaphoreType.DMA(k)
    return pl.pallas_call(
        functools.partial(heads_kernel, n, n_role, n_seq),
        out_shape=pltpu.VMEM((crows, dd), bf16),
        in_specs=[hbm, hbm, smem, smem] + [hbm] * 7,
        out_specs=vmem,
        scratch_shapes=[
            V((seqs, span, width), bf16),
            V((seqs, width + rope, context), bf16),
            V((hk, LATENT, vdim), bf16),
            V((all_rows, dd), bf16),
            V((1, dd), f32),
            V(out_proj.shape, bf16),
            V(gate_weight.shape, bf16),
            V(up_weight.shape, bf16),
            V(down_weight.shape, bf16),
            V((seqs, span + extra, LATENT), bf16),
            V((n, seqs, span + extra, LATENT), bf16),
            V((n, seqs, nr, MTP * hk, LATENT), bf16),
            V((n * nr, seqs, MTP * hk, LATENT), bf16),
            V((n, seqs, 1, 2 * span), f32),
            V((n * nr, seqs, 1, 2 * span), f32),
            V((seqs, span, 128), f32),
            V((hk, seqs, all_rows // seqs, LATENT), f32),
            V((seqs, all_rows // seqs, hk * vdim), bf16),
            V((seqs, nr, all_rows // seqs, hk * vdim), bf16),
            V((all_rows, dd), f32),
            V((seqs, all_rows // seqs, dd), f32),
            V((seqs, all_rows // seqs, dd), bf16),
            V((seqs, n, all_rows // seqs, dd), bf16),
            V((n, crows, dd), f32),
            V((nr, part, 128), f32),
            V((nr, part, 128), f32),
            V((all_rows, ff), f32),
            V((all_rows, ff), f32),
            V((nr, 2, part, ff), bf16),
            V((nr, 2, part, ff), bf16),
            V((part, ff), bf16),
            V((nr, part, ff), bf16),
            V((all_rows, ff), f32),
            V((n, crows, dd), f32),
            V((n, crows, dd), bf16),
            V((n, crows, dd), bf16),
            sems(6),
            sems(4),
            sems(seqs, n),
            sems(11),
            sems(seqs),
            sems(seqs),
            sems(seqs, nr),
            sems(seqs, 2),
            sems(nf),
            sems(nf),
            sems(2),
            sems(2),
        ],
        compiler_params=pltpu.CompilerParams(
            collective_id=0, has_side_effects=True, vmem_limit_bytes=VMEM_BYTES),
        name="layer",
    )(queries.reshape(seqs, span, width), cache.transpose(0, 2, 1), lengths, positions, value_up_weight,
      residual, norm_gain, out_proj, gate_weight, up_weight, down_weight)


def solution(mesh):
    placed = (
        P(("groups", "role", "seq"), "ctx", None),
        P(("groups", "role", "seq"), "ctx", None),
        P(("groups", "role", "seq")),
        P(("groups", "role", "seq")),
        P("ctx", ("role", "seq"), None),
        P("ctx", ("role", "seq")),
        P("groups", ("role", "seq")),
        P(("role", "seq")),
        P(("role", "seq"), "ctx"),
        P(("role", "seq"), "ctx"),
        P("ctx", ("role", "seq")),
    )
    sizes = (mesh.shape["ctx"], mesh.shape["role"], mesh.shape["seq"])
    return jax.shard_map(
        functools.partial(per_device, sizes),
        mesh=mesh,
        in_specs=placed,
        out_specs=P(("groups", "ctx"), ("role", "seq")),
        check_vma=False,
    )
```
